32 devices in a mesh: fsdp: 4 (over z), seq: 8 (over y, x, core).
Axes of the slice: x: 2, y: 2, z: 4, core: 2. Of those that a mesh axis runs over, the one named last changes fastest.
Arguments:
- block_input: bfloat16 [4, 1024, 2048], P('fsdp', 'seq'), may hold values from -6 to 6
- cotangent: bfloat16 [4, 1024, 2048], P('fsdp', 'seq'), may hold values from -6 to 6
- ln1_gain: bfloat16 [2048], P(('fsdp', 'seq')), may hold values from 0.5 to 1.5
- ln1_bias: bfloat16 [2048], P(('fsdp', 'seq')), may hold values from -1.5 to 1.5
- qkv_weight: bfloat16 [2048, 3, 2048], P('fsdp', None, 'seq'), may hold values from -0.125 to 0.125
- qkv_bias: bfloat16 [3, 2048], P(None, ('fsdp', 'seq')), may hold values from -8 to 8
- out_weight: bfloat16 [2048, 2048], P('seq', 'fsdp'), may hold values from -3 to 3
- ln2_gain: bfloat16 [2048], P(('fsdp', 'seq')), may hold values from 0.5 to 1.5
- ln2_bias: bfloat16 [2048], P(('fsdp', 'seq')), may hold values from -1.5 to 1.5
- gate_up_weight: bfloat16 [2048, 2, 5632], P('fsdp', None, 'seq'), may hold values from -0.125 to 0.125
- down_weight: bfloat16 [5632, 2048], P('seq', 'fsdp'), may hold values from -0.078125 to 0.078125
Outputs:
- block_output: bfloat16 [4, 1024, 2048], P('fsdp', 'seq')
- input_grad: float32 [4, 1024, 2048], P('fsdp', 'seq')
- grad_ln1_gain: float32 [2048], P(('fsdp', 'seq'))
- grad_ln1_bias: float32 [2048], P(('fsdp', 'seq'))
- grad_qkv_weight: float32 [2048, 3, 2048], P('fsdp', None, 'seq')
- grad_qkv_bias: float32 [3, 2048], P(None, ('fsdp', 'seq'))
- grad_out_weight: float32 [2048, 2048], P('seq', 'fsdp')
- grad_ln2_gain: float32 [2048], P(('fsdp', 'seq'))
- grad_ln2_bias: float32 [2048], P(('fsdp', 'seq'))
- grad_gate_up_weight: float32 [2048, 2, 5632], P('fsdp', None, 'seq')
- grad_down_weight: float32 [5632, 2048], P('seq', 'fsdp')
The draws below stay inside these ranges and needn't reach their ends.
All inputs are finite; a program needn't handle non-finite values.
Results may differ from the reference program's by a relative error of at most 0.023.
The reference program's roundings to bfloat16 on the way count: a program that leaves them out, or rounds other values in their place, can miss the bound.
Values may be sent and summed in bfloat16 or wider, within the bound.
A program may use at most 512 MiB of HBM per device.

```python
import jax
import jax.numpy as jnp
from jax import lax

D = 2048
HEADS = 32
HEAD_DIM = 64
FF = 5632
ROTARY = 16
SEQ_LEN = 1024
SEQS = 4


def draw_qkv_bias(key, part):
    base_key = jax.random.fold_in(key, 11)
    values = jnp.clip(0.3 * jax.random.normal(base_key, (3 * D,), jnp.float32), -1.5, 1.5)
    return values.reshape(3, D).astype(jnp.bfloat16)


def levels(key, extent, cuts, least, largest):
    factor_of = 1.0
    for position, blocks in cuts:
        steps = jax.random.uniform(jax.random.fold_in(jax.random.fold_in(key, 6), position), (blocks,), jnp.float32, least / len(cuts), largest / len(cuts))
        factor_of = factor_of * jnp.repeat(jnp.exp(steps), extent[position] // blocks).reshape((-1,) + (1,) * (len(extent) - 1 - position))
    return factor_of


def bell_draw(own_key, extent, width, reach, shards=(), held_as=jnp.bfloat16):
    array = jax.random.normal(own_key, extent, jnp.float32) * width
    if len(shards) > 0:
        array = levels(own_key, extent, shards, -0.22, 0.18) * array
    return jnp.clip(array, min=-reach, max=reach).astype(held_as)


def setup_inputs(seed: int = 0) -> dict:
    keys = jax.random.split(jax.random.key(seed), 12)
    return {
        "block_input": bell_draw(keys[0], (SEQS, SEQ_LEN, D), 1.0, 6.0, ((0, 4), (1, 8))),
        "cotangent": bell_draw(keys[1], (SEQS, SEQ_LEN, D), 1.0, 6.0, ((0, 4), (1, 8))),
        "ln1_gain": jnp.clip(1.0 + 0.1 * jax.random.normal(keys[2], (D,), jnp.float32), 0.5, 1.5).astype(jnp.bfloat16),
        "ln1_bias": bell_draw(keys[3], (D,), 0.3, 1.5, ((0, 32),)),
        "qkv_weight": bell_draw(keys[4], (D, 3, D), D ** -0.5, 0.125, ((0, 4), (2, 8))),
        "qkv_bias": draw_qkv_bias(jax.random.fold_in(keys[11], 71), 0),
        "out_weight": bell_draw(keys[6], (D, D), (max(4, D // 512)) ** -0.5, 3.0, ((0, 8), (1, 4))),
        "ln2_gain": jnp.clip(1.0 + 0.1 * jax.random.normal(keys[7], (D,), jnp.float32), 0.5, 1.5).astype(jnp.bfloat16),
        "ln2_bias": bell_draw(keys[8], (D,), 0.3, 1.5, ((0, 32),)),
        "gate_up_weight": bell_draw(keys[9], (D, 2, FF), D ** -0.5, 0.125, ((0, 4), (2, 8))),
        "down_weight": bell_draw(keys[10], (FF, D), FF ** -0.5, 0.078125, ((0, 8), (1, 4))),
    }


epsilon = 1e-05
masked_score = -1e+30

def widen(part):
    return lax.optimization_barrier(part).astype(jnp.float32)

def layer_norm(rows_in, gain, shift):
    center = rows_in - lax.optimization_barrier(jnp.mean(rows_in, axis=-1, keepdims=True))
    inverse = lax.rsqrt(lax.optimization_barrier(jnp.mean(center * center, axis=-1, keepdims=True)) + epsilon)
    normed = center * inverse
    return (normed * gain + shift, normed, inverse)

def norm_back(grad_rows, normed, inverse, gain):
    scaled = grad_rows * gain
    return inverse * (scaled - lax.optimization_barrier(jnp.mean(scaled, axis=-1, keepdims=True)) - normed * lax.optimization_barrier(jnp.mean(scaled * normed, axis=-1, keepdims=True)))

def rotary_tables(positions):
    half_rot = ROTARY // 2
    frequency = 10000.0 ** (-2.0 * jnp.arange(half_rot, dtype=jnp.float32) / ROTARY)
    angles = positions[:, None] * frequency[None, :]
    angles = jnp.concatenate([angles, angles], axis=1)
    return (jnp.cos(angles)[:, None, :], jnp.sin(angles)[:, None, :])

def rotate(field, cosine, sine_part, direction):
    half_rot = ROTARY // 2
    head_part = field[..., :ROTARY]
    turned = jnp.concatenate([-head_part[..., half_rot:], head_part[..., :half_rot]], axis=-1)
    moved = head_part * cosine + direction * turned * sine_part
    return jnp.concatenate([moved, field[..., ROTARY:]], axis=-1)

def attend(queries, key_rows, value_rows):
    length, head_count, head_width = queries.shape
    block_rows = min(512, length)
    score_scale = head_width ** (-0.5)
    key_float = widen(key_rows)
    value_float = widen(value_rows)
    key_pos = jnp.arange(length, dtype=jnp.int32)

    def one_block(row_start):
        query_block = widen(lax.dynamic_slice_in_dim(queries, row_start, block_rows, 0))
        scores = jnp.einsum('qhd,khd->hqk', query_block, key_float) * score_scale
        query_pos = row_start + jnp.arange(block_rows, dtype=jnp.int32)
        causal = key_pos[None, :] <= query_pos[:, None]
        scores = jnp.where(causal[None], scores, masked_score)
        row_max = lax.optimization_barrier(jnp.max(scores, axis=-1, keepdims=True))
        log_total = row_max + jnp.log(lax.optimization_barrier(jnp.sum(jnp.exp(scores - row_max), axis=-1, keepdims=True)))
        attn_probs = widen(jnp.exp(scores - log_total).astype(jnp.bfloat16))
        attn_out = jnp.einsum('hqk,khd->qhd', attn_probs, value_float).astype(jnp.bfloat16)
        return (attn_out, log_total[..., 0])
    starts = jnp.arange(length // block_rows, dtype=jnp.int32) * block_rows
    outs, totals = lax.map(one_block, starts)
    return (outs.reshape(length, head_count, head_width), jnp.transpose(totals, (1, 0, 2)).reshape(head_count, length))

def attend_back(queries, key_rows, value_rows, attn_out, log_total, grad_out):
    length, head_count, head_width = queries.shape
    block_rows = min(512, length)
    score_scale = head_width ** (-0.5)
    key_float = widen(key_rows)
    value_float = widen(value_rows)
    key_pos = jnp.arange(length, dtype=jnp.int32)
    delta = lax.optimization_barrier(jnp.sum(widen(grad_out) * widen(attn_out), axis=-1))

    def one_block(carried, row_start):
        grad_keys, grad_values = carried
        query_block = widen(lax.dynamic_slice_in_dim(queries, row_start, block_rows, 0))
        grad_block = widen(lax.dynamic_slice_in_dim(grad_out, row_start, block_rows, 0))
        total_block = lax.dynamic_slice_in_dim(log_total, row_start, block_rows, 1)
        delta_block = lax.dynamic_slice_in_dim(delta, row_start, block_rows, 0)
        scores = jnp.einsum('qhd,khd->hqk', query_block, key_float) * score_scale
        query_pos = row_start + jnp.arange(block_rows, dtype=jnp.int32)
        causal = key_pos[None, :] <= query_pos[:, None]
        scores = jnp.where(causal[None], scores, masked_score)
        attn_probs = jnp.exp(scores - total_block[..., None])
        grad_values = grad_values + jnp.einsum('hqk,qhd->khd', widen(attn_probs.astype(jnp.bfloat16)), grad_block)
        grad_probs = jnp.einsum('qhd,khd->hqk', grad_block, value_float)
        grad_scores = widen((attn_probs * (grad_probs - jnp.transpose(delta_block)[:, :, None])).astype(jnp.bfloat16))
        grad_query = jnp.einsum('hqk,khd->qhd', grad_scores, key_float) * score_scale
        grad_keys = grad_keys + jnp.einsum('hqk,qhd->khd', grad_scores, query_block) * score_scale
        return ((grad_keys, grad_values), grad_query)
    zeros = jnp.zeros((length, head_count, head_width), jnp.float32)
    starts = jnp.arange(length // block_rows, dtype=jnp.int32) * block_rows
    (grad_keys, grad_values), grad_queries = lax.scan(one_block, (zeros, zeros), starts)
    return (grad_queries.reshape(length, head_count, head_width), grad_keys, grad_values)

def reference(block_input, cotangent, ln1_gain, ln1_bias, qkv_weight, qkv_bias, out_weight, ln2_gain, ln2_bias, gate_up_weight, down_weight):
    gain_one = ln1_gain.astype(jnp.float32)
    shift_one = ln1_bias.astype(jnp.float32)
    gain_two = ln2_gain.astype(jnp.float32)
    shift_two = ln2_bias.astype(jnp.float32)
    bias_float = qkv_bias.reshape(3 * D).astype(jnp.float32)
    qkv_flat = qkv_weight.reshape(D, 3 * D)
    gate_flat = gate_up_weight.reshape(D, 2 * FF)
    cosine, sine_part = rotary_tables(jnp.arange(SEQ_LEN, dtype=jnp.float32))

    def one_sequence(totals, pair):
        seq_rows, seq_cot = pair
        block_float = seq_rows.astype(jnp.float32)
        norm_one, normed_one, inverse_one = layer_norm(block_float, gain_one, shift_one)
        input_one = norm_one.astype(jnp.bfloat16)
        projected = jnp.dot(input_one, qkv_flat, preferred_element_type=jnp.float32) + bias_float
        projected = projected.reshape(SEQ_LEN, 3, HEADS, HEAD_DIM)
        queries = rotate(projected[:, 0], cosine, sine_part, 1.0).astype(jnp.bfloat16)
        key_rows = rotate(projected[:, 1], cosine, sine_part, 1.0).astype(jnp.bfloat16)
        value_rows = projected[:, 2].astype(jnp.bfloat16)
        attn_out, log_total = attend(queries, key_rows, value_rows)
        mixed = attn_out.reshape(SEQ_LEN, D)
        residual = block_float + jnp.dot(mixed, out_weight, preferred_element_type=jnp.float32)
        norm_two, normed_two, inverse_two = layer_norm(residual, gain_two, shift_two)
        input_two = norm_two.astype(jnp.bfloat16)
        gate_up = jnp.dot(input_two, gate_flat, preferred_element_type=jnp.float32)
        gate_part = gate_up[:, :FF]
        up_part = gate_up[:, FF:]
        sigmoid_gate = jax.nn.sigmoid(gate_part)
        silu_gate = gate_part * sigmoid_gate
        hidden = (silu_gate * up_part).astype(jnp.bfloat16)
        block_output = (residual + jnp.dot(hidden, down_weight, preferred_element_type=jnp.float32)).astype(jnp.bfloat16)
        grad_down = jnp.dot(hidden.T, seq_cot, preferred_element_type=jnp.float32)
        grad_hidden = jnp.dot(seq_cot, down_weight.T, preferred_element_type=jnp.float32)
        grad_gate = grad_hidden * up_part * sigmoid_gate * (1.0 + gate_part * (1.0 - sigmoid_gate))
        grad_up = grad_hidden * silu_gate
        grad_gate_up_rows = jnp.concatenate([grad_gate, grad_up], axis=1).astype(jnp.bfloat16)
        grad_gate_up = jnp.dot(input_two.T, grad_gate_up_rows, preferred_element_type=jnp.float32)
        grad_norm_two = jnp.dot(grad_gate_up_rows, gate_flat.T, preferred_element_type=jnp.float32)
        grad_gain_two = lax.optimization_barrier(jnp.sum(grad_norm_two * normed_two, axis=0))
        grad_shift_two = lax.optimization_barrier(jnp.sum(grad_norm_two, axis=0))
        grad_residual = seq_cot.astype(jnp.float32) + norm_back(grad_norm_two, normed_two, inverse_two, gain_two)
        grad_mixed_rows = grad_residual.astype(jnp.bfloat16)
        grad_out = jnp.dot(mixed.T, grad_mixed_rows, preferred_element_type=jnp.float32)
        grad_mixed = jnp.dot(grad_mixed_rows, out_weight.T, preferred_element_type=jnp.float32).astype(jnp.bfloat16)
        grad_query, grad_keys, grad_values = attend_back(queries, key_rows, value_rows, attn_out, log_total, grad_mixed.reshape(SEQ_LEN, HEADS, HEAD_DIM))
        grad_query = rotate(grad_query, cosine, sine_part, -1.0)
        grad_keys = rotate(grad_keys, cosine, sine_part, -1.0)
        grad_qkv = jnp.stack([grad_query, grad_keys, grad_values], axis=1).reshape(SEQ_LEN, 3 * D).astype(jnp.bfloat16)
        grad_bias = lax.optimization_barrier(jnp.sum(grad_qkv.astype(jnp.float32), axis=0))
        grad_qkv_w = jnp.dot(input_one.T, grad_qkv, preferred_element_type=jnp.float32)
        grad_norm_one = jnp.dot(grad_qkv, qkv_flat.T, preferred_element_type=jnp.float32)
        grad_gain_one = lax.optimization_barrier(jnp.sum(grad_norm_one * normed_one, axis=0))
        grad_shift_one = lax.optimization_barrier(jnp.sum(grad_norm_one, axis=0))
        input_grad = grad_residual + norm_back(grad_norm_one, normed_one, inverse_one, gain_one)
        grads = (grad_gain_one, grad_shift_one, grad_qkv_w, grad_bias, grad_out, grad_gain_two, grad_shift_two, grad_gate_up, grad_down)
        return (jax.tree.map(jnp.add, totals, grads), (block_output, input_grad))
    start_totals = (jnp.zeros((D,), jnp.float32), jnp.zeros((D,), jnp.float32), jnp.zeros((D, 3 * D), jnp.float32), jnp.zeros((3 * D,), jnp.float32), jnp.zeros((D, D), jnp.float32), jnp.zeros((D,), jnp.float32), jnp.zeros((D,), jnp.float32), jnp.zeros((D, 2 * FF), jnp.float32), jnp.zeros((FF, D), jnp.float32))
    totals, (block_output, input_grad) = lax.scan(one_sequence, start_totals, (block_input, cotangent))
    return (block_output, input_grad, totals[0], totals[1], totals[2].reshape(D, 3, D), totals[3].reshape(3, D), totals[4], totals[5], totals[6], totals[7].reshape(D, 2, FF), totals[8])
```

```python
import functools

import jax
import jax.numpy as jnp
from jax import lax
from jax.experimental import pallas as pl
from jax.experimental.pallas import tpu as pltpu
from jax.sharding import PartitionSpec as P

HEADS = 32
HEAD_DIM = 64
FF = 5632
ROTARY = 16


epsilon = 1e-05
masked_score = -1e30


def layer_norm(rows_in, gain, shift):
    center = rows_in - jnp.mean(rows_in, axis=-1, keepdims=True)
    inverse = lax.rsqrt(jnp.mean(center * center, axis=-1, keepdims=True) + epsilon)
    normed = center * inverse
    return (normed * gain + shift, normed, inverse)


def norm_back(grad_rows, normed, inverse, gain):
    scaled = grad_rows * gain
    return inverse * (
        scaled
        - jnp.mean(scaled, axis=-1, keepdims=True)
        - normed * jnp.mean(scaled * normed, axis=-1, keepdims=True)
    )


def rotary_tables(positions):
    half_rot = ROTARY // 2
    frequency = 10000.0 ** (-2.0 * jnp.arange(half_rot, dtype=jnp.float32) / ROTARY)
    angles = positions[:, None] * frequency[None, :]
    angles = jnp.concatenate([angles, angles], axis=1)
    return (jnp.cos(angles)[:, None, :], jnp.sin(angles)[:, None, :])


def rotate(field, cosine, sine_part, direction):
    half_rot = ROTARY // 2
    head_part = field[..., :ROTARY]
    turned = jnp.concatenate([-head_part[..., half_rot:], head_part[..., :half_rot]], axis=-1)
    moved = head_part * cosine + direction * turned * sine_part
    return jnp.concatenate([moved, field[..., ROTARY:]], axis=-1)


def attend(queries, key_rows, value_rows):
    length, head_count, head_width = queries.shape
    block_rows = min(512, length)
    score_scale = head_width ** (-0.5)
    key_pos = jnp.arange(length, dtype=jnp.int32)

    def one_block(row_start):
        query_block = lax.dynamic_slice_in_dim(queries, row_start, block_rows, 0)
        scores = (
            jnp.einsum("qhd,khd->hqk", query_block, key_rows, preferred_element_type=jnp.float32)
            * score_scale
        )
        query_pos = row_start + jnp.arange(block_rows, dtype=jnp.int32)
        causal = key_pos[None, :] <= query_pos[:, None]
        scores = jnp.where(causal[None], scores, masked_score)
        row_max = jnp.max(scores, axis=-1, keepdims=True)
        log_total = row_max + jnp.log(jnp.sum(jnp.exp(scores - row_max), axis=-1, keepdims=True))
        attn_probs = jnp.exp(scores - log_total).astype(jnp.bfloat16)
        attn_out = jnp.einsum(
            "hqk,khd->qhd", attn_probs, value_rows, preferred_element_type=jnp.float32
        ).astype(jnp.bfloat16)
        return (attn_out, log_total[..., 0])

    starts = jnp.arange(length // block_rows, dtype=jnp.int32) * block_rows
    outs, totals = lax.map(one_block, starts)
    return (
        outs.reshape(length, head_count, head_width),
        jnp.transpose(totals, (1, 0, 2)).reshape(head_count, length),
    )


def attend_back(queries, key_rows, value_rows, attn_out, log_total, grad_out):
    length, head_count, head_width = queries.shape
    block_rows = min(512, length)
    score_scale = head_width ** (-0.5)
    key_pos = jnp.arange(length, dtype=jnp.int32)
    delta = jnp.sum(grad_out.astype(jnp.float32) * attn_out.astype(jnp.float32), axis=-1)

    def one_block(carried, row_start):
        grad_keys, grad_values = carried
        query_block = lax.dynamic_slice_in_dim(queries, row_start, block_rows, 0)
        grad_block = lax.dynamic_slice_in_dim(grad_out, row_start, block_rows, 0)
        total_block = lax.dynamic_slice_in_dim(log_total, row_start, block_rows, 1)
        delta_block = lax.dynamic_slice_in_dim(delta, row_start, block_rows, 0)
        scores = (
            jnp.einsum("qhd,khd->hqk", query_block, key_rows, preferred_element_type=jnp.float32)
            * score_scale
        )
        query_pos = row_start + jnp.arange(block_rows, dtype=jnp.int32)
        causal = key_pos[None, :] <= query_pos[:, None]
        scores = jnp.where(causal[None], scores, masked_score)
        attn_probs = jnp.exp(scores - total_block[..., None])
        grad_values = grad_values + jnp.einsum(
            "hqk,qhd->khd",
            attn_probs.astype(jnp.bfloat16),
            grad_block,
            preferred_element_type=jnp.float32,
        )
        grad_probs = jnp.einsum(
            "qhd,khd->hqk", grad_block, value_rows, preferred_element_type=jnp.float32
        )
        grad_scores = (attn_probs * (grad_probs - jnp.transpose(delta_block)[:, :, None])).astype(
            jnp.bfloat16
        )
        grad_query = (
            jnp.einsum("hqk,khd->qhd", grad_scores, key_rows, preferred_element_type=jnp.float32)
            * score_scale
        )
        grad_keys = (
            grad_keys
            + jnp.einsum(
                "hqk,qhd->khd", grad_scores, query_block, preferred_element_type=jnp.float32
            )
            * score_scale
        )
        return ((grad_keys, grad_values), grad_query)

    zeros = jnp.zeros((length, head_count, head_width), jnp.float32)
    starts = jnp.arange(length // block_rows, dtype=jnp.int32) * block_rows
    (grad_keys, grad_values), grad_queries = lax.scan(one_block, (zeros, zeros), starts)
    return (grad_queries.reshape(length, head_count, head_width), grad_keys, grad_values)


MESH = pl.DeviceIdType.MESH
NT = (((1,), (1,)), ((), ()))
TN = (((0,), (0,)), ((), ()))
f32, bf16 = jnp.float32, jnp.bfloat16


def dot_nn(a, b):
    return jnp.dot(a, b, preferred_element_type=f32)


def dot_nt(a, b):
    return lax.dot_general(a, b, NT, preferred_element_type=f32)


def dot_tn(a, b):
    return lax.dot_general(a, b, TN, preferred_element_type=f32)


def remote(src, dst, send_sem, recv_sem, device):
    return pltpu.make_async_remote_copy(
        src_ref=src, dst_ref=dst, send_sem=send_sem, recv_sem=recv_sem,
        device_id=device, device_id_type=MESH)


def line_barrier(f, n):
    barrier = pltpu.get_barrier_semaphore()

    @pl.when(f > 0)
    def _():
        pl.semaphore_signal(barrier, inc=1, device_id={"fsdp": f - 1}, device_id_type=MESH)

    @pl.when(f < n - 1)
    def _():
        pl.semaphore_signal(barrier, inc=1, device_id={"fsdp": f + 1}, device_id_type=MESH)

    pl.semaphore_wait(barrier, (f > 0).astype(jnp.int32) + (f < n - 1).astype(jnp.int32))


class LineGather:
    def __init__(self, f, n, count, own, slot, sems):
        self.f, self.n, self.count, self.own, self.slot = f, n, count, own, slot
        self.send_r, self.recv_r, self.send_l, self.recv_l = sems

    def copy(self, src, p, h, source, rightward):
        f = self.f
        send, recv = (self.send_r, self.recv_r) if rightward else (self.send_l, self.recv_l)
        target = f + 1 if rightward else f - 1
        return remote(src, self.slot(p, source), send.at[p, h], recv.at[p, h], {"fsdp": target})

    def tick(self, t):
        f, n, count = self.f, self.n, self.count

        @pl.when((t >= 0) & (t < count))
        def _():
            @pl.when(f < n - 1)
            def _():
                self.own(t, lambda src: self.copy(src, t, 0, f, True).start())

            @pl.when(f > 0)
            def _():
                self.own(t, lambda src: self.copy(src, t, 0, f, False).start())

        for h in range(1, n):
            p = t - h
            valid = (p >= 0) & (p < count)

            @pl.when(valid & (f - h >= 0))
            def _(p=p, h=h):
                here = self.slot(p, f - h)
                self.copy(here, p, h - 1, f - h, True).wait_recv()

                @pl.when(f < n - 1)
                def _():
                    self.copy(here, p, h, f - h, True).start()

            @pl.when(valid & (f + h <= n - 1))
            def _(p=p, h=h):
                here = self.slot(p, f + h)
                self.copy(here, p, h - 1, f + h, False).wait_recv()

                @pl.when(f > 0)
                def _():
                    self.copy(here, p, h, f + h, False).start()

    def drain(self, p):
        f, n = self.f, self.n
        for h in range(0, n - 1):
            @pl.when((f - h >= 0) & (f < n - 1))
            def _(h=h):
                self.copy(self.slot(p, f - h), p, h, f - h, True).wait_send()

            @pl.when((f + h <= n - 1) & (f > 0))
            def _(h=h):
                self.copy(self.slot(p, f + h), p, h, f + h, False).wait_send()


class LineReduce:
    def __init__(self, f, n, count, block, from_left, from_right, sems, finish):
        self.f, self.n, self.count, self.block = f, n, count, block
        self.from_left, self.from_right, self.finish = from_left, from_right, finish
        self.send_r, self.recv_r, self.send_l, self.recv_l = sems

    def right(self, p, j):
        return remote(self.block(p, j), self.from_left.at[p, j - 1], self.send_r.at[p, j - 1],
                      self.recv_r.at[p, j - 1], {"fsdp": self.f + 1})

    def left(self, p, j):
        return remote(self.block(p, j), self.from_right.at[p, j], self.send_l.at[p, j],
                      self.recv_l.at[p, j], {"fsdp": self.f - 1})

    def tick(self, u):
        f, n, count = self.f, self.n, self.count
        p = u - f

        @pl.when((p >= 0) & (p < count))
        def _():
            for j in range(n - 1, 0, -1):
                @pl.when((f > 0) & (j >= f))
                def _(j=j):
                    self.right(p, j).wait_recv()

                @pl.when((f > 0) & (j > f))
                def _(j=j):
                    here = self.block(p, j)
                    here[...] = (here[...].astype(f32) + self.from_left[p, j - 1].astype(f32)).astype(bf16)

                @pl.when(j > f)
                def _(j=j):
                    self.right(p, j).start()

        q = u - (n - 1 - f)

        @pl.when((q >= 0) & (q < count))
        def _():
            for j in range(0, n - 1):
                @pl.when((f < n - 1) & (j <= f))
                def _(j=j):
                    self.left(q, j).wait_recv()

                @pl.when((f < n - 1) & (j < f))
                def _(j=j):
                    here = self.block(q, j)
                    here[...] = (here[...].astype(f32) + self.from_right[q, j].astype(f32)).astype(bf16)

                @pl.when(j < f)
                def _(j=j):
                    self.left(q, j).start()

        e = u - (n - 1)

        @pl.when((e >= 0) & (e < count))
        def _():
            for j in range(n):
                @pl.when(j > f)
                def _(j=j):
                    self.right(e, j).wait_send()

                @pl.when(j < f)
                def _(j=j):
                    self.left(e, j).wait_send()
            self.finish(e)


def mlp_kernel(n, r, rb, in2_hbm, cot_hbm, wgu_hbm, wd_hbm,
               out_hbm, gin_hbm, ggu_hbm, gd_hbm,
               in2, cot, acc_o, acc_g, w, hid, dga, dup, parts, from_left, from_right,
               stage, load_sems, own_sems, ag_sr, ag_rr, ag_sl, ag_rl, rs_sr, rs_rr, rs_sl, rs_rl,
               stage_sems):
    f = lax.axis_index("fsdp")
    tokens, width = in2.shape
    wz = width // n
    ff = wd_hbm.shape[0]
    nc = ff // r
    count = 3 * nc
    ring = parts.shape[0]
    loads = [pltpu.make_async_copy(in2_hbm, in2, load_sems.at[0]),
             pltpu.make_async_copy(cot_hbm, cot, load_sems.at[1])]
    for c in loads:
        c.start()

    def rows_of(p):
        return pl.ds(pl.multiple_of(p // 3 * r, r), r)

    def own(p, use):
        kind = lax.rem(p, 3)

        @pl.when(kind < 2)
        def _():
            use(wgu_hbm.at[kind, rows_of(p)])

        @pl.when(kind == 2)
        def _():
            use(wd_hbm.at[rows_of(p)])

    def slot(p, source):
        return w.at[p, :, pl.ds(pl.multiple_of(source * wz, wz), wz)]

    def own_copy(p, act):
        own(p, lambda src: act(pltpu.make_async_copy(src, slot(p, f), own_sems.at[p])))

    @pl.loop(0, count)
    def _(p):
        own_copy(p, lambda c: c.start())

    line_barrier(f, n)
    gather = LineGather(f, n, count, own, slot, (ag_sr, ag_rr, ag_sl, ag_rl))

    def block(p, j):
        return parts.at[lax.rem(p, ring), :, pl.ds(j * wz, wz)]

    def stage_out(p, act):
        kind = lax.rem(p, 3)
        sl = lax.rem(p, 2)

        @pl.when(kind < 2)
        def _():
            act(pltpu.make_async_copy(stage.at[sl], ggu_hbm.at[kind, rows_of(p)], stage_sems.at[sl]))

        @pl.when(kind == 2)
        def _():
            act(pltpu.make_async_copy(stage.at[sl], gd_hbm.at[rows_of(p)], stage_sems.at[sl]))

    def finish(p):
        @pl.when(p >= 2)
        def _():
            stage_out(p - 2, lambda c: c.wait())
        sl = lax.rem(p, 2)
        mine = parts.at[lax.rem(p, ring), :, pl.ds(pl.multiple_of(f * wz, wz), wz)]
        stage[sl] = mine[...].astype(f32)

        @pl.when(f > 0)
        def _():
            stage[sl] += from_left[p, jnp.maximum(f - 1, 0)].astype(f32)

        @pl.when(f < n - 1)
        def _():
            stage[sl] += from_right[p, jnp.minimum(f, n - 2)].astype(f32)
        stage_out(p, lambda c: c.start())

    reduce = LineReduce(f, n, count, block, from_left, from_right, (rs_sr, rs_rr, rs_sl, rs_rl), finish)

    acc_o[...] = jnp.zeros_like(acc_o)
    acc_g[...] = jnp.zeros_like(acc_g)

    first = 3 + n - 1

    @pl.loop(0, first)
    def _(t):
        gather.tick(t)

    for c in loads:
        c.wait()

    def compute(c):
        for k in range(3):
            own_copy(3 * c + k, lambda cc: cc.wait())

        @pl.loop(0, tokens // rb)
        def _(i):
            rows = pl.ds(pl.multiple_of(i * rb, rb), rb)
            a = in2[rows, :]
            gate = dot_nt(a, w[3 * c])
            up = dot_nt(a, w[3 * c + 1])
            gh = dot_nt(cot[rows, :], w[3 * c + 2])
            sig = jax.nn.sigmoid(gate)
            silu = gate * sig
            h = (silu * up).astype(bf16)
            dg = (gh * up * sig * (1.0 + gate * (1.0 - sig))).astype(bf16)
            du = (gh * silu).astype(bf16)
            hid[rows, :] = h
            dga[rows, :] = dg
            dup[rows, :] = du
            acc_o[rows, :] = (acc_o[rows, :].astype(f32) + dot_nn(h, w[3 * c + 2])).astype(acc_o.dtype)
            acc_g[rows, :] = (acc_g[rows, :].astype(f32) + dot_nn(dg, w[3 * c]) + dot_nn(du, w[3 * c + 1])).astype(acc_g.dtype)

        for k, (small, big) in enumerate(((dga, in2), (dup, in2), (hid, cot))):
            for j in range(n):
                block(3 * c + k, j)[...] = dot_tn(small[...], big[:, pl.ds(j * wz, wz)]).astype(bf16)

    @pl.loop(0, nc)
    def _(c):
        compute(c)

        @pl.loop(0, 3)
        def _(k):
            gather.tick(3 * c + k + first)
            reduce.tick(3 * c + k)

    in2[...] = acc_o[...].astype(bf16)
    cot[...] = acc_g[...].astype(bf16)
    stores = [pltpu.make_async_copy(in2, out_hbm, load_sems.at[0]),
              pltpu.make_async_copy(cot, gin_hbm, load_sems.at[1])]
    for c in stores:
        c.start()

    @pl.loop(0, n - 1)
    def _(k):
        reduce.tick(count + k)

    @pl.loop(0, count)
    def _(p):
        gather.drain(p)
    for p in (count - 2, count - 1):
        stage_out(jnp.int32(p), lambda c: c.wait())
    for c in stores:
        c.wait()


def piece_rows(ff):
    r = 0
    for cand in range(16, 257, 16):
        if ff % cand == 0:
            r = cand
    return r


def mlp(in2, cot, wgu, wd, n, cid):
    tokens, width = in2.shape
    ff, wz = wd.shape
    r = piece_rows(ff)
    rb = min(256, tokens)
    nc = ff // r
    count = 3 * nc
    ring = min(count, 3 * ((n - 1 + 2) // 3) + 3)
    any_spec = pl.BlockSpec(memory_space=pl.ANY)
    acc_dtype = f32 if tokens * width * 8 <= 20 * 2**20 else bf16
    D = pltpu.SemaphoreType.DMA
    return pl.pallas_call(
        functools.partial(mlp_kernel, n, r, rb),
        out_shape=(
            jax.ShapeDtypeStruct((tokens, width), bf16),
            jax.ShapeDtypeStruct((tokens, width), bf16),
            jax.ShapeDtypeStruct((2, ff, wz), f32),
            jax.ShapeDtypeStruct((ff, wz), f32),
        ),
        in_specs=[any_spec] * 4,
        out_specs=[any_spec] * 4,
        scratch_shapes=[
            pltpu.VMEM((tokens, width), bf16),
            pltpu.VMEM((tokens, width), bf16),
            pltpu.VMEM((tokens, width), acc_dtype),
            pltpu.VMEM((tokens, width), acc_dtype),
            pltpu.VMEM((count, r, width), bf16),
            pltpu.VMEM((tokens, r), bf16),
            pltpu.VMEM((tokens, r), bf16),
            pltpu.VMEM((tokens, r), bf16),
            pltpu.VMEM((ring, r, width), bf16),
            pltpu.VMEM((count, n - 1, r, wz), bf16),
            pltpu.VMEM((count, n - 1, r, wz), bf16),
            pltpu.VMEM((2, r, wz), f32),
            D((2,)),
            D((count,)),
        ] + [D((count, n - 1))] * 8 + [D((2,))],
        compiler_params=pltpu.CompilerParams(
            collective_id=cid, has_side_effects=True, vmem_limit_bytes=64 * 1024 * 1024 - 65536),
        name="mlp",
    )(in2, cot, wgu, wd)


def gather_rows(rows):
    return lax.all_gather(rows, "seq", axis=0, tiled=True)


def scatter_rows(partial):
    return lax.psum_scatter(
        partial.astype(jnp.bfloat16), "seq", scatter_dimension=0, tiled=True
    ).astype(jnp.float32)


def scatter_weight(grad, axis):
    return lax.psum_scatter(
        grad.astype(jnp.bfloat16), "fsdp", scatter_dimension=axis, tiled=True
    ).astype(jnp.float32)


def local(
    block_input,
    cotangent,
    ln1_gain,
    ln1_bias,
    qkv_weight,
    qkv_bias,
    out_weight,
    ln2_gain,
    ln2_bias,
    gate_up_weight,
    down_weight,
):
    seq_here, tok_here, model_width = block_input.shape
    groups = lax.axis_size("seq")
    length = tok_here * groups
    heads_here = HEADS // groups
    cols_here = heads_here * HEAD_DIM
    ff_here = FF // groups
    small = jnp.concatenate(
        [
            ln1_gain[None],
            ln1_bias[None],
            ln2_gain[None],
            ln2_bias[None],
            qkv_bias,
        ],
        axis=0,
    )
    small_full = lax.all_gather(small, ("fsdp", "seq"), axis=1, tiled=True).astype(jnp.float32)
    gain_one, shift_one, gain_two, shift_two = [small_full[i] for i in range(4)]
    head_start = lax.axis_index("seq") * cols_here
    bias_here = lax.dynamic_slice_in_dim(small_full[4:], head_start, cols_here, 1)

    qkv_full = lax.all_gather(qkv_weight, "fsdp", axis=0, tiled=True)
    out_full = lax.all_gather(out_weight, "fsdp", axis=1, tiled=True)
    qkv_full = qkv_full.reshape(model_width, 3 * cols_here)

    block_float = block_input[0].astype(jnp.float32)
    cot_here = cotangent[0]
    cot_float = cot_here.astype(jnp.float32)
    norm_one, normed_one, inverse_one = layer_norm(block_float, gain_one, shift_one)
    in_one = gather_rows(norm_one.astype(jnp.bfloat16))
    cot_all = gather_rows(cot_here)

    projected = jnp.dot(in_one, qkv_full, preferred_element_type=jnp.float32) + bias_here.reshape(
        3 * cols_here
    )
    projected = projected.reshape(length, 3, heads_here, HEAD_DIM)
    cosine, sine_part = rotary_tables(jnp.arange(length, dtype=jnp.float32))
    queries = rotate(projected[:, 0], cosine, sine_part, 1.0).astype(jnp.bfloat16)
    key_rows = rotate(projected[:, 1], cosine, sine_part, 1.0).astype(jnp.bfloat16)
    value_rows = projected[:, 2].astype(jnp.bfloat16)
    head_out, head_total = attend(queries, key_rows, value_rows)
    mixed = head_out.reshape(length, cols_here)
    residual = block_float + scatter_rows(
        jnp.dot(mixed, out_full, preferred_element_type=jnp.float32)
    )
    norm_two, normed_two, inverse_two = layer_norm(residual, gain_two, shift_two)
    in_two = gather_rows(norm_two.astype(jnp.bfloat16))
    out_sum, grad_sum, grad_gate_up, grad_down = mlp(
        in_two,
        cot_all,
        jnp.transpose(gate_up_weight, (1, 2, 0)),
        down_weight,
        lax.axis_size("fsdp"),
        0,
    )
    grad_gate_up = jnp.transpose(grad_gate_up, (2, 0, 1))
    block_output = residual + scatter_rows(out_sum)
    grad_norm_two = scatter_rows(grad_sum)
    grad_gain_two = jnp.sum(grad_norm_two * normed_two, axis=0)
    grad_shift_two = jnp.sum(grad_norm_two, axis=0)
    grad_residual = cot_float + norm_back(grad_norm_two, normed_two, inverse_two, gain_two)
    grad_rows = gather_rows(grad_residual.astype(jnp.bfloat16))
    grad_mixed = jnp.einsum(
        "td,cd->tc", grad_rows, out_full, preferred_element_type=jnp.float32
    ).astype(jnp.bfloat16)
    grad_out = scatter_weight(
        jnp.einsum("tc,td->cd", mixed, grad_rows, preferred_element_type=jnp.float32), 1
    )
    grad_query, grad_keys, grad_values = attend_back(
        queries,
        key_rows,
        value_rows,
        head_out,
        head_total,
        grad_mixed.reshape(length, heads_here, HEAD_DIM),
    )
    grad_query = rotate(grad_query, cosine, sine_part, -1.0)
    grad_keys = rotate(grad_keys, cosine, sine_part, -1.0)
    grad_qkv = (
        jnp.stack([grad_query, grad_keys, grad_values], axis=1)
        .astype(jnp.bfloat16)
        .reshape(length, 3 * cols_here)
    )
    bias_grad = jnp.sum(grad_qkv.astype(jnp.float32), axis=0).reshape(3, cols_here)
    grad_norm_one = scatter_rows(
        jnp.einsum("tf,cf->tc", grad_qkv, qkv_full, preferred_element_type=jnp.float32)
    )
    grad_qkv_weight = scatter_weight(
        jnp.einsum("tc,tf->cf", in_one, grad_qkv, preferred_element_type=jnp.float32).reshape(
            model_width, 3, cols_here
        ),
        0,
    )
    grad_gain_one = jnp.sum(grad_norm_one * normed_one, axis=0)
    grad_shift_one = jnp.sum(grad_norm_one, axis=0)
    input_grad = grad_residual + norm_back(grad_norm_one, normed_one, inverse_one, gain_one)
    bias_wide = lax.dynamic_update_slice_in_dim(
        jnp.zeros((3, model_width), jnp.float32), bias_grad, head_start, 1
    )
    vectors = jnp.concatenate(
        [
            grad_gain_one[None],
            grad_shift_one[None],
            grad_gain_two[None],
            grad_shift_two[None],
            bias_wide,
        ],
        axis=0,
    )
    vectors = lax.psum_scatter(vectors, ("fsdp", "seq"), scatter_dimension=1, tiled=True)
    return (
        block_output.astype(jnp.bfloat16)[None],
        input_grad[None],
        vectors[0],
        vectors[1],
        grad_qkv_weight,
        vectors[4:],
        grad_out,
        vectors[2],
        vectors[3],
        grad_gate_up,
        grad_down,
    )


def solution(mesh):
    placed = (
        P("fsdp", "seq", None),
        P("fsdp", "seq", None),
        P(("fsdp", "seq")),
        P(("fsdp", "seq")),
        P("fsdp", None, "seq"),
        P(None, ("fsdp", "seq")),
        P("seq", "fsdp"),
        P(("fsdp", "seq")),
        P(("fsdp", "seq")),
        P("fsdp", None, "seq"),
        P("seq", "fsdp"),
    )
    return jax.shard_map(
        local,
        mesh=mesh,
        in_specs=placed,
        out_specs=(
            P("fsdp", "seq", None),
            P("fsdp", "seq", None),
            P(("fsdp", "seq")),
            P(("fsdp", "seq")),
            P("fsdp", None, "seq"),
            P(None, ("fsdp", "seq")),
            P("seq", "fsdp"),
            P(("fsdp", "seq")),
            P(("fsdp", "seq")),
            P("fsdp", None, "seq"),
            P("seq", "fsdp"),
        ),
        check_vma=False,
    )
```

```python
import functools

import jax
import jax.numpy as jnp
from jax import lax
from jax.experimental import pallas as pl
from jax.experimental.pallas import tpu as pltpu
from jax.sharding import PartitionSpec as P

HEAD_DIM = 64
ROTARY = 16

epsilon = 1e-05
masked_score = -1e30

MESH = pl.DeviceIdType.MESH
NT = (((1,), (1,)), ((), ()))
TN = (((0,), (0,)), ((), ()))
f32, bf16 = jnp.float32, jnp.bfloat16


def dot_nn(a, b):
    return jnp.dot(a, b, preferred_element_type=f32)


def dot_nt(a, b):
    return lax.dot_general(a, b, NT, preferred_element_type=f32)


def dot_tn(a, b):
    return lax.dot_general(a, b, TN, preferred_element_type=f32)


def remote(src, dst, send_sem, recv_sem, device):
    return pltpu.make_async_remote_copy(
        src_ref=src, dst_ref=dst, send_sem=send_sem, recv_sem=recv_sem,
        device_id=device, device_id_type=MESH)


def line_barrier(f, n):
    barrier = pltpu.get_barrier_semaphore()

    @pl.when(f > 0)
    def _():
        pl.semaphore_signal(barrier, inc=1, device_id={"fsdp": f - 1}, device_id_type=MESH)

    @pl.when(f < n - 1)
    def _():
        pl.semaphore_signal(barrier, inc=1, device_id={"fsdp": f + 1}, device_id_type=MESH)

    pl.semaphore_wait(barrier, (f > 0).astype(jnp.int32) + (f < n - 1).astype(jnp.int32))


def when(condition):
    if isinstance(condition, (bool, int)):
        return (lambda body: body()) if condition else (lambda body: None)
    return pl.when(condition)


class LineGather:
    def __init__(self, f, n, count, own, slot, sems):
        self.f, self.n, self.count, self.own, self.slot = f, n, count, own, slot
        self.send_r, self.recv_r, self.send_l, self.recv_l = sems

    def copy(self, src, p, h, source, rightward):
        f = self.f
        send, recv = (self.send_r, self.recv_r) if rightward else (self.send_l, self.recv_l)
        target = f + 1 if rightward else f - 1
        return remote(src, self.slot(p, source), send.at[p, h], recv.at[p, h], {"fsdp": target})

    def tick(self, t):
        f, n, count = self.f, self.n, self.count

        @when((t >= 0) & (t < count))
        def _():
            @pl.when(f < n - 1)
            def _():
                self.own(t, lambda src: self.copy(src, t, 0, f, True).start())

            @pl.when(f > 0)
            def _():
                self.own(t, lambda src: self.copy(src, t, 0, f, False).start())

        for h in range(1, n):
            self.arrive(t - h, h)

    def arrive(self, p, h):
        f, n = self.f, self.n

        @when((p >= 0) & (p < self.count))
        def _():
            @pl.when(f - h >= 0)
            def _():
                here = self.slot(p, f - h)
                self.copy(here, p, h - 1, f - h, True).wait_recv()
                if h < n - 1:
                    @pl.when(f < n - 1)
                    def _():
                        self.copy(here, p, h, f - h, True).start()

            @pl.when(f + h <= n - 1)
            def _():
                here = self.slot(p, f + h)
                self.copy(here, p, h - 1, f + h, False).wait_recv()
                if h < n - 1:
                    @pl.when(f > 0)
                    def _():
                        self.copy(here, p, h, f + h, False).start()

    def drain(self, p):
        f, n = self.f, self.n
        for h in range(0, n - 1):
            @pl.when((f - h >= 0) & (f < n - 1))
            def _(h=h):
                self.copy(self.slot(p, f - h), p, h, f - h, True).wait_send()

            @pl.when((f + h <= n - 1) & (f > 0))
            def _(h=h):
                self.copy(self.slot(p, f + h), p, h, f + h, False).wait_send()


class LineReduce:
    def __init__(self, f, n, count, block, from_left, from_right, sems, finish):
        self.f, self.n, self.count, self.block = f, n, count, block
        self.from_left, self.from_right, self.finish = from_left, from_right, finish
        self.send_r, self.recv_r, self.send_l, self.recv_l = sems

    def right(self, p, j):
        return remote(self.block(p, j), self.from_left.at[p, j - 1], self.send_r.at[p, j - 1],
                      self.recv_r.at[p, j - 1], {"fsdp": self.f + 1})

    def left(self, p, j):
        return remote(self.block(p, j), self.from_right.at[p, j], self.send_l.at[p, j],
                      self.recv_l.at[p, j], {"fsdp": self.f - 1})

    def tick(self, u):
        f, n, count = self.f, self.n, self.count
        p = u - f

        @pl.when((p >= 0) & (p < count))
        def _():
            for j in range(n - 1, 0, -1):
                @pl.when((f > 0) & (j >= f))
                def _(j=j):
                    self.right(p, j).wait_recv()

                @pl.when((f > 0) & (j > f))
                def _(j=j):
                    here = self.block(p, j)
                    here[...] = (here[...].astype(f32) + self.from_left[p, j - 1].astype(f32)).astype(bf16)

                @pl.when(j > f)
                def _(j=j):
                    self.right(p, j).start()

        q = u - (n - 1 - f)

        @pl.when((q >= 0) & (q < count))
        def _():
            for j in range(0, n - 1):
                @pl.when((f < n - 1) & (j <= f))
                def _(j=j):
                    self.left(q, j).wait_recv()

                @pl.when((f < n - 1) & (j < f))
                def _(j=j):
                    here = self.block(q, j)
                    here[...] = (here[...].astype(f32) + self.from_right[q, j].astype(f32)).astype(bf16)

                @pl.when(j < f)
                def _(j=j):
                    self.left(q, j).start()

        e = u - (n - 1)

        @pl.when((e >= 0) & (e < count))
        def _():
            for j in range(n):
                @pl.when(j > f)
                def _(j=j):
                    self.right(e, j).wait_send()

                @pl.when(j < f)
                def _(j=j):
                    self.left(e, j).wait_send()
            self.finish(e)


def mlp_kernel(n, r, rb, in2_hbm, cot_hbm, wgu_hbm, wd_hbm,
               out_hbm, gin_hbm, ggu_hbm, gd_hbm,
               in2, cot, acc_o, acc_g, w, hid, dga, dup, parts, from_left, from_right,
               stage, load_sems, own_sems, ag_sr, ag_rr, ag_sl, ag_rl, rs_sr, rs_rr, rs_sl, rs_rl,
               stage_sems):
    f = lax.axis_index("fsdp")
    tokens, width = in2.shape
    wz = width // n
    ff = wd_hbm.shape[0]
    nc = ff // r
    count = 3 * nc
    ring = parts.shape[0]
    loads = [pltpu.make_async_copy(in2_hbm, in2, load_sems.at[0]),
             pltpu.make_async_copy(cot_hbm, cot, load_sems.at[1])]
    for c in loads:
        c.start()

    def rows_of(p):
        return pl.ds(pl.multiple_of(p // 3 * r, r), r)

    def own(p, use):
        kind = lax.rem(p, 3)

        @pl.when(kind < 2)
        def _():
            use(wgu_hbm.at[kind, rows_of(p)])

        @pl.when(kind == 2)
        def _():
            use(wd_hbm.at[rows_of(p)])

    def slot(p, source):
        return w.at[p, :, pl.ds(pl.multiple_of(source * wz, wz), wz)]

    def own_copy(p, act):
        own(p, lambda src: act(pltpu.make_async_copy(src, slot(p, f), own_sems.at[p])))

    @pl.loop(0, count)
    def _(p):
        own_copy(p, lambda c: c.start())

    line_barrier(f, n)
    gather = LineGather(f, n, count, own, slot, (ag_sr, ag_rr, ag_sl, ag_rl))

    def block(p, j):
        return parts.at[lax.rem(p, ring), :, pl.ds(j * wz, wz)]

    def stage_out(p, act):
        kind = lax.rem(p, 3)
        sl = lax.rem(p, 2)

        @pl.when(kind < 2)
        def _():
            act(pltpu.make_async_copy(stage.at[sl], ggu_hbm.at[kind, rows_of(p)], stage_sems.at[sl]))

        @pl.when(kind == 2)
        def _():
            act(pltpu.make_async_copy(stage.at[sl], gd_hbm.at[rows_of(p)], stage_sems.at[sl]))

    def finish(p):
        @pl.when(p >= 2)
        def _():
            stage_out(p - 2, lambda c: c.wait())
        sl = lax.rem(p, 2)
        mine = parts.at[lax.rem(p, ring), :, pl.ds(pl.multiple_of(f * wz, wz), wz)]
        stage[sl] = mine[...].astype(f32)

        @pl.when(f > 0)
        def _():
            stage[sl] += from_left[p, jnp.maximum(f - 1, 0)].astype(f32)

        @pl.when(f < n - 1)
        def _():
            stage[sl] += from_right[p, jnp.minimum(f, n - 2)].astype(f32)
        stage_out(p, lambda c: c.start())

    reduce = LineReduce(f, n, count, block, from_left, from_right, (rs_sr, rs_rr, rs_sl, rs_rl), finish)

    acc_o[...] = jnp.zeros_like(acc_o)
    acc_g[...] = jnp.zeros_like(acc_g)

    first = 3 + n - 1

    @pl.loop(0, first)
    def _(t):
        gather.tick(t)

    for c in loads:
        c.wait()

    def compute(c):
        for k in range(3):
            own_copy(3 * c + k, lambda cc: cc.wait())

        @pl.loop(0, tokens // rb)
        def _(i):
            rows = pl.ds(pl.multiple_of(i * rb, rb), rb)
            a = in2[rows, :]
            gate = dot_nt(a, w[3 * c])
            up = dot_nt(a, w[3 * c + 1])
            gh = dot_nt(cot[rows, :], w[3 * c + 2])
            sig = jax.nn.sigmoid(gate)
            silu = gate * sig
            h = (silu * up).astype(bf16)
            dg = (gh * up * sig * (1.0 + gate * (1.0 - sig))).astype(bf16)
            du = (gh * silu).astype(bf16)
            hid[rows, :] = h
            dga[rows, :] = dg
            dup[rows, :] = du
            acc_o[rows, :] = (acc_o[rows, :].astype(f32) + dot_nn(h, w[3 * c + 2])).astype(acc_o.dtype)
            acc_g[rows, :] = (acc_g[rows, :].astype(f32) + dot_nn(dg, w[3 * c]) + dot_nn(du, w[3 * c + 1])).astype(acc_g.dtype)

        for k, (small, big) in enumerate(((dga, in2), (dup, in2), (hid, cot))):
            for j in range(n):
                block(3 * c + k, j)[...] = dot_tn(small[...], big[:, pl.ds(j * wz, wz)]).astype(bf16)

    @pl.loop(0, nc)
    def _(c):
        compute(c)

        @pl.loop(0, 3)
        def _(k):
            gather.tick(3 * c + k + first)
            reduce.tick(3 * c + k)

    in2[...] = acc_o[...].astype(bf16)
    cot[...] = acc_g[...].astype(bf16)
    stores = [pltpu.make_async_copy(in2, out_hbm, load_sems.at[0]),
              pltpu.make_async_copy(cot, gin_hbm, load_sems.at[1])]
    for c in stores:
        c.start()

    @pl.loop(0, n - 1)
    def _(k):
        reduce.tick(count + k)

    @pl.loop(0, count)
    def _(p):
        gather.drain(p)
    for p in (count - 2, count - 1):
        stage_out(jnp.int32(p), lambda c: c.wait())
    for c in stores:
        c.wait()


def piece_rows(ff):
    r = 0
    for cand in range(16, 257, 16):
        if ff % cand == 0:
            r = cand
    return r


def mlp(in2, cot, wgu, wd, n, cid):
    tokens, width = in2.shape
    ff, wz = wd.shape
    r = piece_rows(ff)
    rb = min(256, tokens)
    nc = ff // r
    count = 3 * nc
    ring = min(count, 3 * ((n - 1 + 2) // 3) + 3)
    any_spec = pl.BlockSpec(memory_space=pl.ANY)
    acc_dtype = f32 if tokens * width * 8 <= 20 * 2**20 else bf16
    D = pltpu.SemaphoreType.DMA
    return pl.pallas_call(
        functools.partial(mlp_kernel, n, r, rb),
        out_shape=(
            jax.ShapeDtypeStruct((tokens, width), bf16),
            jax.ShapeDtypeStruct((tokens, width), bf16),
            jax.ShapeDtypeStruct((2, ff, wz), f32),
            jax.ShapeDtypeStruct((ff, wz), f32),
        ),
        in_specs=[any_spec] * 4,
        out_specs=[any_spec] * 4,
        scratch_shapes=[
            pltpu.VMEM((tokens, width), bf16),
            pltpu.VMEM((tokens, width), bf16),
            pltpu.VMEM((tokens, width), acc_dtype),
            pltpu.VMEM((tokens, width), acc_dtype),
            pltpu.VMEM((count, r, width), bf16),
            pltpu.VMEM((tokens, r), bf16),
            pltpu.VMEM((tokens, r), bf16),
            pltpu.VMEM((tokens, r), bf16),
            pltpu.VMEM((ring, r, width), bf16),
            pltpu.VMEM((count, n - 1, r, wz), bf16),
            pltpu.VMEM((count, n - 1, r, wz), bf16),
            pltpu.VMEM((2, r, wz), f32),
            D((2,)),
            D((count,)),
        ] + [D((count, n - 1))] * 8 + [D((2,))],
        compiler_params=pltpu.CompilerParams(
            collective_id=cid, has_side_effects=True, vmem_limit_bytes=64 * 1024 * 1024 - 65536),
        name="mlp",
    )(in2, cot, wgu, wd)


LANES = 128
PER = LANES // HEAD_DIM


def xor(a, b, count):
    total = 0
    bit = 1
    while bit < count:
        x, y = (a // bit) % 2, (b // bit) % 2
        total = total + bit * (x + y - 2 * x * y)
        bit *= 2
    return total


def everyone_barrier(me, nf, ns):
    barrier = pltpu.get_barrier_semaphore()
    total = nf * ns

    @pl.loop(1, total)
    def _(k):
        t = lax.rem(me + k, total)
        pl.semaphore_signal(barrier, inc=1, device_id={"fsdp": t // ns, "seq": lax.rem(t, ns)},
                            device_id_type=MESH)
    pl.semaphore_wait(barrier, total - 1)


class RowGather:
    def __init__(self, s, m, tok, buf, sems):
        self.j, self.c, self.m, self.tok, self.buf = s // 2, s % 2, m, tok, buf
        self.send_o, self.recv_o, self.send_s, self.recv_s = sems

    def slot(self, chip, core):
        row = (chip * 2 + core) * self.tok
        return self.buf.at[pl.ds(pl.multiple_of(row, self.tok), self.tok)]

    def off(self, src, d, chip):
        return remote(src, self.slot(chip, self.c), self.send_o.at[d], self.recv_o.at[d],
                      {"seq": xor(self.j, d, self.m) * 2 + self.c})

    def sib(self, src, d, core):
        return remote(src, self.slot(xor(self.j, d, self.m), core), self.send_s.at[d], self.recv_s.at[d],
                      {"seq": self.j * 2 + 1 - self.c})

    def start(self, src):
        for d in range(1, self.m):
            self.off(src, d, self.j).start()
        self.sib(src, 0, self.c).start()

    def relay(self, d):
        chip = xor(self.j, d, self.m)
        here = self.slot(chip, self.c)
        self.off(here, d, chip).wait_recv()
        self.sib(here, d, self.c).start()

    def finish(self):
        for d in range(self.m):
            self.sib(self.slot(xor(self.j, d, self.m), 1 - self.c), d, 1 - self.c).wait_recv()

    def drain(self, src):
        for d in range(1, self.m):
            self.off(src, d, self.j).wait_send()
            chip = xor(self.j, d, self.m)
            self.sib(self.slot(chip, self.c), d, self.c).wait_send()
        self.sib(src, 0, self.c).wait_send()


class RowReduce:
    def __init__(self, s, m, from_sib, from_off, sems):
        self.j, self.c, self.m = s // 2, s % 2, m
        self.from_sib, self.from_off = from_sib, from_off
        self.send_s, self.recv_s, self.send_o, self.recv_o = sems

    def sib(self, src, d):
        return remote(src, self.from_sib.at[d], self.send_s.at[d], self.recv_s.at[d],
                      {"seq": self.j * 2 + 1 - self.c})

    def off(self, d):
        return remote(self.from_sib.at[d], self.from_off.at[d - 1], self.send_o.at[d], self.recv_o.at[d],
                      {"seq": xor(self.j, d, self.m) * 2 + self.c})

    def give(self, d, src):
        self.sib(src, d).start()

    def pass_on(self, d, own):
        here = self.from_sib.at[d]
        self.sib(here, d).wait_recv()
        here[...] = (own.astype(f32) + here[...].astype(f32)).astype(bf16)
        self.off(d).start()

    def total(self, own):
        here = self.from_sib.at[0]
        self.sib(here, 0).wait_recv()
        value = own.astype(f32) + here[...].astype(f32)
        for d in range(self.m - 1, 0, -1):
            self.off(d).wait_recv()
            value = value + self.from_off[d - 1].astype(f32)
        return value

    def drain(self, src_of):
        for d in range(self.m):
            self.sib(src_of(d), d).wait_send()
        for d in range(1, self.m):
            self.off(d).wait_send()


def normed_rows(x):
    center = x - jnp.mean(x, axis=-1, keepdims=True)
    inverse = lax.rsqrt(jnp.mean(center * center, axis=-1, keepdims=True) + epsilon)
    return center * inverse, inverse


def lane_of(shape):
    return lax.broadcasted_iota(jnp.int32, shape, len(shape) - 1)


def rotary_tiles(rows, first):
    half = ROTARY // 2
    lane = lane_of((rows, LANES))
    pos = (first + lax.broadcasted_iota(jnp.int32, (rows, LANES), 0)).astype(f32)
    within = lane % HEAD_DIM
    freq = jnp.zeros((rows, LANES), f32)
    for i in range(half):
        freq = jnp.where(within % half == i, float(10000.0 ** (-2.0 * i / ROTARY)), freq)
    angle = pos * freq
    turned = within < ROTARY
    cosine = jnp.where(turned, jnp.cos(angle), 1.0)
    sine = jnp.where(turned, jnp.sin(angle), 0.0)
    return cosine, sine


def turn(u, cosine, sine, direction):
    half = ROTARY // 2
    within = lane_of(u.shape) % HEAD_DIM
    ahead = pltpu.roll(u, LANES - half, 1)
    behind = pltpu.roll(u, half, 1)
    turned = jnp.where(within < half, -ahead, behind)
    return u * cosine + direction * turned * sine


def front_kernel(nf, ns,
                 x_hbm, cot_hbm, g1, b1, g2, b2, qb, wqkv_hbm, wo_hbm,
                 in1_hbm, cotall_hbm, in2_hbm, qkv_hbm, att_hbm, lse_hbm, res_hbm, wq_hbm, woall_hbm,
                 vec_hbm, cos_hbm, sin_hbm,
                 x, in1, tile, tiles, vecs, wq, wo, qkv, att, lse, cos, sin, part, keep, give,
                 from_sib, from_off, res, in2,
                 load_sems, own_sems, small_s, small_r,
                 ag_sr, ag_rr, ag_sl, ag_rl,
                 a_so, a_ro, a_ss, a_rs, c_so, c_ro, c_ss, c_rs, e_so, e_ro, e_ss, e_rs,
                 r_ss, r_rs, r_so, r_ro, out_sems):
    f, s = lax.axis_index("fsdp"), lax.axis_index("seq")
    total = nf * ns
    me = f * ns + s
    m = ns // 2
    j, c = s // 2, s % 2
    tok, width = x.shape
    length = in1.shape[0]
    cols = qkv.shape[2]
    wz = width // nf
    pairs = cols // LANES
    block_rows = 2 * tok
    load = pltpu.make_async_copy(x_hbm, x, load_sems.at[0])
    load.start()

    def own(p, use):
        use(wqkv_hbm.at[p] if p < 3 else wo_hbm)

    def slot(p, source):
        if p < 3:
            return wq.at[p, pl.ds(pl.multiple_of(source * wz, wz), wz)]
        return wo.at[:, pl.ds(pl.multiple_of(source * wz, wz), wz)]

    def own_copy(p):
        box = []
        own(p, lambda src: box.append(pltpu.make_async_copy(src, slot(p, f), own_sems.at[p])))
        return box[0]

    for p in range(4):
        own_copy(p).start()
    cot_rows = pl.ds(pl.multiple_of(s * tok, tok), tok)
    cot_own = pltpu.make_async_copy(cot_hbm, cotall_hbm.at[cot_rows], load_sems.at[1])

    w = g1.shape[1]
    spread = LANES // w
    here = lane_of((1, LANES)) // w == lax.rem(me, spread)
    tile[...] = jnp.zeros_like(tile)
    for row, piece in enumerate((g1[...], b1[...], g2[...], b2[...], qb[0:1, :], qb[1:2, :], qb[2:3, :])):
        wide = jnp.concatenate([piece.astype(f32)] * spread, axis=1)
        tile[row:row + 1, :] = jnp.where(here, wide, 0.0)

    everyone_barrier(me, nf, ns)
    gather = LineGather(f, nf, 4, own, slot, (ag_sr, ag_rr, ag_sl, ag_rl))
    gather.tick(0)

    def small(k):
        t = lax.rem(me + k, total)
        return remote(tile, tiles.at[k], small_s.at[k], small_r.at[k], {"fsdp": t // ns, "seq": lax.rem(t, ns)})

    @pl.loop(1, total)
    def _(k):
        small(k).start()
    cot_own.start()
    tiles[0] = tile[...]
    for q in range(length // block_rows):
        rows = pl.ds(q * block_rows, block_rows)
        cos[rows, :], sin[rows, :] = rotary_tiles(block_rows, q * block_rows)
    stores = [pltpu.make_async_copy(cos, cos_hbm, out_sems.at[0]), pltpu.make_async_copy(sin, sin_hbm, out_sems.at[1])]
    for st in stores:
        st.start()

    @pl.loop(1, total)
    def _(k):
        small(k).wait_recv()
    vecs[...] = jnp.zeros_like(vecs)

    @pl.loop(0, total)
    def _(k):
        source = lax.rem(me + total - k, total)
        lanes = pl.ds(pl.multiple_of(source // spread * LANES, LANES), LANES)
        vecs[:, lanes] += tiles[k]

    def store(ref, hbm, i):
        st = pltpu.make_async_copy(ref, hbm, out_sems.at[i])
        st.start()
        stores.append(st)

    store(vecs, vec_hbm, 2)
    load.wait()
    normed, _ = normed_rows(x[...].astype(f32))
    mine = pl.ds(pl.multiple_of(s * tok, tok), tok)
    in1[mine, :] = (normed * vecs[0:1, :] + vecs[1:2, :]).astype(bf16)
    rows_in = RowGather(s, m, tok, in1, (a_so, a_ro, a_ss, a_rs))
    rows_in.start(in1.at[mine])
    rows_cot = RowGather(s, m, tok, cotall_hbm, (c_so, c_ro, c_ss, c_rs))
    rows_cot.start(cot_hbm)
    gather.tick(1)
    for d in range(1, m):
        rows_in.relay(d)
        if d == 2:
            gather.tick(2)
    if m <= 2:
        gather.tick(2)
    rows_in.finish()
    store(in1, in1_hbm, 3)
    bias_at = pl.ds(pl.multiple_of(s * cols, LANES), cols)

    def project(k):
        own_copy(k).wait()

        @pl.loop(0, length // block_rows)
        def _(q):
            rows = pl.ds(pl.multiple_of(q * block_rows, block_rows), block_rows)
            value = dot_nn(in1[rows, :], wq[k]) + vecs[4 + k:5 + k, bias_at]
            for g in range(pairs):
                lanes = slice(g * LANES, (g + 1) * LANES)
                u = value[:, lanes]
                if k < 2:
                    u = turn(u, cos[rows, :], sin[rows, :], 1.0)
                qkv[k, rows, lanes] = u.astype(bf16)

    relays = list(range(1, m))
    last = 2
    for k in range(3):
        while last < k + nf - 1:
            last += 1
            gather.tick(last)
        project(k)
        if relays:
            rows_cot.relay(relays.pop(0))
    while last < 3 + nf - 1:
        last += 1
        gather.tick(last)
    own_copy(3).wait()
    while relays:
        rows_cot.relay(relays.pop(0))
    store(qkv, qkv_hbm, 4)
    store(wq, wq_hbm, 5)
    store(wo, woall_hbm, 6)

    def attend(b):
        rows = pl.ds(b * block_rows, block_rows)

        @pl.loop(0, pairs)
        def _(g):
            lanes = pl.ds(pl.multiple_of(g * LANES, LANES), LANES)
            q, kd, vd = qkv[0, rows, lanes], qkv[1, rows, lanes], qkv[2, rows, lanes]
            lane = lane_of((block_rows, LANES))
            seen = lane_of((block_rows, block_rows)) <= lax.broadcasted_iota(jnp.int32, (block_rows, block_rows), 0)
            out = jnp.zeros((block_rows, LANES), f32)
            logs = lse[rows, :]
            for h in range(PER):
                head = lane // HEAD_DIM == h
                qm = jnp.where(head, q.astype(f32) * HEAD_DIM ** -0.5, 0.0).astype(bf16)
                sd = jnp.where(seen, dot_nt(qm, kd), masked_score)
                top = jnp.max(sd, axis=1, keepdims=True)
                if b > 0:
                    before = pl.ds(0, b * block_rows)
                    sl = dot_nt(qm, qkv[1, before, lanes])
                    top = jnp.maximum(top, jnp.max(sl, axis=1, keepdims=True))
                ed = jnp.exp(sd - top)
                tot = jnp.sum(ed, axis=1, keepdims=True)
                if b > 0:
                    el = jnp.exp(sl - top)
                    tot = tot + jnp.sum(el, axis=1, keepdims=True)
                inv = 1.0 / tot
                value = dot_nn((ed * inv).astype(bf16), vd)
                if b > 0:
                    value = value + dot_nn((el * inv).astype(bf16), qkv[2, before, lanes])
                out = jnp.where(head, value, out)
                logs = jnp.where(lane == g * PER + h, top + jnp.log(tot), logs)
            att[rows, lanes] = out.astype(bf16)
            lse[rows, :] = logs

    lse[...] = jnp.zeros_like(lse)
    sums = RowReduce(s, m, from_sib, from_off, (r_ss, r_rs, r_so, r_ro))

    @pl.loop(0, m)
    def _(step):
        d = m - 1 - step
        chip = xor(j, d, m)
        for b in range(m):
            @pl.when(chip == b)
            def _(b=b):
                attend(b)
        rows = pl.ds(pl.multiple_of(chip * block_rows, block_rows), block_rows)
        part[...] = dot_nn(att[rows, :], wo[...])
        give[d] = part[pl.ds(pl.multiple_of((1 - c) * tok, tok), tok), :].astype(bf16)
        keep[d] = part[pl.ds(pl.multiple_of(c * tok, tok), tok), :]
        sums.give(d, give.at[d])

        @pl.when(step > 0)
        def _():
            sums.pass_on(d + 1, keep[d + 1])
    store(att, att_hbm, 7)
    store(lse, lse_hbm, 8)
    rows_cot.finish()
    res[...] = x[...].astype(f32) + sums.total(keep[0])
    store(res, res_hbm, 9)
    normed, _ = normed_rows(res[...])
    in2[...] = (normed * vecs[2:3, :] + vecs[3:4, :]).astype(bf16)
    rows_two = RowGather(s, m, tok, in2_hbm, (e_so, e_ro, e_ss, e_rs))
    rows_two.start(in2)
    in2_own = pltpu.make_async_copy(in2, in2_hbm.at[mine], load_sems.at[2])
    in2_own.start()
    for d in range(1, m):
        rows_two.relay(d)
    rows_two.finish()

    @pl.loop(1, total)
    def _(k):
        small(k).wait_send()
    for p in range(4):
        gather.drain(p)
    rows_in.drain(in1.at[mine])
    rows_cot.drain(cot_hbm)
    rows_two.drain(in2)
    sums.drain(lambda d: give.at[d])
    cot_own.wait()
    in2_own.wait()
    for st in stores:
        st.wait()


def front(x, cot, g1, b1, g2, b2, qb, wqkv, wo, nf, ns, cid):
    tok, width = x.shape
    cols, wz = wo.shape
    length = tok * ns
    m = ns // 2
    w = g1.shape[1]
    D, V = pltpu.SemaphoreType.DMA, pltpu.VMEM
    A = pl.BlockSpec(memory_space=pl.ANY)
    M = pl.BlockSpec(memory_space=pltpu.VMEM)
    S = jax.ShapeDtypeStruct
    return pl.pallas_call(
        functools.partial(front_kernel, nf, ns),
        out_shape=(
            S((length, width), bf16), S((length, width), bf16), S((length, width), bf16),
            S((3, length, cols), bf16), S((length, cols), bf16), S((length, LANES), f32),
            S((tok, width), f32), S((3, width, cols), bf16), S((cols, width), bf16),
            S((8, width), f32), S((length, LANES), f32), S((length, LANES), f32),
        ),
        in_specs=[A, A, M, M, M, M, M, A, A],
        out_specs=[A] * 12,
        scratch_shapes=[
            V((tok, width), bf16), V((length, width), bf16), V((8, LANES), f32), V((nf * ns, 8, LANES), f32),
            V((8, width), f32), V((3, width, cols), bf16), V((cols, width), bf16), V((3, length, cols), bf16),
            V((length, cols), bf16), V((length, LANES), f32), V((length, LANES), f32), V((length, LANES), f32),
            V((2 * tok, width), f32), V((m, tok, width), f32), V((m, tok, width), bf16),
            V((m, tok, width), bf16), V((m - 1, tok, width), bf16), V((tok, width), f32), V((tok, width), bf16),
            D((3,)), D((4,)), D((nf * ns,)), D((nf * ns,)),
        ] + [D((4, nf - 1))] * 4 + [D((m,))] * 16 + [D((10,))],
        compiler_params=pltpu.CompilerParams(
            collective_id=cid, has_side_effects=True, vmem_limit_bytes=64 * 1024 * 1024 - 65536),
        name="front",
    )(x, cot, g1, b1, g2, b2, qb, wqkv, wo)


def back_kernel(nf, ns,
                gsum_hbm, osum_hbm, res_hbm, cot_hbm, x_hbm, vec_hbm, qkv_hbm, att_hbm, lse_hbm, in1_hbm, wq_hbm, wo_hbm,
                cos_hbm, sin_hbm,
                out_hbm, ig_hbm, gqkv_hbm, gout_hbm, o_g1, o_b1, o_g2, o_b2, o_qb,
                gkeep, okeep, res, cot, vec, qkv, att, lse, in1, wq, wo, cos, sin,
                grows, ga, gq, dk, dv, parts, from_left, from_right, stage, stage_t,
                g_sib, g_off, o_sib, o_off, i_sib, i_off, part, gres, sums, tiles,
                load_sems, keep_sems, in1_sems, small_s, small_r,
                rs_sr, rs_rr, rs_sl, rs_rl,
                w_so, w_ro, w_ss, w_rs,
                g_ss, g_rs, g_so, g_ro, o_ss, o_rs, o_so, o_ro, i_ss, i_rs, i_so, i_ro,
                stage_sems, out_sems):
    f, s = lax.axis_index("fsdp"), lax.axis_index("seq")
    total = nf * ns
    me = f * ns + s
    m = ns // 2
    j, c = s // 2, s % 2
    tok, width = cot.shape
    length, cols = att.shape
    wz = width // nf
    pairs = cols // LANES
    block_rows = 2 * tok
    count = 4 * pairs
    span = 768 if length <= 1024 else 256
    mine = pl.ds(pl.multiple_of(s * tok, tok), tok)

    def rows_at(ref, chip, core):
        return ref.at[pl.ds(pl.multiple_of((chip * 2 + core) * tok, tok), tok)]

    keeps = []
    for d in range(m - 1, -1, -1):
        for i, (hbm, ref) in enumerate(((gsum_hbm, gkeep), (osum_hbm, okeep))):
            keeps.append(pltpu.make_async_copy(rows_at(hbm, xor(j, d, m), c), ref.at[d], keep_sems.at[2 * d + i]))
            keeps[-1].start()
    plain = [(res_hbm, res), (cot_hbm, cot), (vec_hbm, vec), (wo_hbm, wo), (att_hbm, att), (qkv_hbm, qkv),
             (lse_hbm, lse), (wq_hbm, wq), (cos_hbm, cos), (sin_hbm, sin)]
    loads = [pltpu.make_async_copy(a, b, load_sems.at[i]) for i, (a, b) in enumerate(plain)]
    for load in loads:
        load.start()

    def in1_load(k):
        return pltpu.make_async_copy(in1_hbm.at[:, pl.ds(k * wz, wz)], in1.at[k % 2], in1_sems.at[k % 2])
    in1_load(0).start()

    everyone_barrier(me, nf, ns)
    two = RowReduce(s, m, g_sib, g_off, (g_ss, g_rs, g_so, g_ro))
    out = RowReduce(s, m, o_sib, o_off, (o_ss, o_rs, o_so, o_ro))

    def two_src(d):
        return rows_at(gsum_hbm, xor(j, d, m), 1 - c)

    def out_src(d):
        return rows_at(osum_hbm, xor(j, d, m), 1 - c)

    for d in range(m - 1, -1, -1):
        two.give(d, two_src(d))
    for d in range(m - 1, -1, -1):
        out.give(d, out_src(d))
    for keep in keeps:
        keep.wait()
    for d in range(m - 1, 0, -1):
        two.pass_on(d, gkeep[d])
    for load in loads[:3]:
        load.wait()
    sums[...] = jnp.zeros_like(sums)
    normed, inverse = normed_rows(res[...])
    grad = two.total(gkeep[0])
    sums[2:3, :] = jnp.sum(grad * normed, axis=0, keepdims=True)
    sums[3:4, :] = jnp.sum(grad, axis=0, keepdims=True)

    def norm_grad(grad, normed, inverse, gain):
        scaled = grad * gain
        return inverse * (scaled - jnp.mean(scaled, axis=-1, keepdims=True)
                          - normed * jnp.mean(scaled * normed, axis=-1, keepdims=True))

    gres[...] = cot[...].astype(f32) + norm_grad(grad, normed, inverse, vec[2:3, :])
    grows[mine, :] = gres[...].astype(bf16)
    x_load = pltpu.make_async_copy(x_hbm, cot, load_sems.at[len(plain)])
    x_load.start()
    rows_w = RowGather(s, m, tok, grows, (w_so, w_ro, w_ss, w_rs))
    rows_w.start(grows.at[mine])
    for d in range(m - 1, 0, -1):
        out.pass_on(d, okeep[d])
    for d in range(1, m):
        rows_w.relay(d)
    rows_w.finish()
    for load in loads[3:]:
        load.wait()

    def block(p, k):
        return parts.at[p, :, pl.ds(k * wz, wz)]

    def staged(p, act):
        sl = lax.rem(p, 2)

        @pl.when(p < pairs)
        def _():
            act(pltpu.make_async_copy(
                stage.at[sl], gout_hbm.at[pl.ds(pl.multiple_of(p * LANES, LANES), LANES)], stage_sems.at[sl]))

        @pl.when(p >= pairs)
        def _():
            q = p - pairs
            lanes = pl.ds(pl.multiple_of(q // 3 * LANES, LANES), LANES)
            act(pltpu.make_async_copy(stage_t.at[sl], gqkv_hbm.at[lax.rem(q, 3), :, lanes], stage_sems.at[sl]))

    def finish(p):
        @pl.when(p >= 2)
        def _():
            staged(p - 2, lambda cc: cc.wait())
        sl = lax.rem(p, 2)
        stage[sl] = parts[p, :, pl.ds(pl.multiple_of(f * wz, wz), wz)].astype(f32)

        @pl.when(f > 0)
        def _():
            stage[sl] += from_left[p, jnp.maximum(f - 1, 0)].astype(f32)

        @pl.when(f < nf - 1)
        def _():
            stage[sl] += from_right[p, jnp.minimum(f, nf - 2)].astype(f32)

        @pl.when(p >= pairs)
        def _():
            stage_t[sl] = stage[sl].T
        staged(p, lambda cc: cc.start())

    reduce = LineReduce(f, nf, count, block, from_left, from_right, (rs_sr, rs_rr, rs_sl, rs_rl), finish)

    for k in range(nf):
        lanes = slice(k * wz, (k + 1) * wz)
        value = dot_tn(att[...], grows[:, lanes]).astype(bf16)
        for g in range(pairs):
            parts[g, :, lanes] = value[g * LANES:(g + 1) * LANES, :]
    for p in range(pairs):
        reduce.tick(jnp.int32(p))

    @pl.loop(0, m)
    def _(b):
        rows = pl.ds(pl.multiple_of(b * block_rows, block_rows), block_rows)
        ga[rows, :] = dot_nt(grows[rows, :], wo[...]).astype(bf16)

    @pl.loop(0, pairs)
    def _(g):
        lanes = pl.ds(pl.multiple_of(g * LANES, LANES), LANES)
        dk[...] = jnp.zeros_like(dk)
        dv[...] = jnp.zeros_like(dv)
        lane = lane_of((block_rows, LANES))
        seen = lane_of((block_rows, block_rows)) <= lax.broadcasted_iota(jnp.int32, (block_rows, block_rows), 0)
        for b in range(m):
            rows = pl.ds(b * block_rows, block_rows)
            q = qkv[0, rows, lanes].astype(f32) * HEAD_DIM ** -0.5
            go = ga[rows, lanes].astype(f32)
            both = go * att[rows, lanes].astype(f32)
            logs = lse[rows, :]
            grad_q = jnp.zeros((block_rows, LANES), f32)
            for h in range(PER):
                head = lane // HEAD_DIM == h
                qm = jnp.where(head, q, 0.0).astype(bf16)
                gm = jnp.where(head, go, 0.0).astype(bf16)
                delta = jnp.sum(jnp.where(head, both, 0.0), axis=1, keepdims=True)
                log = jnp.sum(jnp.where(lane == g * PER + h, logs, 0.0), axis=1, keepdims=True)
                acc = jnp.zeros((block_rows, LANES), f32)
                spans = [(k, min(span, b * block_rows - k)) for k in range(0, b * block_rows, span)]
                for first, size in spans + [(b * block_rows, block_rows)]:
                    at = pl.ds(first, size)
                    key, val = qkv[1, at, lanes], qkv[2, at, lanes]
                    pr = jnp.exp(dot_nt(qm, key) - log)
                    if first == b * block_rows:
                        pr = jnp.where(seen, pr, 0.0)
                    gp = dot_nt(gm, val)
                    gs = (pr * (gp - delta)).astype(bf16)
                    dv[at, :] += dot_tn(pr.astype(bf16), gm)
                    dk[at, :] += dot_tn(gs, qm)
                    acc = acc + dot_nn(gs, key)
                grad_q = jnp.where(head, acc * HEAD_DIM ** -0.5, grad_q)
            gq[0, rows, lanes] = turn(grad_q, cos[rows, :], sin[rows, :], -1.0).astype(bf16)
        gq[1, :, lanes] = turn(dk[...], cos[...], sin[...], -1.0).astype(bf16)
        gq[2, :, lanes] = dv[...].astype(bf16)
        three = jnp.concatenate([gq[0, :, lanes], gq[1, :, lanes], gq[2, :, lanes]], axis=1)
        at = pl.ds(pl.multiple_of(s * cols + g * LANES, LANES), LANES)
        for k in range(3):
            sums[4 + k:5 + k, at] = jnp.sum(gq[k, :, lanes].astype(f32), axis=0, keepdims=True)

        @pl.when(g > 0)
        def _():
            for k in range(3):
                reduce.tick(pairs + 3 * (g - 1) + k)
        for k in range(nf):
            in1_load(k).wait()
            in1_load((k + 1) % nf).start()
            value = dot_tn(three, in1[k % 2]).astype(bf16)
            for i in range(3):
                parts[pairs + 3 * g + i, :, k * wz:(k + 1) * wz] = value[i * LANES:(i + 1) * LANES, :]
    in1_load(0).wait()

    okeep[0] = (res[...] + out.total(okeep[0])).astype(bf16)
    stores = [pltpu.make_async_copy(okeep.at[0], out_hbm, out_sems.at[0])]
    stores[0].start()
    out.drain(out_src)
    one = RowReduce(s, m, i_sib, i_off, (i_ss, i_rs, i_so, i_ro))
    late = list(range(pairs + 3 * (pairs - 1), count + nf - 1))
    for d in range(m - 1, -1, -1):
        if late:
            reduce.tick(jnp.int32(late.pop(0)))
        rows = pl.ds(pl.multiple_of(xor(j, d, m) * block_rows, block_rows), block_rows)
        value = dot_nt(gq[0, rows, :], wq[0])
        for k in (1, 2):
            value = value + dot_nt(gq[k, rows, :], wq[k])
        part[...] = value.astype(bf16)
        if d == 0:
            stores.pop().wait()
        okeep[d] = part[pl.ds(pl.multiple_of((1 - c) * tok, tok), tok), :]
        gkeep[d] = part[pl.ds(pl.multiple_of(c * tok, tok), tok), :]
        one.give(d, okeep.at[d])
        if d < m - 1:
            one.pass_on(d + 1, gkeep[d + 1])
    grad = one.total(gkeep[0])
    x_load.wait()
    normed, inverse = normed_rows(cot[...].astype(f32))
    sums[0:1, :] = jnp.sum(grad * normed, axis=0, keepdims=True)
    sums[1:2, :] = jnp.sum(grad, axis=0, keepdims=True)
    res[...] = gres[...] + norm_grad(grad, normed, inverse, vec[0:1, :])
    stores.append(pltpu.make_async_copy(res, ig_hbm, out_sems.at[1]))
    stores[0].start()

    w = o_g1.shape[1]
    spread = LANES // w

    def tile_of(t):
        return sums.at[:, pl.ds(pl.multiple_of(t // spread * LANES, LANES), LANES)]

    def small(k):
        t = lax.rem(me + k, total)
        return remote(tile_of(t), tiles.at[k], small_s.at[k], small_r.at[k],
                      {"fsdp": t // ns, "seq": lax.rem(t, ns)})

    @pl.loop(1, total)
    def _(k):
        small(k).start()
    for t in late:
        reduce.tick(jnp.int32(t))
    tiles[0] = tile_of(me)[...]

    @pl.loop(1, total)
    def _(k):
        small(k).wait_recv()
        tiles[0] += tiles[k]
    for k in range(spread):
        @pl.when(lax.rem(me, spread) == k)
        def _(k=k):
            lanes = slice(k * w, (k + 1) * w)
            for i, ref in enumerate((o_g1, o_b1, o_g2, o_b2)):
                ref[...] = tiles[0, i:i + 1, lanes]
            o_qb[...] = tiles[0, 4:7, lanes]

    @pl.loop(1, total)
    def _(k):
        small(k).wait_send()
    two.drain(two_src)
    one.drain(lambda d: okeep.at[d])
    rows_w.drain(grows.at[mine])
    for p in (count - 2, count - 1):
        staged(jnp.int32(p), lambda cc: cc.wait())
    for st in stores:
        st.wait()


def back(gsum, osum, res, cot, x, vec, qkv, att, lse, in1, wq, wo, cos, sin, nf, ns, cid):
    tok, width = x.shape
    length, cols = att.shape
    wz = width // nf
    m = ns // 2
    w = width // (nf * ns)
    pairs = cols // LANES
    count = 4 * pairs
    D, V = pltpu.SemaphoreType.DMA, pltpu.VMEM
    A = pl.BlockSpec(memory_space=pl.ANY)
    M = pl.BlockSpec(memory_space=pltpu.VMEM)
    S = jax.ShapeDtypeStruct
    rows_v = V((m, tok, width), bf16)
    offs_v = V((m - 1, tok, width), bf16)
    return pl.pallas_call(
        functools.partial(back_kernel, nf, ns),
        out_shape=(
            S((tok, width), bf16), S((tok, width), f32), S((3, wz, cols), f32), S((cols, wz), f32),
            S((1, w), f32), S((1, w), f32), S((1, w), f32), S((1, w), f32), S((3, w), f32),
        ),
        in_specs=[A] * 14,
        out_specs=[A] * 4 + [M] * 5,
        scratch_shapes=[
            rows_v, rows_v, V((tok, width), f32), V((tok, width), bf16), V((8, width), f32),
            V((3, length, cols), bf16), V((length, cols), bf16), V((length, LANES), f32), V((2, length, wz), bf16),
            V((3, width, cols), bf16), V((cols, width), bf16), V((length, LANES), f32), V((length, LANES), f32),
            V((length, width), bf16), V((length, cols), bf16), V((3, length, cols), bf16),
            V((length, LANES), f32), V((length, LANES), f32),
            V((count, LANES, width), bf16), V((count, nf - 1, LANES, wz), bf16), V((count, nf - 1, LANES, wz), bf16),
            V((2, LANES, wz), f32), V((2, wz, LANES), f32),
            rows_v, offs_v, rows_v, offs_v, rows_v, offs_v,
            V((2 * tok, width), bf16), V((tok, width), f32),
            V((8, width), f32), V((nf * ns, 8, LANES), f32),
            D((11,)), D((2 * m,)), D((2,)), D((nf * ns,)), D((nf * ns,)),
        ] + [D((count, nf - 1))] * 4 + [D((m,))] * 16 + [D((2,)), D((2,))],
        compiler_params=pltpu.CompilerParams(
            collective_id=cid, has_side_effects=True, vmem_limit_bytes=64 * 1024 * 1024 - 65536),
        name="back",
    )(gsum, osum, res, cot, x, vec, qkv, att, lse, in1, wq, wo, cos, sin)


def local(
    block_input,
    cotangent,
    ln1_gain,
    ln1_bias,
    qkv_weight,
    qkv_bias,
    out_weight,
    ln2_gain,
    ln2_bias,
    gate_up_weight,
    down_weight,
):
    fsdp, seq = lax.axis_size("fsdp"), lax.axis_size("seq")
    (in_one, cot_all, in_two, qkv, mixed, logs, residual, qkv_full, out_full, vectors, cosine, sine) = front(
        block_input[0],
        cotangent[0],
        ln1_gain[None],
        ln1_bias[None],
        ln2_gain[None],
        ln2_bias[None],
        qkv_bias,
        jnp.transpose(qkv_weight, (1, 0, 2)),
        out_weight,
        fsdp,
        seq,
        1,
    )
    out_sum, grad_sum, grad_gate_up, grad_down = mlp(
        in_two, cot_all, jnp.transpose(gate_up_weight, (1, 2, 0)), down_weight, fsdp, 0
    )
    block_output, input_grad, grad_qkv, grad_out, gain_one, bias_one, gain_two, bias_two, grad_bias = back(
        grad_sum,
        out_sum,
        residual,
        cotangent[0],
        block_input[0],
        vectors,
        qkv,
        mixed,
        logs,
        in_one,
        qkv_full,
        out_full,
        cosine,
        sine,
        fsdp,
        seq,
        2,
    )
    return (
        block_output[None],
        input_grad[None],
        gain_one[0],
        bias_one[0],
        jnp.transpose(grad_qkv, (1, 0, 2)),
        grad_bias,
        grad_out,
        gain_two[0],
        bias_two[0],
        jnp.transpose(grad_gate_up, (2, 0, 1)),
        grad_down,
    )


def solution(mesh):
    placed = (
        P("fsdp", "seq", None),
        P("fsdp", "seq", None),
        P(("fsdp", "seq")),
        P(("fsdp", "seq")),
        P("fsdp", None, "seq"),
        P(None, ("fsdp", "seq")),
        P("seq", "fsdp"),
        P(("fsdp", "seq")),
        P(("fsdp", "seq")),
        P("fsdp", None, "seq"),
        P("seq", "fsdp"),
    )
    return jax.shard_map(
        local,
        mesh=mesh,
        in_specs=placed,
        out_specs=(
            P("fsdp", "seq", None),
            P("fsdp", "seq", None),
            P(("fsdp", "seq")),
            P(("fsdp", "seq")),
            P("fsdp", None, "seq"),
            P(None, ("fsdp", "seq")),
            P("seq", "fsdp"),
            P(("fsdp", "seq")),
            P(("fsdp", "seq")),
            P("fsdp", None, "seq"),
            P("seq", "fsdp"),
        ),
        check_vma=False,
    )
```

```python
import functools

import jax
import jax.numpy as jnp
from jax import lax
from jax.experimental import pallas as pl
from jax.experimental.pallas import tpu as pltpu
from jax.sharding import PartitionSpec as P

HEAD_DIM = 64
ROTARY = 16

epsilon = 1e-05
masked_score = -1e30

MESH = pl.DeviceIdType.MESH
NT = (((1,), (1,)), ((), ()))
TN = (((0,), (0,)), ((), ()))
f32, bf16 = jnp.float32, jnp.bfloat16


def dot_nn(a, b):
    return jnp.dot(a, b, preferred_element_type=f32)


def dot_nt(a, b):
    return lax.dot_general(a, b, NT, preferred_element_type=f32)


def dot_tn(a, b):
    return lax.dot_general(a, b, TN, preferred_element_type=f32)


def remote(src, dst, send_sem, recv_sem, device):
    return pltpu.make_async_remote_copy(
        src_ref=src, dst_ref=dst, send_sem=send_sem, recv_sem=recv_sem,
        device_id=device, device_id_type=MESH)


def line_barrier(f, n):
    barrier = pltpu.get_barrier_semaphore()

    @pl.when(f > 0)
    def _():
        pl.semaphore_signal(barrier, inc=1, device_id={"fsdp": f - 1}, device_id_type=MESH)

    @pl.when(f < n - 1)
    def _():
        pl.semaphore_signal(barrier, inc=1, device_id={"fsdp": f + 1}, device_id_type=MESH)

    pl.semaphore_wait(barrier, (f > 0).astype(jnp.int32) + (f < n - 1).astype(jnp.int32))


def when(condition):
    if isinstance(condition, (bool, int)):
        return (lambda body: body()) if condition else (lambda body: None)
    return pl.when(condition)


class LineGather:
    def __init__(self, f, n, count, own, slot, sems):
        self.f, self.n, self.count, self.own, self.slot = f, n, count, own, slot
        self.send_r, self.recv_r, self.send_l, self.recv_l = sems

    def copy(self, src, p, h, source, rightward):
        f = self.f
        send, recv = (self.send_r, self.recv_r) if rightward else (self.send_l, self.recv_l)
        target = f + 1 if rightward else f - 1
        return remote(src, self.slot(p, source), send.at[p, h], recv.at[p, h], {"fsdp": target})

    def send_own(self, t):
        f, n = self.f, self.n

        @when((t >= 0) & (t < self.count))
        def _():
            @pl.when(f < n - 1)
            def _():
                self.own(t, lambda src: self.copy(src, t, 0, f, True).start())

            @pl.when(f > 0)
            def _():
                self.own(t, lambda src: self.copy(src, t, 0, f, False).start())

    def arrivals(self, t):
        for h in range(1, self.n):
            self.arrive(t - h, h)

    def tick(self, t):
        self.send_own(t)
        self.arrivals(t)

    def arrive(self, p, h):
        f, n = self.f, self.n

        @when((p >= 0) & (p < self.count))
        def _():
            @pl.when(f - h >= 0)
            def _():
                here = self.slot(p, f - h)
                self.copy(here, p, h - 1, f - h, True).wait_recv()
                if h < n - 1:
                    @pl.when(f < n - 1)
                    def _():
                        self.copy(here, p, h, f - h, True).start()

            @pl.when(f + h <= n - 1)
            def _():
                here = self.slot(p, f + h)
                self.copy(here, p, h - 1, f + h, False).wait_recv()
                if h < n - 1:
                    @pl.when(f > 0)
                    def _():
                        self.copy(here, p, h, f + h, False).start()

    def drain(self, p):
        f, n = self.f, self.n
        for h in range(0, n - 1):
            @pl.when((f - h >= 0) & (f < n - 1))
            def _(h=h):
                self.copy(self.slot(p, f - h), p, h, f - h, True).wait_send()

            @pl.when((f + h <= n - 1) & (f > 0))
            def _(h=h):
                self.copy(self.slot(p, f + h), p, h, f + h, False).wait_send()


class LineReduce:
    def __init__(self, f, n, count, block, from_left, from_right, sems, finish):
        self.f, self.n, self.count, self.block = f, n, count, block
        self.from_left, self.from_right, self.finish = from_left, from_right, finish
        self.send_r, self.recv_r, self.send_l, self.recv_l = sems

    def right(self, p, j):
        return remote(self.block(p, j), self.from_left.at[p, j - 1], self.send_r.at[p, j - 1],
                      self.recv_r.at[p, j - 1], {"fsdp": self.f + 1})

    def left(self, p, j):
        return remote(self.block(p, j), self.from_right.at[p, j], self.send_l.at[p, j],
                      self.recv_l.at[p, j], {"fsdp": self.f - 1})

    def tick(self, u):
        f, n, count = self.f, self.n, self.count
        p = u - f

        @pl.when((p >= 0) & (p < count))
        def _():
            for j in range(n - 1, 0, -1):
                @pl.when((f > 0) & (j >= f))
                def _(j=j):
                    self.right(p, j).wait_recv()

                @pl.when((f > 0) & (j > f))
                def _(j=j):
                    here = self.block(p, j)
                    here[...] = (here[...].astype(f32) + self.from_left[p, j - 1].astype(f32)).astype(bf16)

                @pl.when(j > f)
                def _(j=j):
                    self.right(p, j).start()

        q = u - (n - 1 - f)

        @pl.when((q >= 0) & (q < count))
        def _():
            for j in range(0, n - 1):
                @pl.when((f < n - 1) & (j <= f))
                def _(j=j):
                    self.left(q, j).wait_recv()

                @pl.when((f < n - 1) & (j < f))
                def _(j=j):
                    here = self.block(q, j)
                    here[...] = (here[...].astype(f32) + self.from_right[q, j].astype(f32)).astype(bf16)

                @pl.when(j < f)
                def _(j=j):
                    self.left(q, j).start()

        e = u - (n - 1)

        @pl.when((e >= 0) & (e < count))
        def _():
            for j in range(n):
                @pl.when(j > f)
                def _(j=j):
                    self.right(e, j).wait_send()

                @pl.when(j < f)
                def _(j=j):
                    self.left(e, j).wait_send()
            self.finish(e)


def mlp_kernel(n, r, rb, left, in2_hbm, cot_hbm, w0_hbm, wgu_hbm, wd_hbm,
               out_hbm, gin_hbm, ggu_hbm, gd_hbm, *more):
    rest_hbm, more = (more[0], more[1:]) if left else (None, more)
    (in2, cot, acc_o, acc_g, w, hid, dga, dup, parts, from_left, from_right,
               stage, load_sems, own_sems, ag_sr, ag_rr, ag_sl, ag_rl, rs_sr, rs_rr, rs_sl, rs_rl,
               stage_sems, rest_sems) = more
    f = lax.axis_index("fsdp")
    tokens, width = in2.shape
    wz = width // n
    ff = wd_hbm.shape[0]
    nc = ff // r
    count = 3 * nc
    summed = count - 3 * left
    ahead = max(n - 1, 3)
    ring = parts.shape[0]
    loads = [pltpu.make_async_copy(in2_hbm, in2, load_sems.at[0]),
             pltpu.make_async_copy(cot_hbm, cot, load_sems.at[1]),
             pltpu.make_async_copy(w0_hbm, w.at[pl.ds(0, 3)], load_sems.at[2])]
    for c in loads:
        c.start()

    def rows_of(p):
        return pl.ds(pl.multiple_of(p // 3 * r, r), r)

    def own(p, use):
        kind = lax.rem(p, 3)

        @pl.when(kind < 2)
        def _():
            use(wgu_hbm.at[kind, rows_of(p)])

        @pl.when(kind == 2)
        def _():
            use(wd_hbm.at[rows_of(p)])

    def slot(p, source):
        return w.at[p, :, pl.ds(pl.multiple_of(source * wz, wz), wz)]

    def own_copy(p, act):
        own(p, lambda src: act(pltpu.make_async_copy(src, slot(p, f), own_sems.at[p])))

    @pl.loop(3, count)
    def _(p):
        own_copy(p, lambda c: c.start())

    line_barrier(f, n)
    gather = LineGather(f, n, count - 3, lambda p, use: own(p + 3, use), lambda p, source: slot(p + 3, source),
                        (ag_sr, ag_rr, ag_sl, ag_rl))

    def block(p, j):
        return parts.at[lax.rem(p, ring), :, pl.ds(j * wz, wz)]

    def stage_out(p, act):
        kind = lax.rem(p, 3)
        sl = lax.rem(p, 2)

        @pl.when(kind < 2)
        def _():
            act(pltpu.make_async_copy(stage.at[sl], ggu_hbm.at[kind, rows_of(p)], stage_sems.at[sl]))

        @pl.when(kind == 2)
        def _():
            act(pltpu.make_async_copy(stage.at[sl], gd_hbm.at[rows_of(p)], stage_sems.at[sl]))

    def finish(p):
        @pl.when(p >= 2)
        def _():
            stage_out(p - 2, lambda c: c.wait())
        sl = lax.rem(p, 2)
        mine = parts.at[lax.rem(p, ring), :, pl.ds(pl.multiple_of(f * wz, wz), wz)]
        stage[sl] = mine[...].astype(f32)

        @pl.when(f > 0)
        def _():
            stage[sl] += from_left[p, jnp.maximum(f - 1, 0)].astype(f32)

        @pl.when(f < n - 1)
        def _():
            stage[sl] += from_right[p, jnp.minimum(f, n - 2)].astype(f32)
        stage_out(p, lambda c: c.start())

    reduce = LineReduce(f, n, summed, block, from_left, from_right, (rs_sr, rs_rr, rs_sl, rs_rl), finish)

    acc_o[...] = jnp.zeros_like(acc_o)
    acc_g[...] = jnp.zeros_like(acc_g)

    for t in range(3):
        gather.send_own(t)

    for c in loads:
        c.wait()

    def compute(c):
        @pl.when(c > 0)
        def _():
            for k in range(3):
                own_copy(3 * c + k, lambda cc: cc.wait())

        @pl.loop(0, tokens // rb)
        def _(i):
            rows = pl.ds(pl.multiple_of(i * rb, rb), rb)
            a = in2[rows, :]
            gate = dot_nt(a, w[3 * c])
            up = dot_nt(a, w[3 * c + 1])
            gh = dot_nt(cot[rows, :], w[3 * c + 2])
            sig = jax.nn.sigmoid(gate)
            silu = gate * sig
            h = (silu * up).astype(bf16)
            dg = (gh * up * sig * (1.0 + gate * (1.0 - sig))).astype(bf16)
            du = (gh * silu).astype(bf16)
            hid[rows, :] = h
            dga[rows, :] = dg
            dup[rows, :] = du
            acc_o[rows, :] = (acc_o[rows, :].astype(f32) + dot_nn(h, w[3 * c + 2])).astype(acc_o.dtype)
            acc_g[rows, :] = (acc_g[rows, :].astype(f32) + dot_nn(dg, w[3 * c]) + dot_nn(du, w[3 * c + 1])).astype(acc_g.dtype)

        @pl.when(c == 0)
        def _():
            gather.arrivals(1)

        for k, (small, big) in enumerate(((dga, in2), (dup, in2), (hid, cot))):
            for j in range(n):
                block(3 * c + k, j)[...] = dot_tn(small[...], big[:, pl.ds(j * wz, wz)]).astype(bf16)

    @pl.loop(0, nc)
    def _(c):
        compute(c)

        @pl.when(c == 0)
        def _():
            gather.arrivals(2)

        @pl.when(c == 0)
        def _():
            for t in range(3, ahead):
                gather.tick(t)

        @pl.when(c < nc - left)
        def _():
            @pl.loop(0, 3)
            def _(k):
                reduce.tick(3 * c + k)
                gather.tick(3 * c + k + ahead)

    in2[...] = acc_o[...].astype(bf16)
    cot[...] = acc_g[...].astype(bf16)
    stores = [pltpu.make_async_copy(in2, out_hbm, load_sems.at[0]),
              pltpu.make_async_copy(cot, gin_hbm, load_sems.at[1])]
    for k in range(3 * left):
        stores.append(pltpu.make_async_copy(parts.at[(count - 3 + k) % ring], rest_hbm.at[k], rest_sems.at[k]))
    for c in stores:
        c.start()

    @pl.loop(0, n - 1)
    def _(k):
        reduce.tick(summed + k)

    @pl.loop(0, count - 3)
    def _(p):
        gather.drain(p)
    for p in (summed - 2, summed - 1):
        stage_out(jnp.int32(p), lambda c: c.wait())
    for c in stores:
        c.wait()


def piece_rows(ff):
    r = 0
    for cand in range(16, 257, 16):
        if ff % cand == 0:
            r = cand
    return r


def mlp(in2, cot, w0, wgu, wd, n, left, cid):
    tokens, width = in2.shape
    ff, wz = wd.shape
    r = piece_rows(ff)
    rb = min(256, tokens)
    nc = ff // r
    count = 3 * nc
    ring = min(count, 3 * ((n - 1 + 2) // 3) + 3)
    any_spec = pl.BlockSpec(memory_space=pl.ANY)
    acc_dtype = f32 if tokens * width * 8 <= 20 * 2**20 else bf16
    D = pltpu.SemaphoreType.DMA
    return pl.pallas_call(
        functools.partial(mlp_kernel, n, r, rb, left),
        out_shape=(
            jax.ShapeDtypeStruct((tokens, width), bf16),
            jax.ShapeDtypeStruct((tokens, width), bf16),
            jax.ShapeDtypeStruct((2, ff, wz), f32),
            jax.ShapeDtypeStruct((ff, wz), f32),
        ) + (jax.ShapeDtypeStruct((3, r, width), bf16),) * left,
        in_specs=[any_spec] * 5,
        out_specs=[any_spec] * (4 + left),
        scratch_shapes=[
            pltpu.VMEM((tokens, width), bf16),
            pltpu.VMEM((tokens, width), bf16),
            pltpu.VMEM((tokens, width), acc_dtype),
            pltpu.VMEM((tokens, width), acc_dtype),
            pltpu.VMEM((count, r, width), bf16),
            pltpu.VMEM((tokens, r), bf16),
            pltpu.VMEM((tokens, r), bf16),
            pltpu.VMEM((tokens, r), bf16),
            pltpu.VMEM((ring, r, width), bf16),
            pltpu.VMEM((count - 3 * left, n - 1, r, wz), bf16),
            pltpu.VMEM((count - 3 * left, n - 1, r, wz), bf16),
            pltpu.VMEM((2, r, wz), f32),
            D((3,)),
            D((count,)),
        ] + [D((count - 3, n - 1))] * 4 + [D((count - 3 * left, n - 1))] * 4 + [D((2,)), D((3,))],
        compiler_params=pltpu.CompilerParams(
            collective_id=cid, has_side_effects=True, vmem_limit_bytes=64 * 1024 * 1024 - 65536),
        name="mlp",
    )(in2, cot, w0, wgu, wd)


LANES = 128
PER = LANES // HEAD_DIM


def xor(a, b, count):
    total = 0
    bit = 1
    while bit < count:
        x, y = (a // bit) % 2, (b // bit) % 2
        total = total + bit * (x + y - 2 * x * y)
        bit *= 2
    return total


def everyone_barrier(me, nf, ns):
    barrier = pltpu.get_barrier_semaphore()
    total = nf * ns

    @pl.loop(1, total)
    def _(k):
        t = lax.rem(me + k, total)
        pl.semaphore_signal(barrier, inc=1, device_id={"fsdp": t // ns, "seq": lax.rem(t, ns)},
                            device_id_type=MESH)
    pl.semaphore_wait(barrier, total - 1)


class RowGather:
    def __init__(self, s, m, tok, buf, sems):
        self.j, self.c, self.m, self.tok, self.buf = s // 2, s % 2, m, tok, buf
        self.send_o, self.recv_o, self.send_s, self.recv_s = sems
        self.square = m == 4

    def slot(self, chip, core, part=None):
        row = (chip * 2 + core) * self.tok
        if part is None:
            return self.buf.at[pl.ds(pl.multiple_of(row, self.tok), self.tok)]
        half = self.tok // 2
        return self.buf.at[pl.ds(pl.multiple_of(row + part * half, half), half)]

    def off(self, src, d, chip):
        return remote(src, self.slot(chip, self.c), self.send_o.at[d], self.recv_o.at[d],
                      {"seq": xor(self.j, d, self.m) * 2 + self.c})

    def half(self, part, source, to):
        here = self.slot(xor(self.j, source, 4), self.c, part)
        index = 0 if part else 3
        return remote(here, here, self.send_o.at[index], self.recv_o.at[index],
                      {"seq": xor(self.j, to, 4) * 2 + self.c})

    def sib(self, src, d, core):
        return remote(src, self.slot(xor(self.j, d, self.m), core), self.send_s.at[d], self.recv_s.at[d],
                      {"seq": self.j * 2 + 1 - self.c})

    def start(self, src):
        for d in range(1, 3 if self.square else self.m):
            self.off(src, d, self.j).start()
        self.sib(src, 0, self.c).start()

    def relay(self, d):
        chip = xor(self.j, d, self.m)
        here = self.slot(chip, self.c)
        if self.square and d == 3:
            self.half(0, 3, 2).wait_recv()
            self.half(1, 3, 1).wait_recv()
        else:
            self.off(here, d, chip).wait_recv()
            if self.square:
                self.half(d - 1, d, 3 - d).start()
        self.sib(here, d, self.c).start()

    def finish(self):
        for d in range(self.m):
            self.sib(self.slot(xor(self.j, d, self.m), 1 - self.c), d, 1 - self.c).wait_recv()

    def drain(self, src):
        for d in range(1, self.m):
            chip = xor(self.j, d, self.m)
            if not self.square or d < 3:
                self.off(src, d, self.j).wait_send()
                if self.square:
                    self.half(d - 1, d, 3 - d).wait_send()
            self.sib(self.slot(chip, self.c), d, self.c).wait_send()
        self.sib(src, 0, self.c).wait_send()


class RowReduce:
    def __init__(self, s, m, from_sib, from_off, sems):
        self.j, self.c, self.m = s // 2, s % 2, m
        self.from_sib, self.from_off = from_sib, from_off
        self.send_s, self.recv_s, self.send_o, self.recv_o = sems
        self.square = m == 4
        self.tok = from_sib.shape[1]

    def sib(self, src, d):
        return remote(src, self.from_sib.at[d], self.send_s.at[d], self.recv_s.at[d],
                      {"seq": self.j * 2 + 1 - self.c})

    def off(self, d):
        return remote(self.from_sib.at[d], self.from_off.at[d - 1], self.send_o.at[d], self.recv_o.at[d],
                      {"seq": xor(self.j, d, self.m) * 2 + self.c})

    def half(self, d, part):
        at = pl.ds(part * (self.tok // 2), self.tok // 2)
        last = d // 3
        to = d * (1 - last) + (part + 1) * last
        index = 2 * d + part
        return remote(self.from_sib.at[d, at], self.from_off.at[d - 1, at], self.send_o.at[index], self.recv_o.at[index],
                      {"seq": xor(self.j, to, 4) * 2 + self.c})

    def give(self, d, src):
        self.sib(src, d).start()

    def pass_on(self, d, own):
        here = self.from_sib.at[d]
        self.sib(here, d).wait_recv()
        here[...] = (own.astype(f32) + here[...].astype(f32)).astype(bf16)
        if not self.square:
            self.off(d).start()
            return
        for part in range(2):
            @when((d == 3) | (part == d - 1))
            def _(part=part):
                self.half(d, part).start()

    def total(self, own):
        here = self.from_sib.at[0]
        self.sib(here, 0).wait_recv()
        value = own.astype(f32) + here[...].astype(f32)
        if self.square:
            for part, d in ((0, 2), (1, 1)):
                at = pl.ds(part * (self.tok // 2), self.tok // 2)
                self.half(3, part).wait_recv()
                self.from_sib[d, at] = (self.from_sib[d, at].astype(f32) + self.from_off[2, at].astype(f32)).astype(bf16)
                self.half(d, part).start()
            for d in (1, 2):
                self.half(d, 0).wait_recv()
                self.half(d, 1).wait_recv()
                value = value + self.from_off[d - 1].astype(f32)
            return value
        for d in range(self.m - 1, 0, -1):
            self.off(d).wait_recv()
            value = value + self.from_off[d - 1].astype(f32)
        return value

    def drain(self, src_of):
        for d in range(self.m):
            self.sib(src_of(d), d).wait_send()
        for d in range(1, self.m):
            if self.square:
                self.half(d, 0).wait_send()
                self.half(d, 1).wait_send()
            else:
                self.off(d).wait_send()


def normed_rows(x):
    center = x - jnp.mean(x, axis=-1, keepdims=True)
    inverse = lax.rsqrt(jnp.mean(center * center, axis=-1, keepdims=True) + epsilon)
    return center * inverse, inverse


def lane_of(shape):
    return lax.broadcasted_iota(jnp.int32, shape, len(shape) - 1)


def rotary_tiles(rows, first):
    half = ROTARY // 2
    lane = lane_of((rows, LANES))
    pos = (first + lax.broadcasted_iota(jnp.int32, (rows, LANES), 0)).astype(f32)
    within = lane % HEAD_DIM
    freq = jnp.zeros((rows, LANES), f32)
    for i in range(half):
        freq = jnp.where(within % half == i, float(10000.0 ** (-2.0 * i / ROTARY)), freq)
    angle = pos * freq
    turned = within < ROTARY
    cosine = jnp.where(turned, jnp.cos(angle), 1.0)
    sine = jnp.where(turned, jnp.sin(angle), 0.0)
    return cosine, sine


def turn(u, cosine, sine, direction):
    half = ROTARY // 2
    within = lane_of(u.shape) % HEAD_DIM
    ahead = pltpu.roll(u, LANES - half, 1)
    behind = pltpu.roll(u, half, 1)
    turned = jnp.where(within < half, -ahead, behind)
    return u * cosine + direction * turned * sine


def front_kernel(nf, ns,
                 x_hbm, cot_hbm, g1, b1, g2, b2, qb, wqkv_hbm, wo_hbm, wgu_hbm, wd_hbm,
                 in1_hbm, cotall_hbm, in2_hbm, qkv_hbm, att_hbm, lse_hbm, res_hbm, wq_hbm, woall_hbm,
                 vec_hbm, cos_hbm, sin_hbm, w0_hbm,
                 x, in1, tile, tiles, vecs, wq, wo, qkv, att, lse, cos, sin, part, keep, give,
                 from_sib, from_off, res, in2, w0,
                 load_sems, own_sems, small_s, small_r,
                 ag_sr, ag_rr, ag_sl, ag_rl, m_sr, m_rr, m_sl, m_rl,
                 a_so, a_ro, a_ss, a_rs, c_so, c_ro, c_ss, c_rs, e_so, e_ro, e_ss, e_rs,
                 r_ss, r_rs, r_so, r_ro, out_sems):
    f, s = lax.axis_index("fsdp"), lax.axis_index("seq")
    total = nf * ns
    me = f * ns + s
    m = ns // 2
    j, c = s // 2, s % 2
    tok, width = x.shape
    length = in1.shape[0]
    cols = qkv.shape[2]
    wz = width // nf
    pairs = cols // LANES
    block_rows = 2 * tok
    load = pltpu.make_async_copy(x_hbm, x, load_sems.at[0])
    load.start()

    def own(p, use):
        use(wqkv_hbm.at[p] if p < 3 else wo_hbm)

    def slot(p, source):
        if p < 3:
            return wq.at[p, pl.ds(pl.multiple_of(source * wz, wz), wz)]
        return wo.at[:, pl.ds(pl.multiple_of(source * wz, wz), wz)]

    def own_copy(p):
        box = []
        own(p, lambda src: box.append(pltpu.make_async_copy(src, slot(p, f), own_sems.at[p])))
        return box[0]

    for p in range(4):
        own_copy(p).start()

    r = w0.shape[1]

    def mlp_own(p, use):
        @pl.when(p < 2)
        def _():
            use(wgu_hbm.at[p, pl.ds(0, r)])

        @pl.when(p == 2)
        def _():
            use(wd_hbm.at[pl.ds(0, r)])

    def mlp_slot(p, source):
        return w0.at[p, :, pl.ds(pl.multiple_of(source * wz, wz), wz)]

    mlp_copies = [pltpu.make_async_copy(wgu_hbm.at[p, pl.ds(0, r)] if p < 2 else wd_hbm.at[pl.ds(0, r)],
                                        mlp_slot(p, f), own_sems.at[4 + p]) for p in range(3)]
    for copy in mlp_copies:
        copy.start()
    cot_rows = pl.ds(pl.multiple_of(s * tok, tok), tok)
    cot_own = pltpu.make_async_copy(cot_hbm, cotall_hbm.at[cot_rows], load_sems.at[1])

    w = g1.shape[1]
    spread = LANES // w
    here = lane_of((1, LANES)) // w == lax.rem(me, spread)
    tile[...] = jnp.zeros_like(tile)
    for row, piece in enumerate((g1[...], b1[...], g2[...], b2[...], qb[0:1, :], qb[1:2, :], qb[2:3, :])):
        wide = jnp.concatenate([piece.astype(f32)] * spread, axis=1)
        tile[row:row + 1, :] = jnp.where(here, wide, 0.0)

    everyone_barrier(me, nf, ns)
    gather = LineGather(f, nf, 4, own, slot, (ag_sr, ag_rr, ag_sl, ag_rl))
    second = LineGather(f, nf, 3, mlp_own, mlp_slot, (m_sr, m_rr, m_sl, m_rl))
    gather.tick(0)

    def small(k):
        t = lax.rem(me + k, total)
        return remote(tile, tiles.at[k], small_s.at[k], small_r.at[k], {"fsdp": t // ns, "seq": lax.rem(t, ns)})

    @pl.loop(1, total)
    def _(k):
        small(k).start()
    cot_own.start()
    tiles[0] = tile[...]
    for q in range(length // block_rows):
        rows = pl.ds(q * block_rows, block_rows)
        cos[rows, :], sin[rows, :] = rotary_tiles(block_rows, q * block_rows)
    stores = [pltpu.make_async_copy(cos, cos_hbm, out_sems.at[0]), pltpu.make_async_copy(sin, sin_hbm, out_sems.at[1])]
    for st in stores:
        st.start()

    @pl.loop(1, total)
    def _(k):
        small(k).wait_recv()
    vecs[...] = jnp.zeros_like(vecs)

    @pl.loop(0, total)
    def _(k):
        source = lax.rem(me + total - k, total)
        lanes = pl.ds(pl.multiple_of(source // spread * LANES, LANES), LANES)
        vecs[:, lanes] += tiles[k]

    def store(ref, hbm, i):
        st = pltpu.make_async_copy(ref, hbm, out_sems.at[i])
        st.start()
        stores.append(st)

    store(vecs, vec_hbm, 2)
    load.wait()
    normed, _ = normed_rows(x[...].astype(f32))
    mine = pl.ds(pl.multiple_of(s * tok, tok), tok)
    in1[mine, :] = (normed * vecs[0:1, :] + vecs[1:2, :]).astype(bf16)
    rows_in = RowGather(s, m, tok, in1, (a_so, a_ro, a_ss, a_rs))
    rows_in.start(in1.at[mine])
    rows_cot = RowGather(s, m, tok, cotall_hbm, (c_so, c_ro, c_ss, c_rs))
    rows_cot.start(cot_hbm)
    gather.tick(1)
    for d in range(1, m):
        rows_in.relay(d)
        if d == 2:
            gather.tick(2)
    if m <= 2:
        gather.tick(2)
    rows_in.finish()
    store(in1, in1_hbm, 3)
    bias_at = pl.ds(pl.multiple_of(s * cols, LANES), cols)

    def project(k):
        own_copy(k).wait()

        @pl.loop(0, length // block_rows)
        def _(q):
            rows = pl.ds(pl.multiple_of(q * block_rows, block_rows), block_rows)
            value = dot_nn(in1[rows, :], wq[k]) + vecs[4 + k:5 + k, bias_at]
            for g in range(pairs):
                lanes = slice(g * LANES, (g + 1) * LANES)
                u = value[:, lanes]
                if k < 2:
                    u = turn(u, cos[rows, :], sin[rows, :], 1.0)
                qkv[k, rows, lanes] = u.astype(bf16)

    relays = list(range(1, m))
    last = 2
    for k in range(3):
        while last < k + nf - 1:
            last += 1
            gather.tick(last)
        project(k)
        if relays:
            rows_cot.relay(relays.pop(0))
    while last < 3 + nf - 1:
        last += 1
        gather.tick(last)
    own_copy(3).wait()
    second.tick(jnp.int32(0))
    while relays:
        rows_cot.relay(relays.pop(0))
    store(qkv, qkv_hbm, 4)
    store(wq, wq_hbm, 5)
    store(wo, woall_hbm, 6)

    def attend(b):
        rows = pl.ds(b * block_rows, block_rows)

        @pl.loop(0, pairs)
        def _(g):
            lanes = pl.ds(pl.multiple_of(g * LANES, LANES), LANES)
            q, kd, vd = qkv[0, rows, lanes], qkv[1, rows, lanes], qkv[2, rows, lanes]
            lane = lane_of((block_rows, LANES))
            seen = lane_of((block_rows, block_rows)) <= lax.broadcasted_iota(jnp.int32, (block_rows, block_rows), 0)
            out = jnp.zeros((block_rows, LANES), f32)
            logs = lse[rows, :]
            for h in range(PER):
                head = lane // HEAD_DIM == h
                qm = jnp.where(head, q.astype(f32) * HEAD_DIM ** -0.5, 0.0).astype(bf16)
                sd = jnp.where(seen, dot_nt(qm, kd), masked_score)
                top = jnp.max(sd, axis=1, keepdims=True)
                if b > 0:
                    before = pl.ds(0, b * block_rows)
                    sl = dot_nt(qm, qkv[1, before, lanes])
                    top = jnp.maximum(top, jnp.max(sl, axis=1, keepdims=True))
                ed = jnp.exp(sd - top)
                tot = jnp.sum(ed, axis=1, keepdims=True)
                if b > 0:
                    el = jnp.exp(sl - top)
                    tot = tot + jnp.sum(el, axis=1, keepdims=True)
                inv = 1.0 / tot
                value = dot_nn((ed * inv).astype(bf16), vd)
                if b > 0:
                    value = value + dot_nn((el * inv).astype(bf16), qkv[2, before, lanes])
                out = jnp.where(head, value, out)
                logs = jnp.where(lane == g * PER + h, top + jnp.log(tot), logs)
            att[rows, lanes] = out.astype(bf16)
            lse[rows, :] = logs

    lse[...] = jnp.zeros_like(lse)
    sums = RowReduce(s, m, from_sib, from_off, (r_ss, r_rs, r_so, r_ro))

    @pl.loop(0, m)
    def _(step):
        d = m - 1 - step
        chip = xor(j, d, m)
        for b in range(m):
            @pl.when(chip == b)
            def _(b=b):
                attend(b)
        rows = pl.ds(pl.multiple_of(chip * block_rows, block_rows), block_rows)
        part[...] = dot_nn(att[rows, :], wo[...])
        give[d] = part[pl.ds(pl.multiple_of((1 - c) * tok, tok), tok), :].astype(bf16)
        keep[d] = part[pl.ds(pl.multiple_of(c * tok, tok), tok), :]
        sums.give(d, give.at[d])

        @pl.when((step > 0))
        def _():
            sums.pass_on(d + 1, keep[d + 1])

        @pl.when(step % 2 == 1)
        def _():
            second.tick((step + 1) // 2)
    ticks = list(range(m // 2 + 1, 3 + nf - 1))
    store(att, att_hbm, 7)
    store(lse, lse_hbm, 8)
    rows_cot.finish()
    res[...] = x[...].astype(f32) + sums.total(keep[0])
    store(res, res_hbm, 9)
    normed, _ = normed_rows(res[...])
    in2[...] = (normed * vecs[2:3, :] + vecs[3:4, :]).astype(bf16)
    rows_two = RowGather(s, m, tok, in2_hbm, (e_so, e_ro, e_ss, e_rs))
    rows_two.start(in2)
    in2_own = pltpu.make_async_copy(in2, in2_hbm.at[mine], load_sems.at[2])
    in2_own.start()
    if ticks:
        second.tick(jnp.int32(ticks.pop(0)))
    for d in range(1, m):
        rows_two.relay(d)
        if ticks and d < m - 1:
            second.tick(jnp.int32(ticks.pop(0)))
    rows_two.finish()
    for t in ticks:
        second.tick(jnp.int32(t))
    for copy in mlp_copies:
        copy.wait()
    store(w0, w0_hbm, 10)

    @pl.loop(1, total)
    def _(k):
        small(k).wait_send()
    for p in range(4):
        gather.drain(p)
    for p in range(3):
        second.drain(p)
    rows_in.drain(in1.at[mine])
    rows_cot.drain(cot_hbm)
    rows_two.drain(in2)
    sums.drain(lambda d: give.at[d])
    cot_own.wait()
    in2_own.wait()
    for st in stores:
        st.wait()


def front(x, cot, g1, b1, g2, b2, qb, wqkv, wo, wgu, wd, nf, ns, cid):
    r = piece_rows(wd.shape[0])
    tok, width = x.shape
    cols, wz = wo.shape
    length = tok * ns
    m = ns // 2
    w = g1.shape[1]
    D, V = pltpu.SemaphoreType.DMA, pltpu.VMEM
    A = pl.BlockSpec(memory_space=pl.ANY)
    M = pl.BlockSpec(memory_space=pltpu.VMEM)
    S = jax.ShapeDtypeStruct
    return pl.pallas_call(
        functools.partial(front_kernel, nf, ns),
        out_shape=(
            S((length, width), bf16), S((length, width), bf16), S((length, width), bf16),
            S((3, length, cols), bf16), S((length, cols), bf16), S((length, LANES), f32),
            S((tok, width), f32), S((3, width, cols), bf16), S((cols, width), bf16),
            S((8, width), f32), S((length, LANES), f32), S((length, LANES), f32), S((3, r, width), bf16),
        ),
        in_specs=[A, A, M, M, M, M, M, A, A, A, A],
        out_specs=[A] * 13,
        scratch_shapes=[
            V((tok, width), bf16), V((length, width), bf16), V((8, LANES), f32), V((nf * ns, 8, LANES), f32),
            V((8, width), f32), V((3, width, cols), bf16), V((cols, width), bf16), V((3, length, cols), bf16),
            V((length, cols), bf16), V((length, LANES), f32), V((length, LANES), f32), V((length, LANES), f32),
            V((2 * tok, width), f32), V((m, tok, width), f32), V((m, tok, width), bf16),
            V((m, tok, width), bf16), V((m - 1, tok, width), bf16), V((tok, width), f32), V((tok, width), bf16),
            V((3, r, width), bf16),
            D((3,)), D((7,)), D((nf * ns,)), D((nf * ns,)),
        ] + [D((4, nf - 1))] * 4 + [D((3, nf - 1))] * 4 + [D((m,))] * 14 + [D((2 * m,))] * 2 + [D((11,))],
        compiler_params=pltpu.CompilerParams(
            collective_id=cid, has_side_effects=True, vmem_limit_bytes=64 * 1024 * 1024 - 65536),
        name="front",
    )(x, cot, g1, b1, g2, b2, qb, wqkv, wo, wgu, wd)


def back_kernel(nf, ns, left,
                gsum_hbm, osum_hbm, res_hbm, cot_hbm, x_hbm, vec_hbm, qkv_hbm, att_hbm, lse_hbm, in1_hbm, wq_hbm, wo_hbm,
                cos_hbm, sin_hbm, *more):
    if left:
        (rest_hbm, _, _, out_hbm, ig_hbm, gqkv_hbm, gout_hbm, o_g1, o_b1, o_g2, o_b2, o_qb, ggu_hbm, gd_hbm) = more[:14]
        (rest, rest_left, rest_right, rest_stage, rest_sems, q_sr, q_rr, q_sl, q_rl) = more[-9:]
        more = more[14:-9]
    else:
        (out_hbm, ig_hbm, gqkv_hbm, gout_hbm, o_g1, o_b1, o_g2, o_b2, o_qb) = more[:9]
        more = more[9:]
    (gkeep, okeep, res, cot, vec, qkv, att, lse, in1, wq, wo, cos, sin,
                grows, ga, gq, dk, dv, parts, from_left, from_right, stage, stage_t,
                g_sib, g_off, o_sib, o_off, i_sib, i_off, part, gres, sums, tiles,
                load_sems, keep_sems, in1_sems, small_s, small_r,
                rs_sr, rs_rr, rs_sl, rs_rl,
                w_so, w_ro, w_ss, w_rs,
                g_ss, g_rs, g_so, g_ro, o_ss, o_rs, o_so, o_ro, i_ss, i_rs, i_so, i_ro,
     stage_sems, out_sems) = more
    f, s = lax.axis_index("fsdp"), lax.axis_index("seq")
    total = nf * ns
    me = f * ns + s
    m = ns // 2
    j, c = s // 2, s % 2
    tok, width = cot.shape
    length, cols = att.shape
    wz = width // nf
    pairs = cols // LANES
    block_rows = 2 * tok
    count = 4 * pairs
    span = 768 if length <= 1024 else 256
    mine = pl.ds(pl.multiple_of(s * tok, tok), tok)

    def rows_at(ref, chip, core):
        return ref.at[pl.ds(pl.multiple_of((chip * 2 + core) * tok, tok), tok)]

    keeps = []
    for d in range(m - 1, -1, -1):
        for i, (hbm, ref) in enumerate(((gsum_hbm, gkeep), (osum_hbm, okeep))):
            keeps.append(pltpu.make_async_copy(rows_at(hbm, xor(j, d, m), c), ref.at[d], keep_sems.at[2 * d + i]))
            keeps[-1].start()
    plain = [(res_hbm, res), (cot_hbm, cot), (vec_hbm, vec), (wo_hbm, wo), (att_hbm, att), (qkv_hbm, qkv),
             (lse_hbm, lse), (wq_hbm, wq), (cos_hbm, cos), (sin_hbm, sin)]
    loads = [pltpu.make_async_copy(a, b, load_sems.at[i]) for i, (a, b) in enumerate(plain)]
    for load in loads:
        load.start()

    def in1_load(k):
        return pltpu.make_async_copy(in1_hbm.at[:, pl.ds(k * wz, wz)], in1.at[k % 2], in1_sems.at[k % 2])
    in1_load(0).start()
    if left:
        rest_load = pltpu.make_async_copy(rest_hbm, rest, rest_sems.at[0])
        rest_load.start()

    everyone_barrier(me, nf, ns)
    two = RowReduce(s, m, g_sib, g_off, (g_ss, g_rs, g_so, g_ro))
    out = RowReduce(s, m, o_sib, o_off, (o_ss, o_rs, o_so, o_ro))

    waiting = []
    if left:
        r = rest.shape[1]
        last_rows = pl.ds(gd_hbm.shape[0] - r, r)

        def rest_out(p, act):
            @pl.when(p < 2)
            def _():
                act(pltpu.make_async_copy(rest_stage.at[p], ggu_hbm.at[p, last_rows], rest_sems.at[p]))

            @pl.when(p == 2)
            def _():
                act(pltpu.make_async_copy(rest_stage.at[p], gd_hbm.at[last_rows], rest_sems.at[p]))

        def rest_finish(p):
            rest_stage[p] = rest[p, :, pl.ds(pl.multiple_of(f * wz, wz), wz)].astype(f32)

            @pl.when(f > 0)
            def _():
                rest_stage[p] += rest_left[p, jnp.maximum(f - 1, 0)].astype(f32)

            @pl.when(f < nf - 1)
            def _():
                rest_stage[p] += rest_right[p, jnp.minimum(f, nf - 2)].astype(f32)
            rest_out(p, lambda cc: cc.start())

        rest_sum = LineReduce(f, nf, 3, lambda p, k: rest.at[p, :, pl.ds(k * wz, wz)], rest_left, rest_right,
                              (q_sr, q_rr, q_sl, q_rl), rest_finish)
        waiting = list(range(3 + nf - 1))

    def rest_tick(how_many=1):
        for _ in range(how_many):
            if waiting:
                rest_sum.tick(jnp.int32(waiting.pop(0)))

    def two_src(d):
        return rows_at(gsum_hbm, xor(j, d, m), 1 - c)

    def out_src(d):
        return rows_at(osum_hbm, xor(j, d, m), 1 - c)

    for d in range(m - 1, -1, -1):
        two.give(d, two_src(d))
    if left:
        rest_load.wait()
    rest_tick()
    for keep in keeps:
        keep.wait()
    for d in range(m - 1, 0, -1):
        two.pass_on(d, gkeep[d])
    for d in range(m - 1, -1, -1):
        out.give(d, out_src(d))
    rest_tick()
    for load in loads[:3]:
        load.wait()
    sums[...] = jnp.zeros_like(sums)
    normed, inverse = normed_rows(res[...])
    grad = two.total(gkeep[0])
    sums[2:3, :] = jnp.sum(grad * normed, axis=0, keepdims=True)
    sums[3:4, :] = jnp.sum(grad, axis=0, keepdims=True)

    def norm_grad(grad, normed, inverse, gain):
        scaled = grad * gain
        return inverse * (scaled - jnp.mean(scaled, axis=-1, keepdims=True)
                          - normed * jnp.mean(scaled * normed, axis=-1, keepdims=True))

    gres[...] = cot[...].astype(f32) + norm_grad(grad, normed, inverse, vec[2:3, :])
    grows[mine, :] = gres[...].astype(bf16)
    x_load = pltpu.make_async_copy(x_hbm, cot, load_sems.at[len(plain)])
    x_load.start()
    rows_w = RowGather(s, m, tok, grows, (w_so, w_ro, w_ss, w_rs))
    rows_w.start(grows.at[mine])
    rest_tick()
    for d in range(1, m):
        rows_w.relay(d)
        rest_tick()
    rows_w.finish()
    for d in range(m - 1, 0, -1):
        out.pass_on(d, okeep[d])
    for load in loads[3:]:
        load.wait()

    def block(p, k):
        return parts.at[p, :, pl.ds(k * wz, wz)]

    def staged(p, act):
        sl = lax.rem(p, 2)

        @pl.when(p < pairs)
        def _():
            act(pltpu.make_async_copy(
                stage.at[sl], gout_hbm.at[pl.ds(pl.multiple_of(p * LANES, LANES), LANES)], stage_sems.at[sl]))

        @pl.when(p >= pairs)
        def _():
            q = p - pairs
            lanes = pl.ds(pl.multiple_of(q // 3 * LANES, LANES), LANES)
            act(pltpu.make_async_copy(stage_t.at[sl], gqkv_hbm.at[lax.rem(q, 3), :, lanes], stage_sems.at[sl]))

    def finish(p):
        @pl.when(p >= 2)
        def _():
            staged(p - 2, lambda cc: cc.wait())
        sl = lax.rem(p, 2)
        stage[sl] = parts[p, :, pl.ds(pl.multiple_of(f * wz, wz), wz)].astype(f32)

        @pl.when(f > 0)
        def _():
            stage[sl] += from_left[p, jnp.maximum(f - 1, 0)].astype(f32)

        @pl.when(f < nf - 1)
        def _():
            stage[sl] += from_right[p, jnp.minimum(f, nf - 2)].astype(f32)

        @pl.when(p >= pairs)
        def _():
            stage_t[sl] = stage[sl].T
        staged(p, lambda cc: cc.start())

    reduce = LineReduce(f, nf, count, block, from_left, from_right, (rs_sr, rs_rr, rs_sl, rs_rl), finish)

    for k in range(nf):
        lanes = slice(k * wz, (k + 1) * wz)
        value = dot_tn(att[...], grows[:, lanes]).astype(bf16)
        for g in range(pairs):
            parts[g, :, lanes] = value[g * LANES:(g + 1) * LANES, :]
    rest_tick(len(waiting))
    for p in range(pairs):
        reduce.tick(jnp.int32(p))

    @pl.loop(0, m)
    def _(b):
        rows = pl.ds(pl.multiple_of(b * block_rows, block_rows), block_rows)
        ga[rows, :] = dot_nt(grows[rows, :], wo[...]).astype(bf16)

    @pl.loop(0, pairs)
    def _(g):
        lanes = pl.ds(pl.multiple_of(g * LANES, LANES), LANES)
        dk[...] = jnp.zeros_like(dk)
        dv[...] = jnp.zeros_like(dv)
        lane = lane_of((block_rows, LANES))
        seen = lane_of((block_rows, block_rows)) <= lax.broadcasted_iota(jnp.int32, (block_rows, block_rows), 0)
        for b in range(m):
            rows = pl.ds(b * block_rows, block_rows)
            q = qkv[0, rows, lanes].astype(f32) * HEAD_DIM ** -0.5
            go = ga[rows, lanes].astype(f32)
            both = go * att[rows, lanes].astype(f32)
            logs = lse[rows, :]
            grad_q = jnp.zeros((block_rows, LANES), f32)
            for h in range(PER):
                head = lane // HEAD_DIM == h
                qm = jnp.where(head, q, 0.0).astype(bf16)
                gm = jnp.where(head, go, 0.0).astype(bf16)
                delta = jnp.sum(jnp.where(head, both, 0.0), axis=1, keepdims=True)
                log = jnp.sum(jnp.where(lane == g * PER + h, logs, 0.0), axis=1, keepdims=True)
                acc = jnp.zeros((block_rows, LANES), f32)
                spans = [(k, min(span, b * block_rows - k)) for k in range(0, b * block_rows, span)]
                for first, size in spans + [(b * block_rows, block_rows)]:
                    at = pl.ds(first, size)
                    key, val = qkv[1, at, lanes], qkv[2, at, lanes]
                    pr = jnp.exp(dot_nt(qm, key) - log)
                    if first == b * block_rows:
                        pr = jnp.where(seen, pr, 0.0)
                    gp = dot_nt(gm, val)
                    gs = (pr * (gp - delta)).astype(bf16)
                    dv[at, :] += dot_tn(pr.astype(bf16), gm)
                    dk[at, :] += dot_tn(gs, qm)
                    acc = acc + dot_nn(gs, key)
                grad_q = jnp.where(head, acc * HEAD_DIM ** -0.5, grad_q)
            gq[0, rows, lanes] = turn(grad_q, cos[rows, :], sin[rows, :], -1.0).astype(bf16)
        gq[1, :, lanes] = turn(dk[...], cos[...], sin[...], -1.0).astype(bf16)
        gq[2, :, lanes] = dv[...].astype(bf16)
        three = jnp.concatenate([gq[0, :, lanes], gq[1, :, lanes], gq[2, :, lanes]], axis=1)
        at = pl.ds(pl.multiple_of(s * cols + g * LANES, LANES), LANES)
        for k in range(3):
            sums[4 + k:5 + k, at] = jnp.sum(gq[k, :, lanes].astype(f32), axis=0, keepdims=True)

        @pl.when(g > 0)
        def _():
            for k in range(3):
                reduce.tick(pairs + 3 * (g - 1) + k)
        for k in range(nf):
            in1_load(k).wait()
            in1_load((k + 1) % nf).start()
            value = dot_tn(three, in1[k % 2]).astype(bf16)
            for i in range(3):
                parts[pairs + 3 * g + i, :, k * wz:(k + 1) * wz] = value[i * LANES:(i + 1) * LANES, :]
    in1_load(0).wait()

    okeep[0] = (res[...] + out.total(okeep[0])).astype(bf16)
    stores = [pltpu.make_async_copy(okeep.at[0], out_hbm, out_sems.at[0])]
    stores[0].start()
    out.drain(out_src)
    one = RowReduce(s, m, i_sib, i_off, (i_ss, i_rs, i_so, i_ro))
    late = list(range(pairs + 3 * (pairs - 1), count + nf - 1))
    for d in range(m - 1, -1, -1):
        if late:
            reduce.tick(jnp.int32(late.pop(0)))
        rows = pl.ds(pl.multiple_of(xor(j, d, m) * block_rows, block_rows), block_rows)
        value = dot_nt(gq[0, rows, :], wq[0])
        for k in (1, 2):
            value = value + dot_nt(gq[k, rows, :], wq[k])
        part[...] = value.astype(bf16)
        if d == 0:
            stores.pop().wait()
        okeep[d] = part[pl.ds(pl.multiple_of((1 - c) * tok, tok), tok), :]
        gkeep[d] = part[pl.ds(pl.multiple_of(c * tok, tok), tok), :]
        one.give(d, okeep.at[d])
        if d < m - 1:
            one.pass_on(d + 1, gkeep[d + 1])
    grad = one.total(gkeep[0])
    x_load.wait()
    normed, inverse = normed_rows(cot[...].astype(f32))
    sums[0:1, :] = jnp.sum(grad * normed, axis=0, keepdims=True)
    sums[1:2, :] = jnp.sum(grad, axis=0, keepdims=True)
    res[...] = gres[...] + norm_grad(grad, normed, inverse, vec[0:1, :])
    stores.append(pltpu.make_async_copy(res, ig_hbm, out_sems.at[1]))
    stores[0].start()

    w = o_g1.shape[1]
    spread = LANES // w

    def tile_of(t):
        return sums.at[:, pl.ds(pl.multiple_of(t // spread * LANES, LANES), LANES)]

    def small(k):
        t = lax.rem(me + k, total)
        return remote(tile_of(t), tiles.at[k], small_s.at[k], small_r.at[k],
                      {"fsdp": t // ns, "seq": lax.rem(t, ns)})

    @pl.loop(1, total)
    def _(k):
        small(k).start()
    for t in late:
        reduce.tick(jnp.int32(t))
    tiles[0] = tile_of(me)[...]

    @pl.loop(1, total)
    def _(k):
        small(k).wait_recv()
        tiles[0] += tiles[k]
    for k in range(spread):
        @pl.when(lax.rem(me, spread) == k)
        def _(k=k):
            lanes = slice(k * w, (k + 1) * w)
            for i, ref in enumerate((o_g1, o_b1, o_g2, o_b2)):
                ref[...] = tiles[0, i:i + 1, lanes]
            o_qb[...] = tiles[0, 4:7, lanes]

    @pl.loop(1, total)
    def _(k):
        small(k).wait_send()
    two.drain(two_src)
    one.drain(lambda d: okeep.at[d])
    rows_w.drain(grows.at[mine])
    for p in (count - 2, count - 1):
        staged(jnp.int32(p), lambda cc: cc.wait())
    for st in stores:
        st.wait()
    if left:
        for p in range(3):
            rest_out(jnp.int32(p), lambda cc: cc.wait())


def back(gsum, osum, res, cot, x, vec, qkv, att, lse, in1, wq, wo, cos, sin, rest, ggu, gd, nf, ns, cid):
    left = 0 if rest is None else 1
    tok, width = x.shape
    length, cols = att.shape
    wz = width // nf
    m = ns // 2
    w = width // (nf * ns)
    pairs = cols // LANES
    count = 4 * pairs
    D, V = pltpu.SemaphoreType.DMA, pltpu.VMEM
    A = pl.BlockSpec(memory_space=pl.ANY)
    M = pl.BlockSpec(memory_space=pltpu.VMEM)
    S = jax.ShapeDtypeStruct
    extra_in, extra_out, extra_scratch = (), (), []
    if left:
        r = rest.shape[1]
        extra_in = (rest, ggu, gd)
        extra_out = (S(ggu.shape, f32), S(gd.shape, f32))
        extra_scratch = [V((3, r, width), bf16), V((3, nf - 1, r, wz), bf16), V((3, nf - 1, r, wz), bf16),
                         V((3, r, wz), f32), D((3,))] + [D((3, nf - 1))] * 4
    rows_v = V((m, tok, width), bf16)
    offs_v = V((m - 1, tok, width), bf16)
    return pl.pallas_call(
        functools.partial(back_kernel, nf, ns, left),
        out_shape=(
            S((tok, width), bf16), S((tok, width), f32), S((3, wz, cols), f32), S((cols, wz), f32),
            S((1, w), f32), S((1, w), f32), S((1, w), f32), S((1, w), f32), S((3, w), f32),
        ) + extra_out,
        in_specs=[A] * (14 + 3 * left),
        out_specs=[A] * 4 + [M] * 5 + [A] * (2 * left),
        input_output_aliases={15: 9, 16: 10} if left else {},
        scratch_shapes=[
            rows_v, rows_v, V((tok, width), f32), V((tok, width), bf16), V((8, width), f32),
            V((3, length, cols), bf16), V((length, cols), bf16), V((length, LANES), f32), V((2, length, wz), bf16),
            V((3, width, cols), bf16), V((cols, width), bf16), V((length, LANES), f32), V((length, LANES), f32),
            V((length, width), bf16), V((length, cols), bf16), V((3, length, cols), bf16),
            V((length, LANES), f32), V((length, LANES), f32),
            V((count, LANES, width), bf16), V((count, nf - 1, LANES, wz), bf16), V((count, nf - 1, LANES, wz), bf16),
            V((2, LANES, wz), f32), V((2, wz, LANES), f32),
            rows_v, offs_v, rows_v, offs_v, rows_v, offs_v,
            V((2 * tok, width), bf16), V((tok, width), f32),
            V((8, width), f32), V((nf * ns, 8, LANES), f32),
            D((11,)), D((2 * m,)), D((2,)), D((nf * ns,)), D((nf * ns,)),
        ] + [D((count, nf - 1))] * 4 + [D((m,))] * 4 + [D((m,)), D((m,)), D((2 * m,)), D((2 * m,))] * 3 + [D((2,)), D((2,))]
        + extra_scratch,
        compiler_params=pltpu.CompilerParams(
            collective_id=cid, has_side_effects=True, vmem_limit_bytes=64 * 1024 * 1024 - 65536),
        name="back",
    )(gsum, osum, res, cot, x, vec, qkv, att, lse, in1, wq, wo, cos, sin, *extra_in)


def local(
    block_input,
    cotangent,
    ln1_gain,
    ln1_bias,
    qkv_weight,
    qkv_bias,
    out_weight,
    ln2_gain,
    ln2_bias,
    gate_up_weight,
    down_weight,
):
    fsdp, seq = lax.axis_size("fsdp"), lax.axis_size("seq")
    gate_up = jnp.transpose(gate_up_weight, (1, 2, 0))
    left = 1 if seq * block_input.shape[1] <= 1024 else 0
    (in_one, cot_all, in_two, qkv, mixed, logs, residual, qkv_full, out_full, vectors, cosine, sine, first) = front(
        block_input[0],
        cotangent[0],
        ln1_gain[None],
        ln1_bias[None],
        ln2_gain[None],
        ln2_bias[None],
        qkv_bias,
        jnp.transpose(qkv_weight, (1, 0, 2)),
        out_weight,
        gate_up,
        down_weight,
        fsdp,
        seq,
        1,
    )
    out_sum, grad_sum, grad_gate_up, grad_down, *rest = mlp(
        in_two, cot_all, first, gate_up, down_weight, fsdp, left, 0
    )
    block_output, input_grad, grad_qkv, grad_out, gain_one, bias_one, gain_two, bias_two, grad_bias, *grads = back(
        grad_sum,
        out_sum,
        residual,
        cotangent[0],
        block_input[0],
        vectors,
        qkv,
        mixed,
        logs,
        in_one,
        qkv_full,
        out_full,
        cosine,
        sine,
        rest[0] if left else None,
        grad_gate_up,
        grad_down,
        fsdp,
        seq,
        2,
    )
    if left:
        grad_gate_up, grad_down = grads
    return (
        block_output[None],
        input_grad[None],
        gain_one[0],
        bias_one[0],
        jnp.transpose(grad_qkv, (1, 0, 2)),
        grad_bias,
        grad_out,
        gain_two[0],
        bias_two[0],
        jnp.transpose(grad_gate_up, (2, 0, 1)),
        grad_down,
    )


def solution(mesh):
    placed = (
        P("fsdp", "seq", None),
        P("fsdp", "seq", None),
        P(("fsdp", "seq")),
        P(("fsdp", "seq")),
        P("fsdp", None, "seq"),
        P(None, ("fsdp", "seq")),
        P("seq", "fsdp"),
        P(("fsdp", "seq")),
        P(("fsdp", "seq")),
        P("fsdp", None, "seq"),
        P("seq", "fsdp"),
    )
    return jax.shard_map(
        local,
        mesh=mesh,
        in_specs=placed,
        out_specs=(
            P("fsdp", "seq", None),
            P("fsdp", "seq", None),
            P(("fsdp", "seq")),
            P(("fsdp", "seq")),
            P("fsdp", None, "seq"),
            P(None, ("fsdp", "seq")),
            P("seq", "fsdp"),
            P(("fsdp", "seq")),
            P(("fsdp", "seq")),
            P("fsdp", None, "seq"),
            P("seq", "fsdp"),
        ),
        check_vma=False,
    )
```

```python
import functools

import jax
import jax.numpy as jnp
from jax import lax
from jax.experimental import pallas as pl
from jax.experimental.pallas import tpu as pltpu
from jax.sharding import PartitionSpec as P

HEAD_DIM = 64
ROTARY = 16

epsilon = 1e-05
masked_score = -1e30

MESH = pl.DeviceIdType.MESH
NT = (((1,), (1,)), ((), ()))
TN = (((0,), (0,)), ((), ()))
f32, bf16 = jnp.float32, jnp.bfloat16


def dot_nn(a, b):
    return jnp.dot(a, b, preferred_element_type=f32)


def dot_nt(a, b):
    return lax.dot_general(a, b, NT, preferred_element_type=f32)


def dot_tn(a, b):
    return lax.dot_general(a, b, TN, preferred_element_type=f32)


def remote(src, dst, send_sem, recv_sem, device):
    return pltpu.make_async_remote_copy(
        src_ref=src, dst_ref=dst, send_sem=send_sem, recv_sem=recv_sem,
        device_id=device, device_id_type=MESH)


def line_barrier(f, n):
    barrier = pltpu.get_barrier_semaphore()

    @pl.when(f > 0)
    def _():
        pl.semaphore_signal(barrier, inc=1, device_id={"fsdp": f - 1}, device_id_type=MESH)

    @pl.when(f < n - 1)
    def _():
        pl.semaphore_signal(barrier, inc=1, device_id={"fsdp": f + 1}, device_id_type=MESH)

    pl.semaphore_wait(barrier, (f > 0).astype(jnp.int32) + (f < n - 1).astype(jnp.int32))


def when(condition):
    if isinstance(condition, (bool, int)):
        return (lambda body: body()) if condition else (lambda body: None)
    return pl.when(condition)


class LineGather:
    def __init__(self, f, n, count, own, slot, sems):
        self.f, self.n, self.count, self.own, self.slot = f, n, count, own, slot
        self.send_r, self.recv_r, self.send_l, self.recv_l = sems

    def copy(self, src, p, h, source, rightward):
        f = self.f
        send, recv = (self.send_r, self.recv_r) if rightward else (self.send_l, self.recv_l)
        target = f + 1 if rightward else f - 1
        return remote(src, self.slot(p, source), send.at[p, h], recv.at[p, h], {"fsdp": target})

    def send_own(self, t):
        f, n = self.f, self.n

        @when((t >= 0) & (t < self.count))
        def _():
            @pl.when(f < n - 1)
            def _():
                self.own(t, lambda src: self.copy(src, t, 0, f, True).start())

            @pl.when(f > 0)
            def _():
                self.own(t, lambda src: self.copy(src, t, 0, f, False).start())

    def arrivals(self, t):
        for h in range(self.n - 1, 0, -1):
            self.arrive(t - h, h)

    def tick(self, t):
        self.send_own(t)
        self.arrivals(t)

    def arrive(self, p, h):
        f, n = self.f, self.n

        @when((p >= 0) & (p < self.count))
        def _():
            @pl.when(f - h >= 0)
            def _():
                here = self.slot(p, f - h)
                self.copy(here, p, h - 1, f - h, True).wait_recv()
                if h < n - 1:
                    @pl.when(f < n - 1)
                    def _():
                        self.copy(here, p, h, f - h, True).start()

            @pl.when(f + h <= n - 1)
            def _():
                here = self.slot(p, f + h)
                self.copy(here, p, h - 1, f + h, False).wait_recv()
                if h < n - 1:
                    @pl.when(f > 0)
                    def _():
                        self.copy(here, p, h, f + h, False).start()

    def drain(self, p):
        f, n = self.f, self.n
        for h in range(0, n - 1):
            @pl.when((f - h >= 0) & (f < n - 1))
            def _(h=h):
                self.copy(self.slot(p, f - h), p, h, f - h, True).wait_send()

            @pl.when((f + h <= n - 1) & (f > 0))
            def _(h=h):
                self.copy(self.slot(p, f + h), p, h, f + h, False).wait_send()


class LineReduce:
    def __init__(self, f, n, count, block, from_left, from_right, sems, finish):
        self.f, self.n, self.count, self.block = f, n, count, block
        self.from_left, self.from_right, self.finish = from_left, from_right, finish
        self.send_r, self.recv_r, self.send_l, self.recv_l = sems

    def right(self, p, j):
        return remote(self.block(p, j), self.from_left.at[p, j - 1], self.send_r.at[p, j - 1],
                      self.recv_r.at[p, j - 1], {"fsdp": self.f + 1})

    def left(self, p, j):
        return remote(self.block(p, j), self.from_right.at[p, j], self.send_l.at[p, j],
                      self.recv_l.at[p, j], {"fsdp": self.f - 1})

    def tick(self, u):
        f, n, count = self.f, self.n, self.count
        p = u - f

        @pl.when((p >= 0) & (p < count))
        def _():
            @pl.loop(0, n - 1)
            def _(i):
                j = n - 1 - i

                @pl.when((f > 0) & (j >= f))
                def _():
                    self.right(p, j).wait_recv()

                @pl.when((f > 0) & (j > f))
                def _():
                    here = self.block(p, j)
                    here[...] = (here[...].astype(f32) + self.from_left[p, j - 1].astype(f32)).astype(bf16)

                @pl.when(j > f)
                def _():
                    self.right(p, j).start()

        q = u - (n - 1 - f)

        @pl.when((q >= 0) & (q < count))
        def _():
            @pl.loop(0, n - 1)
            def _(j):
                @pl.when((f < n - 1) & (j <= f))
                def _():
                    self.left(q, j).wait_recv()

                @pl.when((f < n - 1) & (j < f))
                def _():
                    here = self.block(q, j)
                    here[...] = (here[...].astype(f32) + self.from_right[q, j].astype(f32)).astype(bf16)

                @pl.when(j < f)
                def _():
                    self.left(q, j).start()

        e = u - (n - 1)

        @pl.when((e >= 0) & (e < count))
        def _():
            @pl.loop(0, n)
            def _(j):
                @pl.when(j > f)
                def _():
                    self.right(e, j).wait_send()

                @pl.when(j < f)
                def _():
                    self.left(e, j).wait_send()
            self.finish(e)


def mlp_kernel(n, r, rb, left, in2_hbm, cot_hbm, w0_hbm, wgu_hbm, wd_hbm,
               out_hbm, gin_hbm, ggu_hbm, gd_hbm, *more):
    rest_hbm, more = (more[0], more[1:]) if left else (None, more)
    (in2, cot, acc_o, acc_g, w, hid, dga, dup, parts, from_left, from_right,
               stage, load_sems, own_sems, ag_sr, ag_rr, ag_sl, ag_rl, rs_sr, rs_rr, rs_sl, rs_rl,
               stage_sems, rest_sems) = more
    f = lax.axis_index("fsdp")
    tokens, width = in2.shape
    wz = width // n
    ff = wd_hbm.shape[0]
    nc = ff // r
    count = 3 * nc
    summed = count - 3 * left
    ahead = max(n - 1, 3)
    ring = parts.shape[0]
    loads = [pltpu.make_async_copy(in2_hbm, in2, load_sems.at[0]),
             pltpu.make_async_copy(cot_hbm, cot, load_sems.at[1]),
             pltpu.make_async_copy(w0_hbm, w.at[pl.ds(0, 3)], load_sems.at[2])]
    for c in loads:
        c.start()

    def rows_of(p):
        return pl.ds(pl.multiple_of(p // 3 * r, r), r)

    def own(p, use):
        kind = lax.rem(p, 3)

        @pl.when(kind < 2)
        def _():
            use(wgu_hbm.at[kind, rows_of(p)])

        @pl.when(kind == 2)
        def _():
            use(wd_hbm.at[rows_of(p)])

    def slot(p, source):
        return w.at[p, :, pl.ds(pl.multiple_of(source * wz, wz), wz)]

    def own_copy(p, act):
        own(p, lambda src: act(pltpu.make_async_copy(src, slot(p, f), own_sems.at[p])))

    @pl.loop(3, count)
    def _(p):
        own_copy(p, lambda c: c.start())

    line_barrier(f, n)
    gather = LineGather(f, n, count - 3, lambda p, use: own(p + 3, use), lambda p, source: slot(p + 3, source),
                        (ag_sr, ag_rr, ag_sl, ag_rl))

    def block(p, j):
        return parts.at[lax.rem(p, ring), :, pl.ds(pl.multiple_of(j * wz, wz), wz)]

    def stage_out(p, act):
        kind = lax.rem(p, 3)
        sl = lax.rem(p, 2)

        @pl.when(kind < 2)
        def _():
            act(pltpu.make_async_copy(stage.at[sl], ggu_hbm.at[kind, rows_of(p)], stage_sems.at[sl]))

        @pl.when(kind == 2)
        def _():
            act(pltpu.make_async_copy(stage.at[sl], gd_hbm.at[rows_of(p)], stage_sems.at[sl]))

    def finish(p):
        @pl.when(p >= 2)
        def _():
            stage_out(p - 2, lambda c: c.wait())
        sl = lax.rem(p, 2)
        mine = parts.at[lax.rem(p, ring), :, pl.ds(pl.multiple_of(f * wz, wz), wz)]
        stage[sl] = mine[...].astype(f32)

        @pl.when(f > 0)
        def _():
            stage[sl] += from_left[p, jnp.maximum(f - 1, 0)].astype(f32)

        @pl.when(f < n - 1)
        def _():
            stage[sl] += from_right[p, jnp.minimum(f, n - 2)].astype(f32)
        stage_out(p, lambda c: c.start())

    reduce = LineReduce(f, n, summed, block, from_left, from_right, (rs_sr, rs_rr, rs_sl, rs_rl), finish)

    acc_o[...] = jnp.zeros_like(acc_o)
    acc_g[...] = jnp.zeros_like(acc_g)

    for t in range(3):
        gather.send_own(t)

    for c in loads:
        c.wait()

    def compute(c):
        @pl.when(c > 0)
        def _():
            for k in range(3):
                own_copy(3 * c + k, lambda cc: cc.wait())

        @pl.loop(0, tokens // rb)
        def _(i):
            rows = pl.ds(pl.multiple_of(i * rb, rb), rb)
            a = in2[rows, :]
            gate = dot_nt(a, w[3 * c])
            up = dot_nt(a, w[3 * c + 1])
            gh = dot_nt(cot[rows, :], w[3 * c + 2])
            sig = jax.nn.sigmoid(gate)
            silu = gate * sig
            h = (silu * up).astype(bf16)
            dg = (gh * up * sig * (1.0 + gate * (1.0 - sig))).astype(bf16)
            du = (gh * silu).astype(bf16)
            hid[rows, :] = h
            dga[rows, :] = dg
            dup[rows, :] = du
            acc_o[rows, :] = (acc_o[rows, :].astype(f32) + dot_nn(h, w[3 * c + 2])).astype(acc_o.dtype)
            acc_g[rows, :] = (acc_g[rows, :].astype(f32) + dot_nn(dg, w[3 * c]) + dot_nn(du, w[3 * c + 1])).astype(acc_g.dtype)

    @pl.loop(0, nc)
    def _(c):
        compute(c)

        @pl.when(c == 0)
        def _():
            gather.arrivals(1)
        for k, (small, big) in enumerate(((dga, in2), (dup, in2), (hid, cot))):
            for j in range(n):
                block(3 * c + k, j)[...] = dot_tn(small[...], big[:, pl.ds(j * wz, wz)]).astype(bf16)
            reduce.tick(3 * c + k)
            if k == 0:
                @pl.when(c == 0)
                def _():
                    for t in range(2, ahead):
                        if t < 3:
                            gather.arrivals(t)
                        else:
                            gather.tick(t)
            gather.tick(3 * c + k + ahead)

    in2[...] = acc_o[...].astype(bf16)
    cot[...] = acc_g[...].astype(bf16)
    stores = [pltpu.make_async_copy(in2, out_hbm, load_sems.at[0]),
              pltpu.make_async_copy(cot, gin_hbm, load_sems.at[1])]
    for k in range(3 * left):
        stores.append(pltpu.make_async_copy(parts.at[(summed + k) % ring], rest_hbm.at[k], rest_sems.at[k]))
    for c in stores:
        c.start()

    if left == 0:
        @pl.loop(count, summed + n - 1)
        def _(u):
            reduce.tick(u)

    @pl.loop(0, count - 3)
    def _(p):
        gather.drain(p)
    for p in (summed - 2, summed - 1):
        stage_out(jnp.int32(p), lambda c: c.wait())
    for c in stores:
        c.wait()


def piece_rows(ff):
    r = 0
    for cand in range(16, 257, 16):
        if ff % cand == 0:
            r = cand
    return r


def mlp(in2, cot, w0, wgu, wd, n, left, cid):
    tokens, width = in2.shape
    ff, wz = wd.shape
    r = piece_rows(ff)
    rb = min(256, tokens)
    nc = ff // r
    count = 3 * nc
    ring = min(count, 3 * max((n - 1 + 2) // 3, left) + 3)
    any_spec = pl.BlockSpec(memory_space=pl.ANY)
    acc_dtype = f32 if tokens * width * 8 <= 20 * 2**20 else bf16
    D = pltpu.SemaphoreType.DMA
    return pl.pallas_call(
        functools.partial(mlp_kernel, n, r, rb, left),
        out_shape=(
            jax.ShapeDtypeStruct((tokens, width), bf16),
            jax.ShapeDtypeStruct((tokens, width), bf16),
            jax.ShapeDtypeStruct((2, ff, wz), f32),
            jax.ShapeDtypeStruct((ff, wz), f32),
        ) + (jax.ShapeDtypeStruct((3 * left, r, width), bf16),) * min(left, 1),
        in_specs=[any_spec] * 5,
        out_specs=[any_spec] * (4 + min(left, 1)),
        scratch_shapes=[
            pltpu.VMEM((tokens, width), bf16),
            pltpu.VMEM((tokens, width), bf16),
            pltpu.VMEM((tokens, width), acc_dtype),
            pltpu.VMEM((tokens, width), acc_dtype),
            pltpu.VMEM((count, r, width), bf16),
            pltpu.VMEM((tokens, r), bf16),
            pltpu.VMEM((tokens, r), bf16),
            pltpu.VMEM((tokens, r), bf16),
            pltpu.VMEM((ring, r, width), bf16),
            pltpu.VMEM((count - 3 * left, n - 1, r, wz), bf16),
            pltpu.VMEM((count - 3 * left, n - 1, r, wz), bf16),
            pltpu.VMEM((2, r, wz), f32),
            D((3,)),
            D((count,)),
        ] + [D((count - 3, n - 1))] * 4 + [D((count - 3 * left, n - 1))] * 4 + [D((2,)), D((max(3 * left, 1),))],
        compiler_params=pltpu.CompilerParams(
            collective_id=cid, has_side_effects=True, vmem_limit_bytes=64 * 1024 * 1024 - 65536),
        name="mlp",
    )(in2, cot, w0, wgu, wd)


LANES = 128
PER = LANES // HEAD_DIM


def xor(a, b, count):
    total = 0
    bit = 1
    while bit < count:
        x, y = (a // bit) % 2, (b // bit) % 2
        total = total + bit * (x + y - 2 * x * y)
        bit *= 2
    return total


def everyone_barrier(me, nf, ns):
    barrier = pltpu.get_barrier_semaphore()
    total = nf * ns

    @pl.loop(1, total)
    def _(k):
        t = lax.rem(me + k, total)
        pl.semaphore_signal(barrier, inc=1, device_id={"fsdp": t // ns, "seq": lax.rem(t, ns)},
                            device_id_type=MESH)
    pl.semaphore_wait(barrier, total - 1)


class RowGather:
    def __init__(self, s, m, tok, buf, sems):
        self.j, self.c, self.m, self.tok, self.buf = s // 2, s % 2, m, tok, buf
        self.send_o, self.recv_o, self.send_s, self.recv_s = sems
        self.square = m == 4

    def slot(self, chip, core, part=None):
        row = (chip * 2 + core) * self.tok
        if part is None:
            return self.buf.at[pl.ds(pl.multiple_of(row, self.tok), self.tok)]
        half = self.tok // 2
        return self.buf.at[pl.ds(pl.multiple_of(row + part * half, half), half)]

    def off(self, src, d, chip):
        return remote(src, self.slot(chip, self.c), self.send_o.at[d], self.recv_o.at[d],
                      {"seq": xor(self.j, d, self.m) * 2 + self.c})

    def part_of(self, src, d, part):
        half = self.tok // 2
        return remote(src.at[pl.ds(part * half, half)], self.slot(self.j, self.c, part),
                      self.send_o.at[2 * d + part], self.recv_o.at[2 * d + part],
                      {"seq": xor(self.j, d, 4) * 2 + self.c})

    def half(self, part, source, to, index):
        here = self.slot(xor(self.j, source, 4), self.c, part)
        return remote(here, here, self.send_o.at[index], self.recv_o.at[index],
                      {"seq": xor(self.j, to, 4) * 2 + self.c})

    def sib(self, src, d, core):
        return remote(src, self.slot(xor(self.j, d, self.m), core), self.send_s.at[d], self.recv_s.at[d],
                      {"seq": self.j * 2 + 1 - self.c})

    def start(self, src):
        if self.square:
            for d, part in ((1, 0), (2, 1), (1, 1), (2, 0)):
                self.part_of(src, d, part).start()
        else:
            for d in range(1, self.m):
                self.off(src, d, self.j).start()
        self.sib(src, 0, self.c).start()

    def relay(self, d):
        chip = xor(self.j, d, self.m)
        here = self.slot(chip, self.c)
        if not self.square:
            self.off(here, d, chip).wait_recv()
        elif d == 3:
            self.half(0, 3, 2, 6).wait_recv()
            self.half(1, 3, 1, 7).wait_recv()
        else:
            if d == 1:
                for n in (1, 2):
                    self.half(n - 1, n, n, 3 * n - 1).wait_recv()
                    self.half(n - 1, n, 3 - n, 5 + n).start()
            self.half(2 - d, d, d, d + 2).wait_recv()
        self.sib(here, d, self.c).start()

    def arrived(self, d):
        self.sib(self.slot(xor(self.j, d, self.m), 1 - self.c), d, 1 - self.c).wait_recv()

    def finish(self):
        for d in range(self.m):
            self.arrived(d)

    def drain(self, src):
        for d in range(1, self.m):
            if not self.square:
                self.off(src, d, self.j).wait_send()
            elif d < 3:
                for part in range(2):
                    self.part_of(src, d, part).wait_send()
                self.half(d - 1, d, 3 - d, 5 + d).wait_send()
            self.sib(self.slot(xor(self.j, d, self.m), self.c), d, self.c).wait_send()
        self.sib(src, 0, self.c).wait_send()


class RowReduce:
    def __init__(self, s, m, from_sib, from_off, sems):
        self.j, self.c, self.m = s // 2, s % 2, m
        self.from_sib, self.from_off = from_sib, from_off
        self.send_s, self.recv_s, self.send_o, self.recv_o = sems
        self.square = m == 4
        self.tok = from_sib.shape[1]

    def sib(self, src, d):
        return remote(src, self.from_sib.at[d], self.send_s.at[d], self.recv_s.at[d],
                      {"seq": self.j * 2 + 1 - self.c})

    def off(self, d):
        return remote(self.from_sib.at[d], self.from_off.at[d - 1], self.send_o.at[d], self.recv_o.at[d],
                      {"seq": xor(self.j, d, self.m) * 2 + self.c})

    def half(self, d, part):
        at = pl.ds(part * (self.tok // 2), self.tok // 2)
        last = d // 3
        to = d * (1 - last) + (part + 1) * last
        index = 2 * d + part
        return remote(self.from_sib.at[d, at], self.from_off.at[d - 1, at], self.send_o.at[index], self.recv_o.at[index],
                      {"seq": xor(self.j, to, 4) * 2 + self.c})

    def give(self, d, src):
        self.sib(src, d).start()

    def pass_on(self, d, own):
        here = self.from_sib.at[d]
        self.sib(here, d).wait_recv()
        here[...] = (own.astype(f32) + here[...].astype(f32)).astype(bf16)
        if not self.square:
            self.off(d).start()
            return
        for part in range(2):
            @when((d == 3) | (part == d - 1))
            def _(part=part):
                self.half(d, part).start()

    def forward(self):
        if self.square:
            for part, d in ((0, 2), (1, 1)):
                at = pl.ds(part * (self.tok // 2), self.tok // 2)
                self.half(3, part).wait_recv()
                self.from_sib[d, at] = (self.from_sib[d, at].astype(f32) + self.from_off[2, at].astype(f32)).astype(bf16)
                self.half(d, part).start()

    def collect(self, own):
        here = self.from_sib.at[0]
        self.sib(here, 0).wait_recv()
        value = own.astype(f32) + here[...].astype(f32)
        for d in (1, 2) if self.square else range(self.m - 1, 0, -1):
            if self.square:
                self.half(d, 0).wait_recv()
                self.half(d, 1).wait_recv()
            else:
                self.off(d).wait_recv()
            value = value + self.from_off[d - 1].astype(f32)
        return value

    def total(self, own):
        self.forward()
        return self.collect(own)

    def drain(self, src_of):
        for d in range(self.m):
            self.sib(src_of(d), d).wait_send()
        for d in range(1, self.m):
            if self.square:
                self.half(d, 0).wait_send()
                self.half(d, 1).wait_send()
            else:
                self.off(d).wait_send()


def normed_rows(x):
    center = x - jnp.mean(x, axis=-1, keepdims=True)
    inverse = lax.rsqrt(jnp.mean(center * center, axis=-1, keepdims=True) + epsilon)
    return center * inverse, inverse


def lane_of(shape):
    return lax.broadcasted_iota(jnp.int32, shape, len(shape) - 1)


def rotary_tiles(rows, first):
    half = ROTARY // 2
    lane = lane_of((rows, LANES))
    pos = (first + lax.broadcasted_iota(jnp.int32, (rows, LANES), 0)).astype(f32)
    within = lane % HEAD_DIM
    freq = jnp.zeros((rows, LANES), f32)
    for i in range(half):
        freq = jnp.where(within % half == i, float(10000.0 ** (-2.0 * i / ROTARY)), freq)
    angle = pos * freq
    turned = within < ROTARY
    cosine = jnp.where(turned, jnp.cos(angle), 1.0)
    sine = jnp.where(turned, jnp.sin(angle), 0.0)
    return cosine, sine


def turn(u, cosine, sine, direction):
    half = ROTARY // 2
    within = lane_of(u.shape) % HEAD_DIM
    ahead = pltpu.roll(u, LANES - half, 1)
    behind = pltpu.roll(u, half, 1)
    turned = jnp.where(within < half, -ahead, behind)
    return u * cosine + direction * turned * sine


def front_kernel(nf, ns,
                 x_hbm, cot_hbm, g1, b1, g2, b2, qb, wqkv_hbm, wo_hbm, wgu_hbm, wd_hbm,
                 in1_hbm, cotall_hbm, in2_hbm, qkv_hbm, att_hbm, lse_hbm, res_hbm, wq_hbm, woall_hbm,
                 vec_hbm, cos_hbm, sin_hbm, w0_hbm,
                 xall, in1, tile, tiles, vecs, wq, wo, qkv, att, lse, cos, sin, part, keep, give,
                 from_sib, from_off, res, in2, w0,
                 load_sems, own_sems, small_s, small_r,
                 ag_sr, ag_rr, ag_sl, ag_rl, m_sr, m_rr, m_sl, m_rl,
                 a_so, a_ro, a_ss, a_rs, c_so, c_ro, c_ss, c_rs, e_so, e_ro, e_ss, e_rs,
                 r_ss, r_rs, r_so, r_ro, out_sems):
    f, s = lax.axis_index("fsdp"), lax.axis_index("seq")
    total = nf * ns
    me = f * ns + s
    m = ns // 2
    j, c = s // 2, s % 2
    tok, width = x_hbm.shape
    length = in1.shape[0]
    cols = qkv.shape[2]
    wz = width // nf
    pairs = cols // LANES
    block_rows = 2 * tok

    last_piece = 3 * pairs

    def own(p, use):
        use(wqkv_hbm.at[p % 3, :, pl.ds(p // 3 * LANES, LANES)] if p < last_piece else wo_hbm)

    def slot(p, source):
        if p < last_piece:
            return wq.at[p % 3, pl.ds(pl.multiple_of(source * wz, wz), wz), pl.ds(p // 3 * LANES, LANES)]
        return wo.at[:, pl.ds(pl.multiple_of(source * wz, wz), wz)]

    def own_copy(p):
        box = []
        own(p, lambda src: box.append(pltpu.make_async_copy(src, slot(p, f), own_sems.at[p])))
        return box[0]

    for p in range(last_piece + 1):
        own_copy(p).start()

    r = w0.shape[1]

    def mlp_own(p, use):
        @pl.when(p < 2)
        def _():
            use(wgu_hbm.at[p, pl.ds(0, r)])

        @pl.when(p == 2)
        def _():
            use(wd_hbm.at[pl.ds(0, r)])

    def mlp_slot(p, source):
        return w0.at[p, :, pl.ds(pl.multiple_of(source * wz, wz), wz)]

    mlp_copies = [pltpu.make_async_copy(wgu_hbm.at[p, pl.ds(0, r)] if p < 2 else wd_hbm.at[pl.ds(0, r)],
                                        mlp_slot(p, f), own_sems.at[last_piece + 1 + p]) for p in range(3)]
    for copy in mlp_copies:
        copy.start()
    cot_rows = pl.ds(pl.multiple_of(s * tok, tok), tok)
    cot_own = pltpu.make_async_copy(cot_hbm, cotall_hbm.at[cot_rows], load_sems.at[1])

    w = g1.shape[1]
    spread = LANES // w
    here = lane_of((1, LANES)) // w == lax.rem(me, spread)
    tile[...] = jnp.zeros_like(tile)
    for row, piece in enumerate((g1[...], b1[...], g2[...], b2[...], qb[0:1, :], qb[1:2, :], qb[2:3, :])):
        wide = jnp.concatenate([piece.astype(f32)] * spread, axis=1)
        tile[row:row + 1, :] = jnp.where(here, wide, 0.0)

    everyone_barrier(me, nf, ns)
    gather = LineGather(f, nf, last_piece + 1, own, slot, (ag_sr, ag_rr, ag_sl, ag_rl))
    second = LineGather(f, nf, 3, mlp_own, mlp_slot, (m_sr, m_rr, m_sl, m_rl))
    mine = pl.ds(pl.multiple_of(s * tok, tok), tok)

    def small(k):
        t = lax.rem(me + k, total)
        return remote(tile, tiles.at[k], small_s.at[k], small_r.at[k], {"fsdp": t // ns, "seq": lax.rem(t, ns)})

    @pl.loop(1, total)
    def _(k):
        small(k).start()
    for t in range(3):
        gather.send_own(t)
    rows_x = RowGather(s, m, tok, xall, (a_so, a_ro, a_ss, a_rs))
    rows_x.start(x_hbm)
    x_own = pltpu.make_async_copy(x_hbm, xall.at[mine], load_sems.at[3])
    x_own.start()
    cot_own.start()
    tiles[0] = tile[...]
    vecs[...] = jnp.zeros_like(vecs)
    stores = []

    def store(ref, hbm, i):
        st = pltpu.make_async_copy(ref, hbm, out_sems.at[i])
        st.start()
        stores.append(st)

    state = [2]

    def ticks_to(t):
        while state[0] < t:
            state[0] += 1
            gather.tick(state[0])

    gather.arrivals(1)

    @pl.loop(1, total)
    def _(k):
        small(k).wait_recv()

    @pl.loop(0, total)
    def _(k):
        source = lax.rem(me + total - k, total)
        lanes = pl.ds(pl.multiple_of(source // spread * LANES, LANES), LANES)
        vecs[:, lanes] += tiles[k]
    store(vecs, vec_hbm, 2)
    gather.arrivals(2)

    @pl.loop(0, length // block_rows)
    def _(q):
        rows = pl.ds(pl.multiple_of(q * block_rows, block_rows), block_rows)
        cos[rows, :], sin[rows, :] = rotary_tiles(block_rows, q * block_rows)
    store(cos, cos_hbm, 0)
    store(sin, sin_hbm, 1)
    rows_cot = RowGather(s, m, tok, cotall_hbm, (c_so, c_ro, c_ss, c_rs))

    def norm_chip(d):
        @pl.loop(0, 2)
        def _(core):
            rows = pl.ds(pl.multiple_of((xor(j, d, m) * 2 + core) * tok, tok), tok)
            normed, _ = normed_rows(xall[rows, :].astype(f32))
            in1[rows, :] = (normed * vecs[0:1, :] + vecs[1:2, :]).astype(bf16)

    x_own.wait()
    for d in range(m):
        if d > 0:
            rows_x.relay(d)
        if d == min(2, m - 1):
            rows_cot.start(cot_hbm)
            ticks_to(min(3, nf + 1))
        if d > 2:
            rows_x.arrived(d - 1)
            norm_chip(d - 1)
            ticks_to(min(1 + d, nf + 1))
        elif d > 0:
            rows_x.arrived(d - 1)
            norm_chip(d - 1)
    rows_x.arrived(m - 1)
    norm_chip(m - 1)
    store(in1, in1_hbm, 3)

    def project(g):
        lanes = slice(g * LANES, (g + 1) * LANES)
        bias_at = pl.ds(pl.multiple_of(s * cols + g * LANES, LANES), LANES)
        for k in range(3):
            own_copy(3 * g + k).wait()

        @pl.loop(0, length // block_rows)
        def _(q):
            rows = pl.ds(pl.multiple_of(q * block_rows, block_rows), block_rows)
            for k in range(3):
                u = dot_nn(in1[rows, :], wq[k, :, lanes]) + vecs[4 + k:5 + k, bias_at]
                if k < 2:
                    u = turn(u, cos[rows, :], sin[rows, :], 1.0)
                qkv[k, rows, lanes] = u.astype(bf16)

    ticks_to(2 + nf - 1)
    project(0)

    def attend(b, g):
        rows = pl.ds(b * block_rows, block_rows)

        if True:
            lanes = pl.ds(pl.multiple_of(g * LANES, LANES), LANES)
            q, kd, vd = qkv[0, rows, lanes], qkv[1, rows, lanes], qkv[2, rows, lanes]
            lane = lane_of((block_rows, LANES))
            seen = lane_of((block_rows, block_rows)) <= lax.broadcasted_iota(jnp.int32, (block_rows, block_rows), 0)
            out = jnp.zeros((block_rows, LANES), f32)
            logs = lse[rows, :]
            for h in range(PER):
                head = lane // HEAD_DIM == h
                qm = jnp.where(head, q.astype(f32) * HEAD_DIM ** -0.5, 0.0).astype(bf16)
                sd = jnp.where(seen, dot_nt(qm, kd), masked_score)
                top = jnp.max(sd, axis=1, keepdims=True)
                if b > 0:
                    before = pl.ds(0, b * block_rows)
                    sl = dot_nt(qm, qkv[1, before, lanes])
                    top = jnp.maximum(top, jnp.max(sl, axis=1, keepdims=True))
                ed = jnp.exp(sd - top)
                tot = jnp.sum(ed, axis=1, keepdims=True)
                if b > 0:
                    el = jnp.exp(sl - top)
                    tot = tot + jnp.sum(el, axis=1, keepdims=True)
                inv = 1.0 / tot
                value = dot_nn((ed * inv).astype(bf16), vd)
                if b > 0:
                    value = value + dot_nn((el * inv).astype(bf16), qkv[2, before, lanes])
                out = jnp.where(head, value, out)
                logs = jnp.where(lane == g * PER + h, top + jnp.log(tot), logs)
            att[rows, lanes] = out.astype(bf16)
            lse[rows, :] = logs

    lse[...] = jnp.zeros_like(lse)
    sums = RowReduce(s, m, from_sib, from_off, (r_ss, r_rs, r_so, r_ro))

    @pl.loop(0, (pairs + 1) * m)
    def _(turn_here):
        g, step = turn_here // m, lax.rem(turn_here, m)
        d = m - 1 - step
        chip = xor(j, d, m)

        for later in range(1, pairs):
            @pl.when((g == later) & (step == 0))
            def _(later=later):
                project(later)
        for b in range(m):
            @pl.when((g < pairs) & (chip == b))
            def _(b=b):
                attend(b, g)

        for later in range(1, pairs):
            for t in range(3 * later + nf - 1, 3 * later + nf + 2):
                @pl.when((g == later - 1) & (step == min(t - 3 * later - nf + 1, m - 1)))
                def _(t=t):
                    gather.tick(t)
                    if t == last_piece + nf - 2:
                        for p in range(3):
                            second.send_own(jnp.int32(p))
        for k in range(1, m):
            @pl.when((g == (0 if k < m - 1 else pairs - 1)) & (step == k))
            def _(k=k):
                rows_cot.relay(k)

        @pl.when((g == pairs) & (step == 0))
        def _():
            gather.tick(last_piece + nf - 1)
            own_copy(last_piece).wait()
            if pairs == 1:
                for p in range(3):
                    second.send_own(jnp.int32(p))

        @pl.when(g == pairs)
        def _():
            rows = pl.ds(pl.multiple_of(chip * block_rows, block_rows), block_rows)
            part[...] = dot_nn(att[rows, :], wo[...])
            give[d] = part[pl.ds(pl.multiple_of((1 - c) * tok, tok), tok), :].astype(bf16)
            keep[d] = part[pl.ds(pl.multiple_of(c * tok, tok), tok), :]
            sums.give(d, give.at[d])

            @pl.when(step > 0)
            def _():
                sums.pass_on(d + 1, keep[d + 1])
    second.arrivals(jnp.int32(1))
    ticks = list(range(2, 3 + nf - 1))
    store(qkv, qkv_hbm, 4)
    store(wq, wq_hbm, 5)
    store(wo, woall_hbm, 6)
    store(att, att_hbm, 7)
    store(lse, lse_hbm, 8)
    rows_cot.finish()
    res[...] = xall[mine, :].astype(f32) + sums.total(keep[0])
    store(res, res_hbm, 9)
    normed, _ = normed_rows(res[...])
    in2[...] = (normed * vecs[2:3, :] + vecs[3:4, :]).astype(bf16)
    rows_two = RowGather(s, m, tok, in2_hbm, (e_so, e_ro, e_ss, e_rs))
    rows_two.start(in2)
    in2_own = pltpu.make_async_copy(in2, in2_hbm.at[mine], load_sems.at[2])
    in2_own.start()
    if ticks:
        second.arrivals(jnp.int32(ticks.pop(0)))
    for d in range(1, m):
        rows_two.relay(d)
        if ticks and d < m - 1:
            second.arrivals(jnp.int32(ticks.pop(0)))
    rows_two.finish()
    for t in ticks:
        second.arrivals(jnp.int32(t))
    for copy in mlp_copies:
        copy.wait()
    store(w0, w0_hbm, 10)

    @pl.loop(1, total)
    def _(k):
        small(k).wait_send()
    for p in range(last_piece + 1):
        gather.drain(p)
    for p in range(3):
        second.drain(p)
    rows_x.drain(x_hbm)
    rows_cot.drain(cot_hbm)
    rows_two.drain(in2)
    sums.drain(lambda d: give.at[d])
    cot_own.wait()
    in2_own.wait()
    for st in stores:
        st.wait()


def front(x, cot, g1, b1, g2, b2, qb, wqkv, wo, wgu, wd, nf, ns, cid):
    r = piece_rows(wd.shape[0])
    tok, width = x.shape
    cols, wz = wo.shape
    length = tok * ns
    m = ns // 2
    w = g1.shape[1]
    pairs = cols // LANES
    D, V = pltpu.SemaphoreType.DMA, pltpu.VMEM
    A = pl.BlockSpec(memory_space=pl.ANY)
    M = pl.BlockSpec(memory_space=pltpu.VMEM)
    S = jax.ShapeDtypeStruct
    return pl.pallas_call(
        functools.partial(front_kernel, nf, ns),
        out_shape=(
            S((length, width), bf16), S((length, width), bf16), S((length, width), bf16),
            S((3, length, cols), bf16), S((length, cols), bf16), S((length, LANES), f32),
            S((tok, width), f32), S((3, width, cols), bf16), S((cols, width), bf16),
            S((8, width), f32), S((length, LANES), f32), S((length, LANES), f32), S((3, r, width), bf16),
        ),
        in_specs=[A, A, M, M, M, M, M, A, A, A, A],
        out_specs=[A] * 13,
        scratch_shapes=[
            V((length, width), bf16), V((length, width), bf16), V((8, LANES), f32), V((nf * ns, 8, LANES), f32),
            V((8, width), f32), V((3, width, cols), bf16), V((cols, width), bf16), V((3, length, cols), bf16),
            V((length, cols), bf16), V((length, LANES), f32), V((length, LANES), f32), V((length, LANES), f32),
            V((2 * tok, width), f32), V((m, tok, width), f32), V((m, tok, width), bf16),
            V((m, tok, width), bf16), V((m - 1, tok, width), bf16), V((tok, width), f32), V((tok, width), bf16),
            V((3, r, width), bf16),
            D((4,)), D((3 * pairs + 4,)), D((nf * ns,)), D((nf * ns,)),
        ] + [D((3 * pairs + 1, nf - 1))] * 4 + [D((3, nf - 1))] * 4 + ([D((2 * m,))] * 2 + [D((m,))] * 2) * 3 + [D((m,))] * 2 + [D((2 * m,))] * 2 + [D((11,))],
        compiler_params=pltpu.CompilerParams(
            collective_id=cid, has_side_effects=True, vmem_limit_bytes=64 * 1024 * 1024 - 65536),
        name="front",
    )(x, cot, g1, b1, g2, b2, qb, wqkv, wo, wgu, wd)


def back_kernel(nf, ns, left,
                gsum_hbm, osum_hbm, res_hbm, cot_hbm, x_hbm, vec_hbm, qkv_hbm, att_hbm, lse_hbm, in1_hbm, wq_hbm, wo_hbm,
                cos_hbm, sin_hbm, *more):
    if left:
        (rest_hbm, _, _, out_hbm, ig_hbm, gqkv_hbm, gout_hbm, o_g1, o_b1, o_g2, o_b2, o_qb, ggu_hbm, gd_hbm) = more[:14]
        (rest, rest_left, rest_right, rest_stage, rest_sems, q_sr, q_rr, q_sl, q_rl) = more[-9:]
        more = more[14:-9]
    else:
        (out_hbm, ig_hbm, gqkv_hbm, gout_hbm, o_g1, o_b1, o_g2, o_b2, o_qb) = more[:9]
        more = more[9:]
    (keep, res, cot, vec, qkv, att, lse, in1, wq, wo, cos, sin,
                grows, ga, gq, dk, dv, parts, from_left, from_right, stage, stage_t,
                g_sib, g_off, o_sib, o_off, i_sib, i_off, gres, sums, tiles,
                load_sems, keep_sems, in1_sems, small_s, small_r,
                rs_sr, rs_rr, rs_sl, rs_rl,
                w_so, w_ro, w_ss, w_rs,
                g_ss, g_rs, g_so, g_ro, o_ss, o_rs, o_so, o_ro, i_ss, i_rs, i_so, i_ro,
     stage_sems, out_sems) = more
    f, s = lax.axis_index("fsdp"), lax.axis_index("seq")
    total = nf * ns
    me = f * ns + s
    m = ns // 2
    j, c = s // 2, s % 2
    tok, width = cot.shape
    length, cols = att.shape
    wz = width // nf
    pairs = cols // LANES
    block_rows = 2 * tok
    count = 4 * pairs
    span = 768 if length <= 1024 else 256
    mine = pl.ds(pl.multiple_of(s * tok, tok), tok)

    def rows_at(ref, chip, core):
        return ref.at[pl.ds(pl.multiple_of((chip * 2 + core) * tok, tok), tok)]

    def keep_load(hbm, d, at):
        return pltpu.make_async_copy(rows_at(hbm, xor(j, d, m), c), keep.at[d], keep_sems.at[2 * d + at])

    for d in range(m - 1, -1, -1):
        keep_load(gsum_hbm, d, 0).start()
    plain = [(res_hbm, res), (cot_hbm, cot), (vec_hbm, vec), (wo_hbm, wo), (att_hbm, att), (qkv_hbm, qkv),
             (lse_hbm, lse), (wq_hbm, wq), (cos_hbm, cos), (sin_hbm, sin)]
    loads = [pltpu.make_async_copy(a, b, load_sems.at[i]) for i, (a, b) in enumerate(plain)]
    for load in loads:
        load.start()

    def in1_load(k):
        return pltpu.make_async_copy(in1_hbm.at[:, pl.ds(k * wz, wz)], in1.at[k % 2], in1_sems.at[k % 2])
    in1_load(0).start()
    if left:
        rest_load = pltpu.make_async_copy(rest_hbm, rest, rest_sems.at[0])
        rest_load.start()

    everyone_barrier(me, nf, ns)
    two = RowReduce(s, m, g_sib, g_off, (g_ss, g_rs, g_so, g_ro))
    out = RowReduce(s, m, o_sib, o_off, (o_ss, o_rs, o_so, o_ro))

    waiting = []
    if left:
        r = rest.shape[1]
        first_row = gd_hbm.shape[0] - left * r

        def rest_out(p, act):
            kind, sl = lax.rem(p, 3), lax.rem(p, 2)
            at = pl.ds(pl.multiple_of(first_row + p // 3 * r, 16), r)

            @pl.when(kind < 2)
            def _():
                act(pltpu.make_async_copy(rest_stage.at[sl], ggu_hbm.at[kind, at], rest_sems.at[sl]))

            @pl.when(kind == 2)
            def _():
                act(pltpu.make_async_copy(rest_stage.at[sl], gd_hbm.at[at], rest_sems.at[sl]))

        def rest_finish(p):
            @pl.when(p >= 2)
            def _():
                rest_out(p - 2, lambda cc: cc.wait())
            sl = lax.rem(p, 2)
            rest_stage[sl] = rest[p, :, pl.ds(pl.multiple_of(f * wz, wz), wz)].astype(f32)

            @pl.when(f > 0)
            def _():
                rest_stage[sl] += rest_left[p, jnp.maximum(f - 1, 0)].astype(f32)

            @pl.when(f < nf - 1)
            def _():
                rest_stage[sl] += rest_right[p, jnp.minimum(f, nf - 2)].astype(f32)
            rest_out(p, lambda cc: cc.start())

        rest_sum = LineReduce(f, nf, 3 * left, lambda p, k: rest.at[p, :, pl.ds(pl.multiple_of(k * wz, wz), wz)], rest_left, rest_right,
                              (q_sr, q_rr, q_sl, q_rl), rest_finish)
        waiting = list(range(3 * left + nf - 1))

    def rest_tick(how_many=1):
        for _ in range(how_many):
            if waiting:
                rest_sum.tick(jnp.int32(waiting.pop(0)))

    def two_src(d):
        return rows_at(gsum_hbm, xor(j, d, m), 1 - c)

    def out_src(d):
        return rows_at(osum_hbm, xor(j, d, m), 1 - c)

    for d in range(m - 1, -1, -1):
        two.give(d, two_src(d))
    if left:
        rest_load.wait()
    rest_tick()
    for d in range(m - 1, -1, -1):
        keep_load(gsum_hbm, d, 0).wait()
    for d in range(m - 1, 0, -1):
        two.pass_on(d, keep[d])
    two.forward()
    for d in range(m - 1, -1, -1):
        out.give(d, out_src(d))
    rest_tick()
    for load in loads[:3]:
        load.wait()
    sums[...] = jnp.zeros_like(sums)
    normed, inverse = normed_rows(res[...])
    grad = two.collect(keep[0])
    for d in range(m - 1, -1, -1):
        keep_load(osum_hbm, d, 1).start()
    sums[2:3, :] = jnp.sum(grad * normed, axis=0, keepdims=True)
    sums[3:4, :] = jnp.sum(grad, axis=0, keepdims=True)

    def norm_grad(grad, normed, inverse, gain):
        scaled = grad * gain
        return inverse * (scaled - jnp.mean(scaled, axis=-1, keepdims=True)
                          - normed * jnp.mean(scaled * normed, axis=-1, keepdims=True))

    gres[...] = cot[...].astype(f32) + norm_grad(grad, normed, inverse, vec[2:3, :])
    grows[mine, :] = gres[...].astype(bf16)
    x_load = pltpu.make_async_copy(x_hbm, cot, load_sems.at[len(plain)])
    x_load.start()
    rows_w = RowGather(s, m, tok, grows, (w_so, w_ro, w_ss, w_rs))
    rows_w.start(grows.at[mine])
    rest_tick()
    for load in loads[3:]:
        load.wait()

    def block(p, k):
        return parts.at[p, :, pl.ds(pl.multiple_of(k * wz, wz), wz)]

    def staged(p, act):
        sl = lax.rem(p, 2)

        @pl.when(p < pairs)
        def _():
            act(pltpu.make_async_copy(
                stage.at[sl], gout_hbm.at[pl.ds(pl.multiple_of(p * LANES, LANES), LANES)], stage_sems.at[sl]))

        @pl.when(p >= pairs)
        def _():
            q = p - pairs
            lanes = pl.ds(pl.multiple_of(q // 3 * LANES, LANES), LANES)
            act(pltpu.make_async_copy(stage_t.at[sl], gqkv_hbm.at[lax.rem(q, 3), :, lanes], stage_sems.at[sl]))

    def finish(p):
        @pl.when(p >= 2)
        def _():
            staged(p - 2, lambda cc: cc.wait())
        sl = lax.rem(p, 2)
        stage[sl] = parts[p, :, pl.ds(pl.multiple_of(f * wz, wz), wz)].astype(f32)

        @pl.when(f > 0)
        def _():
            stage[sl] += from_left[p, jnp.maximum(f - 1, 0)].astype(f32)

        @pl.when(f < nf - 1)
        def _():
            stage[sl] += from_right[p, jnp.minimum(f, nf - 2)].astype(f32)

        @pl.when(p >= pairs)
        def _():
            stage_t[sl] = stage[sl].T
        staged(p, lambda cc: cc.start())

    reduce = LineReduce(f, nf, count, block, from_left, from_right, (rs_sr, rs_rr, rs_sl, rs_rl), finish)

    def attend_back(b, g):
        lanes = pl.ds(pl.multiple_of(g * LANES, LANES), LANES)
        lane = lane_of((block_rows, LANES))
        seen = lane_of((block_rows, block_rows)) <= lax.broadcasted_iota(jnp.int32, (block_rows, block_rows), 0)
        rows = pl.ds(b * block_rows, block_rows)
        q = qkv[0, rows, lanes].astype(f32) * HEAD_DIM ** -0.5
        go = ga[rows, lanes].astype(f32)
        both = go * att[rows, lanes].astype(f32)
        logs = lse[rows, :]
        grad_q = jnp.zeros((block_rows, LANES), f32)
        for h in range(PER):
            head = lane // HEAD_DIM == h
            qm = jnp.where(head, q, 0.0).astype(bf16)
            gm = jnp.where(head, go, 0.0).astype(bf16)
            delta = jnp.sum(jnp.where(head, both, 0.0), axis=1, keepdims=True)
            log = jnp.sum(jnp.where(lane == g * PER + h, logs, 0.0), axis=1, keepdims=True)
            acc = jnp.zeros((block_rows, LANES), f32)
            spans = [(k, min(span, b * block_rows - k)) for k in range(0, b * block_rows, span)]
            for first, size in spans + [(b * block_rows, block_rows)]:
                at = pl.ds(first, size)
                key, val = qkv[1, at, lanes], qkv[2, at, lanes]
                pr = jnp.exp(dot_nt(qm, key) - log)
                if first == b * block_rows:
                    pr = jnp.where(seen, pr, 0.0)
                gp = dot_nt(gm, val)
                gs = (pr * (gp - delta)).astype(bf16)
                dv[at, :] += dot_tn(pr.astype(bf16), gm)
                dk[at, :] += dot_tn(gs, qm)
                acc = acc + dot_nn(gs, key)
            grad_q = jnp.where(head, acc * HEAD_DIM ** -0.5, grad_q)
        gq[0, rows, lanes] = turn(grad_q, cos[rows, :], sin[rows, :], -1.0).astype(bf16)

    def weight_pieces(g):
        lanes = pl.ds(pl.multiple_of(g * LANES, LANES), LANES)

        @pl.loop(0, m)
        def _(b):
            rows = pl.ds(pl.multiple_of(b * block_rows, block_rows), block_rows)
            gq[1, rows, lanes] = turn(dk[rows, :], cos[rows, :], sin[rows, :], -1.0).astype(bf16)
            gq[2, rows, lanes] = dv[rows, :].astype(bf16)
        at_once = 3 if length <= 1024 else 1
        wide = [[gq[i, :, lanes] for i in range(3)]] if at_once == 3 else [[gq[i, :, lanes]] for i in range(3)]
        at = pl.ds(pl.multiple_of(s * cols + g * LANES, LANES), LANES)
        for k in range(3):
            sums[4 + k:5 + k, at] = jnp.sum(gq[k, :, lanes].astype(f32), axis=0, keepdims=True)
        for k in range(nf):
            in1_load(k).wait()
            in1_load((k + 1) % nf).start()
            for n, some in enumerate(wide):
                value = dot_tn(jnp.concatenate(some, axis=1), in1[k % 2]).astype(bf16)
                for i in range(at_once):
                    parts[pairs + 3 * g + n + i, :, k * wz:(k + 1) * wz] = value[i * LANES:(i + 1) * LANES, :]

    @pl.loop(0, pairs * m)
    def _(turn_here):
        g, step = turn_here // m, lax.rem(turn_here, m)
        chip = xor(j, step, m)
        rows = pl.ds(pl.multiple_of(chip * block_rows, block_rows), block_rows)

        @pl.when(step == 0)
        def _():
            dk[...] = jnp.zeros_like(dk)
            dv[...] = jnp.zeros_like(dv)
        for d in range(m):
            @pl.when((g == 0) & (step == d))
            def _(d=d):
                if d > 0:
                    rows_w.relay(d)
                rows_w.arrived(d)
                if d > 0:
                    rest_tick()

        @pl.when(g == 0)
        def _():
            ga[rows, :] = dot_nt(grows[rows, :], wo[...]).astype(bf16)

        @pl.when((g == 0) & (step == m - 1))
        def _():
            for d in range(m - 1, -1, -1):
                keep_load(osum_hbm, d, 1).wait()
            for d in range(m - 1, 0, -1):
                out.pass_on(d, keep[d])
            for k in range(nf):
                lanes = slice(k * wz, (k + 1) * wz)
                value = dot_tn(att[...], grows[:, lanes]).astype(bf16)
                for i in range(pairs):
                    parts[i, :, lanes] = value[i * LANES:(i + 1) * LANES, :]
            rest_tick(len(waiting))
            reduce.tick(jnp.int32(0))
        for b in range(m):
            @pl.when(chip == b)
            def _(b=b):
                attend_back(b, g)

        @pl.when((g > 0) & (step % (m // 2) == m // 2 - 1))
        def _():
            reduce.tick(pairs + 3 * (g - 1) + 1 + (step + 1) // (m // 2) - 1)

        @pl.when((g == pairs - 1) & (step == m - 1))
        def _():
            out.forward()

        @pl.when(step == m - 1)
        def _():
            @pl.when(g == 0)
            def _():
                for p in range(1, pairs):
                    reduce.tick(jnp.int32(p))
            weight_pieces(g)
            reduce.tick(pairs + 3 * g)
    in1_load(0).wait()

    keep[0] = (res[...] + out.collect(keep[0])).astype(bf16)
    stores = [pltpu.make_async_copy(keep.at[0], out_hbm, out_sems.at[0])]
    stores[0].start()
    out.drain(out_src)
    one = RowReduce(s, m, i_sib, i_off, (i_ss, i_rs, i_so, i_ro))
    rows_w.drain(grows.at[mine])

    def half_of(d, core):
        return grows.at[pl.ds(pl.multiple_of((2 * d + core) * tok, tok), tok)]

    late = list(range(pairs + 3 * (pairs - 1) + 1, count + nf - 1))
    for d in range(m - 1, -1, -1):
        rows = pl.ds(pl.multiple_of(xor(j, d, m) * block_rows, block_rows), block_rows)
        value = dot_nt(gq[0, rows, :], wq[0])
        for k in (1, 2):
            value = value + dot_nt(gq[k, rows, :], wq[k])
        grows[d * block_rows:(d + 1) * block_rows, :] = value.astype(bf16)
        one.give(d, half_of(d, 1 - c))
        if d < m - 1:
            one.pass_on(d + 1, half_of(d + 1, c)[...])
        if late and d % 2 == 1:
            reduce.tick(jnp.int32(late.pop(0)))
    grad = one.total(half_of(0, c)[...])
    x_load.wait()
    normed, inverse = normed_rows(cot[...].astype(f32))
    sums[0:1, :] = jnp.sum(grad * normed, axis=0, keepdims=True)
    sums[1:2, :] = jnp.sum(grad, axis=0, keepdims=True)
    res[...] = gres[...] + norm_grad(grad, normed, inverse, vec[0:1, :])
    stores.append(pltpu.make_async_copy(res, ig_hbm, out_sems.at[1]))
    stores[1].start()

    w = o_g1.shape[1]
    spread = LANES // w

    def tile_of(t):
        return sums.at[:, pl.ds(pl.multiple_of(t // spread * LANES, LANES), LANES)]

    def small(k):
        t = lax.rem(me + k, total)
        return remote(tile_of(t), tiles.at[k], small_s.at[k], small_r.at[k],
                      {"fsdp": t // ns, "seq": lax.rem(t, ns)})

    @pl.loop(1, total)
    def _(k):
        small(k).start()
    @pl.loop(late[0], late[-1] + 1)
    def _(t):
        reduce.tick(t)
    tiles[0] = tile_of(me)[...]

    @pl.loop(1, total)
    def _(k):
        small(k).wait_recv()
        tiles[0] += tiles[k]
    for k in range(spread):
        @pl.when(lax.rem(me, spread) == k)
        def _(k=k):
            lanes = slice(k * w, (k + 1) * w)
            for i, ref in enumerate((o_g1, o_b1, o_g2, o_b2)):
                ref[...] = tiles[0, i:i + 1, lanes]
            o_qb[...] = tiles[0, 4:7, lanes]

    @pl.loop(1, total)
    def _(k):
        small(k).wait_send()
    two.drain(two_src)
    one.drain(lambda d: half_of(d, 1 - c))
    for p in (count - 2, count - 1):
        staged(jnp.int32(p), lambda cc: cc.wait())
    for st in stores:
        st.wait()
    if left:
        for p in (3 * left - 2, 3 * left - 1):
            rest_out(jnp.int32(p), lambda cc: cc.wait())


def back(gsum, osum, res, cot, x, vec, qkv, att, lse, in1, wq, wo, cos, sin, rest, ggu, gd, nf, ns, cid):
    left = 0 if rest is None else rest.shape[0] // 3
    tok, width = x.shape
    length, cols = att.shape
    wz = width // nf
    m = ns // 2
    w = width // (nf * ns)
    pairs = cols // LANES
    count = 4 * pairs
    D, V = pltpu.SemaphoreType.DMA, pltpu.VMEM
    A = pl.BlockSpec(memory_space=pl.ANY)
    M = pl.BlockSpec(memory_space=pltpu.VMEM)
    S = jax.ShapeDtypeStruct
    extra_in, extra_out, extra_scratch = (), (), []
    if left:
        r = rest.shape[1]
        extra_in = (rest, ggu, gd)
        extra_out = (S(ggu.shape, f32), S(gd.shape, f32))
        extra_scratch = [V((3 * left, r, width), bf16), V((3 * left, nf - 1, r, wz), bf16),
                         V((3 * left, nf - 1, r, wz), bf16), V((2, r, wz), f32), D((2,))] + [D((3 * left, nf - 1))] * 4
    rows_v = V((m, tok, width), bf16)
    offs_v = V((m - 1, tok, width), bf16)
    return pl.pallas_call(
        functools.partial(back_kernel, nf, ns, left),
        out_shape=(
            S((tok, width), bf16), S((tok, width), f32), S((3, wz, cols), f32), S((cols, wz), f32),
            S((1, w), f32), S((1, w), f32), S((1, w), f32), S((1, w), f32), S((3, w), f32),
        ) + extra_out,
        in_specs=[A] * (14 + len(extra_in)),
        out_specs=[A] * 4 + [M] * 5 + [A] * len(extra_out),
        input_output_aliases={15: 9, 16: 10} if left else {},
        scratch_shapes=[
            rows_v, V((tok, width), f32), V((tok, width), bf16), V((8, width), f32),
            V((3, length, cols), bf16), V((length, cols), bf16), V((length, LANES), f32), V((2, length, wz), bf16),
            V((3, width, cols), bf16), V((cols, width), bf16), V((length, LANES), f32), V((length, LANES), f32),
            V((length, width), bf16), V((length, cols), bf16), V((3, length, cols), bf16),
            V((length, LANES), f32), V((length, LANES), f32),
            V((count, LANES, width), bf16), V((count, nf - 1, LANES, wz), bf16), V((count, nf - 1, LANES, wz), bf16),
            V((2, LANES, wz), f32), V((2, wz, LANES), f32),
            rows_v, offs_v, rows_v, offs_v, rows_v, offs_v,
            V((tok, width), f32),
            V((8, width), f32), V((nf * ns, 8, LANES), f32),
            D((11,)), D((2 * m,)), D((2,)), D((nf * ns,)), D((nf * ns,)),
        ] + [D((count, nf - 1))] * 4 + [D((2 * m,))] * 2 + [D((m,))] * 2 + [D((m,)), D((m,)), D((2 * m,)), D((2 * m,))] * 3 + [D((2,)), D((2,))]
        + extra_scratch,
        compiler_params=pltpu.CompilerParams(
            collective_id=cid, has_side_effects=True, vmem_limit_bytes=64 * 1024 * 1024 - 65536),
        name="back",
    )(gsum, osum, res, cot, x, vec, qkv, att, lse, in1, wq, wo, cos, sin, *extra_in)


def local(
    block_input,
    cotangent,
    ln1_gain,
    ln1_bias,
    qkv_weight,
    qkv_bias,
    out_weight,
    ln2_gain,
    ln2_bias,
    gate_up_weight,
    down_weight,
):
    fsdp, seq = lax.axis_size("fsdp"), lax.axis_size("seq")
    gate_up = jnp.transpose(gate_up_weight, (1, 2, 0))
    left = 1 if seq * block_input.shape[1] <= 1024 else 0
    (in_one, cot_all, in_two, qkv, mixed, logs, residual, qkv_full, out_full, vectors, cosine, sine, first) = front(
        block_input[0],
        cotangent[0],
        ln1_gain[None],
        ln1_bias[None],
        ln2_gain[None],
        ln2_bias[None],
        qkv_bias,
        jnp.transpose(qkv_weight, (1, 0, 2)),
        out_weight,
        gate_up,
        down_weight,
        fsdp,
        seq,
        1,
    )
    out_sum, grad_sum, grad_gate_up, grad_down, *rest = mlp(
        in_two, cot_all, first, gate_up, down_weight, fsdp, left, 0
    )
    block_output, input_grad, grad_qkv, grad_out, gain_one, bias_one, gain_two, bias_two, grad_bias, *grads = back(
        grad_sum,
        out_sum,
        residual,
        cotangent[0],
        block_input[0],
        vectors,
        qkv,
        mixed,
        logs,
        in_one,
        qkv_full,
        out_full,
        cosine,
        sine,
        rest[0] if left else None,
        grad_gate_up,
        grad_down,
        fsdp,
        seq,
        2,
    )
    if left:
        grad_gate_up, grad_down = grads
    return (
        block_output[None],
        input_grad[None],
        gain_one[0],
        bias_one[0],
        jnp.transpose(grad_qkv, (1, 0, 2)),
        grad_bias,
        grad_out,
        gain_two[0],
        bias_two[0],
        jnp.transpose(grad_gate_up, (2, 0, 1)),
        grad_down,
    )


def solution(mesh):
    placed = (
        P("fsdp", "seq", None),
        P("fsdp", "seq", None),
        P(("fsdp", "seq")),
        P(("fsdp", "seq")),
        P("fsdp", None, "seq"),
        P(None, ("fsdp", "seq")),
        P("seq", "fsdp"),
        P(("fsdp", "seq")),
        P(("fsdp", "seq")),
        P("fsdp", None, "seq"),
        P("seq", "fsdp"),
    )
    return jax.shard_map(
        local,
        mesh=mesh,
        in_specs=placed,
        out_specs=(
            P("fsdp", "seq", None),
            P("fsdp", "seq", None),
            P(("fsdp", "seq")),
            P(("fsdp", "seq")),
            P("fsdp", None, "seq"),
            P(None, ("fsdp", "seq")),
            P("seq", "fsdp"),
            P(("fsdp", "seq")),
            P(("fsdp", "seq")),
            P("fsdp", None, "seq"),
            P("seq", "fsdp"),
        ),
        check_vma=False,
    )
```

```python
import functools

import jax
import jax.numpy as jnp
from jax import lax
from jax.experimental import pallas as pl
from jax.experimental.pallas import tpu as pltpu
from jax.sharding import PartitionSpec as P

HEAD_DIM = 64
ROTARY = 16

epsilon = 1e-05
masked_score = -1e30

MESH = pl.DeviceIdType.MESH
NT = (((1,), (1,)), ((), ()))
TN = (((0,), (0,)), ((), ()))
f32, bf16 = jnp.float32, jnp.bfloat16


def dot_nn(a, b):
    return jnp.dot(a, b, preferred_element_type=f32)


def dot_nt(a, b):
    return lax.dot_general(a, b, NT, preferred_element_type=f32)


def dot_tn(a, b):
    return lax.dot_general(a, b, TN, preferred_element_type=f32)


def remote(src, dst, send_sem, recv_sem, device):
    return pltpu.make_async_remote_copy(
        src_ref=src, dst_ref=dst, send_sem=send_sem, recv_sem=recv_sem,
        device_id=device, device_id_type=MESH)


def line_barrier(f, n):
    barrier = pltpu.get_barrier_semaphore()

    @pl.when(f > 0)
    def _():
        pl.semaphore_signal(barrier, inc=1, device_id={"fsdp": f - 1}, device_id_type=MESH)

    @pl.when(f < n - 1)
    def _():
        pl.semaphore_signal(barrier, inc=1, device_id={"fsdp": f + 1}, device_id_type=MESH)

    pl.semaphore_wait(barrier, (f > 0).astype(jnp.int32) + (f < n - 1).astype(jnp.int32))


def when(condition):
    if isinstance(condition, (bool, int)):
        return (lambda body: body()) if condition else (lambda body: None)
    return pl.when(condition)


class LineGather:
    def __init__(self, f, n, count, own, slot, sems):
        self.f, self.n, self.count, self.own, self.slot = f, n, count, own, slot
        self.send_r, self.recv_r, self.send_l, self.recv_l = sems

    def copy(self, src, p, h, source, rightward):
        f = self.f
        send, recv = (self.send_r, self.recv_r) if rightward else (self.send_l, self.recv_l)
        target = f + 1 if rightward else f - 1
        return remote(src, self.slot(p, source), send.at[p, h], recv.at[p, h], {"fsdp": target})

    def send_own(self, t):
        f, n = self.f, self.n

        @when((t >= 0) & (t < self.count))
        def _():
            @pl.when(f < n - 1)
            def _():
                self.own(t, lambda src: self.copy(src, t, 0, f, True).start())

            @pl.when(f > 0)
            def _():
                self.own(t, lambda src: self.copy(src, t, 0, f, False).start())

    def arrivals(self, t):
        for h in range(self.n - 1, 0, -1):
            self.arrive(t - h, h)

    def tick(self, t):
        self.send_own(t)
        self.arrivals(t)

    def arrive(self, p, h):
        f, n = self.f, self.n

        @when((p >= 0) & (p < self.count))
        def _():
            @pl.when(f - h >= 0)
            def _():
                here = self.slot(p, f - h)
                self.copy(here, p, h - 1, f - h, True).wait_recv()
                if h < n - 1:
                    @pl.when(f < n - 1)
                    def _():
                        self.copy(here, p, h, f - h, True).start()

            @pl.when(f + h <= n - 1)
            def _():
                here = self.slot(p, f + h)
                self.copy(here, p, h - 1, f + h, False).wait_recv()
                if h < n - 1:
                    @pl.when(f > 0)
                    def _():
                        self.copy(here, p, h, f + h, False).start()

    def drain(self, p):
        f, n = self.f, self.n
        for h in range(0, n - 1):
            @pl.when((f - h >= 0) & (f < n - 1))
            def _(h=h):
                self.copy(self.slot(p, f - h), p, h, f - h, True).wait_send()

            @pl.when((f + h <= n - 1) & (f > 0))
            def _(h=h):
                self.copy(self.slot(p, f + h), p, h, f + h, False).wait_send()


class LineReduce:
    def __init__(self, f, n, count, block, from_left, from_right, sems, finish):
        self.f, self.n, self.count, self.block = f, n, count, block
        self.from_left, self.from_right, self.finish = from_left, from_right, finish
        self.send_r, self.recv_r, self.send_l, self.recv_l = sems

    def right(self, p, j):
        return remote(self.block(p, j), self.from_left.at[p, j - 1], self.send_r.at[p, j - 1],
                      self.recv_r.at[p, j - 1], {"fsdp": self.f + 1})

    def left(self, p, j):
        return remote(self.block(p, j), self.from_right.at[p, j], self.send_l.at[p, j],
                      self.recv_l.at[p, j], {"fsdp": self.f - 1})

    def tick(self, u):
        f, n, count = self.f, self.n, self.count
        p = u - f

        @pl.when((p >= 0) & (p < count))
        def _():
            @pl.loop(0, n - 1)
            def _(i):
                j = n - 1 - i

                @pl.when((f > 0) & (j >= f))
                def _():
                    self.right(p, j).wait_recv()

                @pl.when((f > 0) & (j > f))
                def _():
                    here = self.block(p, j)
                    here[...] = (here[...].astype(f32) + self.from_left[p, j - 1].astype(f32)).astype(bf16)

                @pl.when(j > f)
                def _():
                    self.right(p, j).start()

        q = u - (n - 1 - f)

        @pl.when((q >= 0) & (q < count))
        def _():
            @pl.loop(0, n - 1)
            def _(j):
                @pl.when((f < n - 1) & (j <= f))
                def _():
                    self.left(q, j).wait_recv()

                @pl.when((f < n - 1) & (j < f))
                def _():
                    here = self.block(q, j)
                    here[...] = (here[...].astype(f32) + self.from_right[q, j].astype(f32)).astype(bf16)

                @pl.when(j < f)
                def _():
                    self.left(q, j).start()

        e = u - (n - 1)

        @pl.when((e >= 0) & (e < count))
        def _():
            @pl.loop(0, n)
            def _(j):
                @pl.when(j > f)
                def _():
                    self.right(e, j).wait_send()

                @pl.when(j < f)
                def _():
                    self.left(e, j).wait_send()
            self.finish(e)


def mlp_kernel(n, r, rb, head, left, in2_hbm, cot_hbm, w0_hbm, wgu_hbm, wd_hbm,
               out_hbm, gin_hbm, ggu_hbm, gd_hbm, *more):
    rest_hbm, more = (more[0], more[1:]) if left else (None, more)
    (in2, cot, acc_o, acc_g, w, hid, dga, dup, parts, from_left, from_right,
               stage, load_sems, own_sems, ag_sr, ag_rr, ag_sl, ag_rl, rs_sr, rs_rr, rs_sl, rs_rl,
               stage_sems, rest_sems) = more
    f = lax.axis_index("fsdp")
    tokens, width = in2.shape
    wz = width // n
    ff = wd_hbm.shape[0]
    nc = ff // r
    count = 3 * nc
    summed = count - left
    ahead = max(n - 1, 3)
    ring = parts.shape[0]
    loads = [pltpu.make_async_copy(in2_hbm, in2, load_sems.at[0]),
             pltpu.make_async_copy(cot_hbm, cot, load_sems.at[1]),
             pltpu.make_async_copy(w0_hbm, w.at[pl.ds(0, head)], load_sems.at[2])]
    for c in loads:
        c.start()

    def rows_of(p):
        return pl.ds(pl.multiple_of(p // 3 * r, r), r)

    def own(p, use):
        kind = lax.rem(p, 3)

        @pl.when(kind < 2)
        def _():
            use(wgu_hbm.at[kind, rows_of(p)])

        @pl.when(kind == 2)
        def _():
            use(wd_hbm.at[rows_of(p)])

    def slot(p, source):
        return w.at[p, :, pl.ds(pl.multiple_of(source * wz, wz), wz)]

    def own_copy(p, act):
        own(p, lambda src: act(pltpu.make_async_copy(src, slot(p, f), own_sems.at[p])))

    @pl.loop(head, count)
    def _(p):
        own_copy(p, lambda c: c.start())

    line_barrier(f, n)
    gather = LineGather(f, n, count - head, lambda p, use: own(p + head, use), lambda p, source: slot(p + head, source),
                        (ag_sr, ag_rr, ag_sl, ag_rl))

    def block(p, j):
        return parts.at[lax.rem(p, ring), :, pl.ds(pl.multiple_of(j * wz, wz), wz)]

    def stage_out(p, act):
        kind = lax.rem(p, 3)
        sl = lax.rem(p, 2)

        @pl.when(kind < 2)
        def _():
            act(pltpu.make_async_copy(stage.at[sl], ggu_hbm.at[kind, rows_of(p)], stage_sems.at[sl]))

        @pl.when(kind == 2)
        def _():
            act(pltpu.make_async_copy(stage.at[sl], gd_hbm.at[rows_of(p)], stage_sems.at[sl]))

    def finish(p):
        @pl.when(p >= 2)
        def _():
            stage_out(p - 2, lambda c: c.wait())
        sl = lax.rem(p, 2)
        mine = parts.at[lax.rem(p, ring), :, pl.ds(pl.multiple_of(f * wz, wz), wz)]
        stage[sl] = mine[...].astype(f32)

        @pl.when(f > 0)
        def _():
            stage[sl] += from_left[p, jnp.maximum(f - 1, 0)].astype(f32)

        @pl.when(f < n - 1)
        def _():
            stage[sl] += from_right[p, jnp.minimum(f, n - 2)].astype(f32)
        stage_out(p, lambda c: c.start())

    reduce = LineReduce(f, n, summed, block, from_left, from_right, (rs_sr, rs_rr, rs_sl, rs_rl), finish)

    acc_o[...] = jnp.zeros_like(acc_o)
    acc_g[...] = jnp.zeros_like(acc_g)

    for t in range(3):
        gather.send_own(t)

    for c in loads:
        c.wait()

    def compute(c):
        @pl.when(c > 0)
        def _():
            for k in range(3):
                @pl.when(3 * c + k >= head)
                def _(k=k):
                    own_copy(3 * c + k, lambda cc: cc.wait())

        @pl.loop(0, tokens // rb)
        def _(i):
            rows = pl.ds(pl.multiple_of(i * rb, rb), rb)
            a = in2[rows, :]
            gate = dot_nt(a, w[3 * c])
            up = dot_nt(a, w[3 * c + 1])
            gh = dot_nt(cot[rows, :], w[3 * c + 2])
            sig = jax.nn.sigmoid(gate)
            silu = gate * sig
            h = (silu * up).astype(bf16)
            dg = (gh * up * sig * (1.0 + gate * (1.0 - sig))).astype(bf16)
            du = (gh * silu).astype(bf16)
            hid[rows, :] = h
            dga[rows, :] = dg
            dup[rows, :] = du
            acc_o[rows, :] = (acc_o[rows, :].astype(f32) + dot_nn(h, w[3 * c + 2])).astype(acc_o.dtype)
            acc_g[rows, :] = (acc_g[rows, :].astype(f32) + dot_nn(dg, w[3 * c]) + dot_nn(du, w[3 * c + 1])).astype(acc_g.dtype)

    @pl.loop(0, nc)
    def _(c):
        compute(c)

        @pl.when(c == 0)
        def _():
            gather.arrivals(1)
        for k, (small, big) in enumerate(((dga, in2), (dup, in2), (hid, cot))):
            @pl.loop(0, n)
            def _(j, k=k, small=small, big=big):
                lanes = pl.ds(pl.multiple_of(j * wz, wz), wz)
                block(3 * c + k, j)[...] = dot_tn(small[...], big[:, lanes]).astype(bf16)

            reduce.tick(3 * c + k)
            after = k + ahead - (head - 3)
            if k == 0:
                @pl.when(c == 0)
                def _():
                    for t in range(2, after + 1):
                        gather.arrivals(t) if t < 3 else gather.tick(t)

                @pl.when(c > 0)
                def _():
                    gather.tick(3 * c + after)
            else:
                gather.tick(3 * c + after)

    in2[...] = acc_o[...].astype(bf16)
    cot[...] = acc_g[...].astype(bf16)
    stores = [pltpu.make_async_copy(in2, out_hbm, load_sems.at[0]),
              pltpu.make_async_copy(cot, gin_hbm, load_sems.at[1])]
    for k in range(left):
        stores.append(pltpu.make_async_copy(parts.at[(summed + k) % ring], rest_hbm.at[k], rest_sems.at[k]))
    for c in stores:
        c.start()

    if left == 0:
        @pl.loop(count, summed + n - 1)
        def _(u):
            reduce.tick(u)

    @pl.loop(0, count - head)
    def _(p):
        gather.drain(p)
    for p in (summed - 2, summed - 1):
        stage_out(jnp.int32(p), lambda c: c.wait())
    for c in stores:
        c.wait()


def piece_rows(ff):
    r = 0
    for cand in range(16, 257, 16):
        if ff % cand == 0:
            r = cand
    return r


def mlp(in2, cot, w0, wgu, wd, n, left, cid):
    head = w0.shape[0]
    tokens, width = in2.shape
    ff, wz = wd.shape
    r = piece_rows(ff)
    rb = min(256, tokens)
    nc = ff // r
    count = 3 * nc
    ring = min(count, 3 * max((n - 1 + 2) // 3, (left + 2) // 3) + 3)
    any_spec = pl.BlockSpec(memory_space=pl.ANY)
    acc_dtype = f32 if tokens * width * 8 <= 20 * 2**20 else bf16
    D = pltpu.SemaphoreType.DMA
    return pl.pallas_call(
        functools.partial(mlp_kernel, n, r, rb, head, left),
        out_shape=(
            jax.ShapeDtypeStruct((tokens, width), bf16),
            jax.ShapeDtypeStruct((tokens, width), bf16),
            jax.ShapeDtypeStruct((2, ff, wz), f32),
            jax.ShapeDtypeStruct((ff, wz), f32),
        ) + (jax.ShapeDtypeStruct((left, r, width), bf16),) * min(left, 1),
        in_specs=[any_spec] * 5,
        out_specs=[any_spec] * (4 + min(left, 1)),
        scratch_shapes=[
            pltpu.VMEM((tokens, width), bf16),
            pltpu.VMEM((tokens, width), bf16),
            pltpu.VMEM((tokens, width), acc_dtype),
            pltpu.VMEM((tokens, width), acc_dtype),
            pltpu.VMEM((count, r, width), bf16),
            pltpu.VMEM((tokens, r), bf16),
            pltpu.VMEM((tokens, r), bf16),
            pltpu.VMEM((tokens, r), bf16),
            pltpu.VMEM((ring, r, width), bf16),
            pltpu.VMEM((count - left, n - 1, r, wz), bf16),
            pltpu.VMEM((count - left, n - 1, r, wz), bf16),
            pltpu.VMEM((2, r, wz), f32),
            D((3,)),
            D((count,)),
        ] + [D((count - head, n - 1))] * 4 + [D((count - left, n - 1))] * 4 + [D((2,)), D((max(left, 1),))],
        compiler_params=pltpu.CompilerParams(
            collective_id=cid, has_side_effects=True, vmem_limit_bytes=64 * 1024 * 1024 - 65536),
        name="mlp",
    )(in2, cot, w0, wgu, wd)


LANES = 128
HEAD_PIECES = 4
PER = LANES // HEAD_DIM


def xor(a, b, count):
    total = 0
    bit = 1
    while bit < count:
        x, y = (a // bit) % 2, (b // bit) % 2
        total = total + bit * (x + y - 2 * x * y)
        bit *= 2
    return total


def everyone_barrier(me, nf, ns):
    barrier = pltpu.get_barrier_semaphore()
    total = nf * ns

    @pl.loop(1, total)
    def _(k):
        t = lax.rem(me + k, total)
        pl.semaphore_signal(barrier, inc=1, device_id={"fsdp": t // ns, "seq": lax.rem(t, ns)},
                            device_id_type=MESH)
    pl.semaphore_wait(barrier, total - 1)


class RowGather:
    def __init__(self, s, m, tok, buf, sems):
        self.j, self.c, self.m, self.tok, self.buf = s // 2, s % 2, m, tok, buf
        self.send_o, self.recv_o, self.send_s, self.recv_s = sems
        self.square = m == 4

    def slot(self, chip, core, part=None):
        row = (chip * 2 + core) * self.tok
        if part is None:
            return self.buf.at[pl.ds(pl.multiple_of(row, self.tok), self.tok)]
        half = self.tok // 2
        return self.buf.at[pl.ds(pl.multiple_of(row + part * half, half), half)]

    def off(self, src, d, chip):
        return remote(src, self.slot(chip, self.c), self.send_o.at[d], self.recv_o.at[d],
                      {"seq": xor(self.j, d, self.m) * 2 + self.c})

    def part_of(self, src, d, part):
        half = self.tok // 2
        return remote(src.at[pl.ds(part * half, half)], self.slot(self.j, self.c, part),
                      self.send_o.at[2 * d + part], self.recv_o.at[2 * d + part],
                      {"seq": xor(self.j, d, 4) * 2 + self.c})

    def half(self, part, source, to, index):
        here = self.slot(xor(self.j, source, 4), self.c, part)
        return remote(here, here, self.send_o.at[index], self.recv_o.at[index],
                      {"seq": xor(self.j, to, 4) * 2 + self.c})

    def sib(self, src, d, core):
        return remote(src, self.slot(xor(self.j, d, self.m), core), self.send_s.at[d], self.recv_s.at[d],
                      {"seq": self.j * 2 + 1 - self.c})

    def start(self, src):
        if self.square:
            for d, part in ((1, 0), (2, 1), (1, 1), (2, 0)):
                self.part_of(src, d, part).start()
        else:
            for d in range(1, self.m):
                self.off(src, d, self.j).start()
        self.sib(src, 0, self.c).start()

    def relay(self, d):
        chip = xor(self.j, d, self.m)
        here = self.slot(chip, self.c)
        if not self.square:
            self.off(here, d, chip).wait_recv()
        elif d == 3:
            self.half(0, 3, 2, 6).wait_recv()
            self.half(1, 3, 1, 7).wait_recv()
        else:
            if d == 1:
                for n in (1, 2):
                    self.half(n - 1, n, n, 3 * n - 1).wait_recv()
                    self.half(n - 1, n, 3 - n, 5 + n).start()
            self.half(2 - d, d, d, d + 2).wait_recv()
        self.sib(here, d, self.c).start()

    def arrived(self, d):
        self.sib(self.slot(xor(self.j, d, self.m), 1 - self.c), d, 1 - self.c).wait_recv()

    def finish(self):
        for d in range(self.m):
            self.arrived(d)

    def drain(self, src):
        for d in range(1, self.m):
            if not self.square:
                self.off(src, d, self.j).wait_send()
            elif d < 3:
                for part in range(2):
                    self.part_of(src, d, part).wait_send()
                self.half(d - 1, d, 3 - d, 5 + d).wait_send()
            self.sib(self.slot(xor(self.j, d, self.m), self.c), d, self.c).wait_send()
        self.sib(src, 0, self.c).wait_send()


class RowReduce:
    def __init__(self, s, m, from_sib, from_off, sems):
        self.j, self.c, self.m = s // 2, s % 2, m
        self.from_sib, self.from_off = from_sib, from_off
        self.send_s, self.recv_s, self.send_o, self.recv_o = sems
        self.square = m == 4
        self.tok = from_sib.shape[1]

    def sib(self, src, d):
        return remote(src, self.from_sib.at[d], self.send_s.at[d], self.recv_s.at[d],
                      {"seq": self.j * 2 + 1 - self.c})

    def off(self, d):
        return remote(self.from_sib.at[d], self.from_off.at[d - 1], self.send_o.at[d], self.recv_o.at[d],
                      {"seq": xor(self.j, d, self.m) * 2 + self.c})

    def half(self, d, part):
        at = pl.ds(part * (self.tok // 2), self.tok // 2)
        last = d // 3
        to = d * (1 - last) + (part + 1) * last
        index = 2 * d + part
        return remote(self.from_sib.at[d, at], self.from_off.at[d - 1, at], self.send_o.at[index], self.recv_o.at[index],
                      {"seq": xor(self.j, to, 4) * 2 + self.c})

    def give(self, d, src):
        self.sib(src, d).start()

    def pass_on(self, d, own):
        here = self.from_sib.at[d]
        self.sib(here, d).wait_recv()
        here[...] = (own.astype(f32) + here[...].astype(f32)).astype(bf16)
        if not self.square:
            self.off(d).start()
            return
        for part in range(2):
            @when((d == 3) | (part == d - 1))
            def _(part=part):
                self.half(d, part).start()

    def forward(self):
        if self.square:
            for part, d in ((0, 2), (1, 1)):
                at = pl.ds(part * (self.tok // 2), self.tok // 2)
                self.half(3, part).wait_recv()
                self.from_sib[d, at] = (self.from_sib[d, at].astype(f32) + self.from_off[2, at].astype(f32)).astype(bf16)
                self.half(d, part).start()

    def collect(self, own):
        here = self.from_sib.at[0]
        self.sib(here, 0).wait_recv()
        value = own.astype(f32) + here[...].astype(f32)
        for d in (1, 2) if self.square else range(self.m - 1, 0, -1):
            if self.square:
                self.half(d, 0).wait_recv()
                self.half(d, 1).wait_recv()
            else:
                self.off(d).wait_recv()
            value = value + self.from_off[d - 1].astype(f32)
        return value

    def total(self, own):
        self.forward()
        return self.collect(own)

    def drain(self, src_of):
        for d in range(self.m):
            self.sib(src_of(d), d).wait_send()
        for d in range(1, self.m):
            if self.square:
                self.half(d, 0).wait_send()
                self.half(d, 1).wait_send()
            else:
                self.off(d).wait_send()


def normed_rows(x):
    center = x - jnp.mean(x, axis=-1, keepdims=True)
    inverse = lax.rsqrt(jnp.mean(center * center, axis=-1, keepdims=True) + epsilon)
    return center * inverse, inverse


def lane_of(shape):
    return lax.broadcasted_iota(jnp.int32, shape, len(shape) - 1)


def rotary_tiles(rows, first):
    half = ROTARY // 2
    lane = lane_of((rows, LANES))
    pos = (first + lax.broadcasted_iota(jnp.int32, (rows, LANES), 0)).astype(f32)
    within = lane % HEAD_DIM
    freq = jnp.zeros((rows, LANES), f32)
    for i in range(half):
        freq = jnp.where(within % half == i, float(10000.0 ** (-2.0 * i / ROTARY)), freq)
    angle = pos * freq
    turned = within < ROTARY
    cosine = jnp.where(turned, jnp.cos(angle), 1.0)
    sine = jnp.where(turned, jnp.sin(angle), 0.0)
    return cosine, sine


def turn(u, cosine, sine, direction):
    half = ROTARY // 2
    within = lane_of(u.shape) % HEAD_DIM
    ahead = pltpu.roll(u, LANES - half, 1)
    behind = pltpu.roll(u, half, 1)
    turned = jnp.where(within < half, -ahead, behind)
    return u * cosine + direction * turned * sine


def front_kernel(nf, ns,
                 x_hbm, cot_hbm, g1, b1, g2, b2, qb, wqkv_hbm, wo_hbm, wgu_hbm, wd_hbm,
                 in1_hbm, cotall_hbm, in2_hbm, qkv_hbm, att_hbm, lse_hbm, res_hbm, wq_hbm, woall_hbm,
                 vec_hbm, cos_hbm, sin_hbm, w0_hbm,
                 xall, in1, tile, tiles, vecs, wq, wo, qkv, att, lse, cos, sin, part, keep, give,
                 from_sib, from_off, res, in2, w0,
                 load_sems, own_sems, small_s, small_r,
                 ag_sr, ag_rr, ag_sl, ag_rl, m_sr, m_rr, m_sl, m_rl,
                 a_so, a_ro, a_ss, a_rs, c_so, c_ro, c_ss, c_rs, e_so, e_ro, e_ss, e_rs,
                 r_ss, r_rs, r_so, r_ro, out_sems):
    f, s = lax.axis_index("fsdp"), lax.axis_index("seq")
    total = nf * ns
    me = f * ns + s
    m = ns // 2
    j, c = s // 2, s % 2
    tok, width = x_hbm.shape
    length = in1.shape[0]
    cols = qkv.shape[2]
    wz = width // nf
    pairs = cols // LANES
    block_rows = 2 * tok

    last_piece = 3 * pairs

    def own(p, use):
        use(wqkv_hbm.at[p % 3, :, pl.ds(p // 3 * LANES, LANES)] if p < last_piece else wo_hbm)

    def slot(p, source):
        if p < last_piece:
            return wq.at[p % 3, pl.ds(pl.multiple_of(source * wz, wz), wz), pl.ds(p // 3 * LANES, LANES)]
        return wo.at[:, pl.ds(pl.multiple_of(source * wz, wz), wz)]

    def own_copy(p):
        box = []
        own(p, lambda src: box.append(pltpu.make_async_copy(src, slot(p, f), own_sems.at[p])))
        return box[0]

    for p in range(last_piece + 1):
        own_copy(p).start()

    head, r = w0.shape[0], w0.shape[1]

    def mlp_own(p, use):
        rows = pl.ds(pl.multiple_of(p // 3 * r, r), r)
        kind = lax.rem(p, 3)

        @pl.when(kind < 2)
        def _():
            use(wgu_hbm.at[kind, rows])

        @pl.when(kind == 2)
        def _():
            use(wd_hbm.at[rows])

    def mlp_slot(p, source):
        return w0.at[p, :, pl.ds(pl.multiple_of(source * wz, wz), wz)]

    mlp_copies = []
    for p in range(head):
        rows = pl.ds(p // 3 * r, r)
        mlp_copies.append(pltpu.make_async_copy(wgu_hbm.at[p % 3, rows] if p % 3 < 2 else wd_hbm.at[rows],
                                                mlp_slot(p, f), own_sems.at[last_piece + 1 + p]))
    for copy in mlp_copies:
        copy.start()
    cot_rows = pl.ds(pl.multiple_of(s * tok, tok), tok)
    cot_own = pltpu.make_async_copy(cot_hbm, cotall_hbm.at[cot_rows], load_sems.at[1])

    w = g1.shape[1]
    spread = LANES // w
    here = lane_of((1, LANES)) // w == lax.rem(me, spread)
    tile[...] = jnp.zeros_like(tile)
    for row, piece in enumerate((g1[...], b1[...], g2[...], b2[...], qb[0:1, :], qb[1:2, :], qb[2:3, :])):
        wide = jnp.concatenate([piece.astype(f32)] * spread, axis=1)
        tile[row:row + 1, :] = jnp.where(here, wide, 0.0)

    everyone_barrier(me, nf, ns)
    gather = LineGather(f, nf, last_piece + 1, own, slot, (ag_sr, ag_rr, ag_sl, ag_rl))
    second = LineGather(f, nf, head, mlp_own, mlp_slot, (m_sr, m_rr, m_sl, m_rl))
    mine = pl.ds(pl.multiple_of(s * tok, tok), tok)

    def small(k):
        t = lax.rem(me + k, total)
        return remote(tile, tiles.at[k], small_s.at[k], small_r.at[k], {"fsdp": t // ns, "seq": lax.rem(t, ns)})

    @pl.loop(1, total)
    def _(k):
        small(k).start()
    for t in range(3):
        gather.send_own(t)
    rows_x = RowGather(s, m, tok, xall, (a_so, a_ro, a_ss, a_rs))
    rows_x.start(x_hbm)
    x_own = pltpu.make_async_copy(x_hbm, xall.at[mine], load_sems.at[3])
    x_own.start()
    cot_own.start()
    tiles[0] = tile[...]
    vecs[...] = jnp.zeros_like(vecs)
    stores = []

    def store(ref, hbm, i):
        st = pltpu.make_async_copy(ref, hbm, out_sems.at[i])
        st.start()
        stores.append(st)

    state = [2]

    def ticks_to(t):
        while state[0] < t:
            state[0] += 1
            gather.tick(state[0])

    gather.arrivals(1)

    @pl.loop(1, total)
    def _(k):
        small(k).wait_recv()

    @pl.loop(0, total)
    def _(k):
        source = lax.rem(me + total - k, total)
        lanes = pl.ds(pl.multiple_of(source // spread * LANES, LANES), LANES)
        vecs[:, lanes] += tiles[k]
    store(vecs, vec_hbm, 2)
    gather.arrivals(2)

    @pl.loop(0, length // block_rows)
    def _(q):
        rows = pl.ds(pl.multiple_of(q * block_rows, block_rows), block_rows)
        cos[rows, :], sin[rows, :] = rotary_tiles(block_rows, q * block_rows)
    store(cos, cos_hbm, 0)
    store(sin, sin_hbm, 1)
    rows_cot = RowGather(s, m, tok, cotall_hbm, (c_so, c_ro, c_ss, c_rs))

    def norm_chip(d):
        @pl.loop(0, 2)
        def _(core):
            rows = pl.ds(pl.multiple_of((xor(j, d, m) * 2 + core) * tok, tok), tok)
            normed, _ = normed_rows(xall[rows, :].astype(f32))
            in1[rows, :] = (normed * vecs[0:1, :] + vecs[1:2, :]).astype(bf16)

    x_own.wait()
    for d in range(m):
        if d > 0:
            rows_x.relay(d)
        if d == min(2, m - 1):
            rows_cot.start(cot_hbm)
            ticks_to(min(3, nf + 1))
        if d > 2:
            rows_x.arrived(d - 1)
            norm_chip(d - 1)
            ticks_to(min(1 + d, nf + 1))
        elif d > 0:
            rows_x.arrived(d - 1)
            norm_chip(d - 1)
    rows_x.arrived(m - 1)
    norm_chip(m - 1)
    store(in1, in1_hbm, 3)

    def project(g):
        lanes = slice(g * LANES, (g + 1) * LANES)
        bias_at = pl.ds(pl.multiple_of(s * cols + g * LANES, LANES), LANES)
        for k in range(3):
            own_copy(3 * g + k).wait()

        @pl.loop(0, length // block_rows)
        def _(q):
            rows = pl.ds(pl.multiple_of(q * block_rows, block_rows), block_rows)
            for k in range(3):
                u = dot_nn(in1[rows, :], wq[k, :, lanes]) + vecs[4 + k:5 + k, bias_at]
                if k < 2:
                    u = turn(u, cos[rows, :], sin[rows, :], 1.0)
                qkv[k, rows, lanes] = u.astype(bf16)

    ticks_to(2 + nf - 1)
    project(0)

    def attend(b, g):
        rows = pl.ds(b * block_rows, block_rows)

        if True:
            lanes = pl.ds(pl.multiple_of(g * LANES, LANES), LANES)
            q, kd, vd = qkv[0, rows, lanes], qkv[1, rows, lanes], qkv[2, rows, lanes]
            lane = lane_of((block_rows, LANES))
            seen = lane_of((block_rows, block_rows)) <= lax.broadcasted_iota(jnp.int32, (block_rows, block_rows), 0)
            out = jnp.zeros((block_rows, LANES), f32)
            logs = lse[rows, :]
            def one_head(h, carry):
                out, logs = carry
                head = lane // HEAD_DIM == h
                qm = jnp.where(head, q.astype(f32) * HEAD_DIM ** -0.5, 0.0).astype(bf16)
                sd = jnp.where(seen, dot_nt(qm, kd), masked_score)
                top = jnp.max(sd, axis=1, keepdims=True)
                if b > 0:
                    before = pl.ds(0, b * block_rows)
                    sl = dot_nt(qm, qkv[1, before, lanes])
                    top = jnp.maximum(top, jnp.max(sl, axis=1, keepdims=True))
                ed = jnp.exp(sd - top)
                tot = jnp.sum(ed, axis=1, keepdims=True)
                if b > 0:
                    el = jnp.exp(sl - top)
                    tot = tot + jnp.sum(el, axis=1, keepdims=True)
                inv = 1.0 / tot
                value = dot_nn((ed * inv).astype(bf16), vd)
                if b > 0:
                    value = value + dot_nn((el * inv).astype(bf16), qkv[2, before, lanes])
                out = jnp.where(head, value, out)
                logs = jnp.where(lane == g * PER + h, top + jnp.log(tot), logs)
                return out, logs

            out, logs = lax.fori_loop(0, PER, one_head, (out, logs))
            att[rows, lanes] = out.astype(bf16)
            lse[rows, :] = logs

    lse[...] = jnp.zeros_like(lse)
    sums = RowReduce(s, m, from_sib, from_off, (r_ss, r_rs, r_so, r_ro))

    @pl.loop(0, (pairs + 1) * m)
    def _(turn_here):
        g, step = turn_here // m, lax.rem(turn_here, m)
        d = m - 1 - step
        chip = xor(j, d, m)

        for later in range(1, pairs):
            @pl.when((g == later) & (step == 0))
            def _(later=later):
                project(later)
        for b in range(m):
            @pl.when((g < pairs) & (chip == b))
            def _(b=b):
                attend(b, g)

        for later in range(1, pairs):
            for t in range(3 * later + nf - 1, 3 * later + nf + 2):
                @pl.when((g == later - 1) & (step == min(t - 3 * later - nf + 1, m - 1)))
                def _(t=t):
                    gather.tick(t)
                    if t == last_piece + nf - 2:
                        for p in range(head):
                            second.send_own(jnp.int32(p))
        for k in range(1, m):
            @pl.when((g == (0 if k < m - 1 else pairs - 1)) & (step == k))
            def _(k=k):
                rows_cot.relay(k)

        @pl.when((g == pairs) & (step == 0))
        def _():
            gather.tick(last_piece + nf - 1)
            own_copy(last_piece).wait()
            if pairs == 1:
                for p in range(head):
                    second.send_own(jnp.int32(p))

        @pl.when(g == pairs)
        def _():
            rows = pl.ds(pl.multiple_of(chip * block_rows, block_rows), block_rows)
            part[...] = dot_nn(att[rows, :], wo[...])
            give[d] = part[pl.ds(pl.multiple_of((1 - c) * tok, tok), tok), :].astype(bf16)
            keep[d] = part[pl.ds(pl.multiple_of(c * tok, tok), tok), :]
            sums.give(d, give.at[d])

            @pl.when(step > 0)
            def _():
                sums.pass_on(d + 1, keep[d + 1])
    second.arrivals(jnp.int32(1))
    ticks = list(range(2, head + nf - 1))
    store(qkv, qkv_hbm, 4)
    store(wq, wq_hbm, 5)
    store(wo, woall_hbm, 6)
    store(att, att_hbm, 7)
    store(lse, lse_hbm, 8)
    rows_cot.finish()
    res[...] = xall[mine, :].astype(f32) + sums.total(keep[0])
    store(res, res_hbm, 9)
    normed, _ = normed_rows(res[...])
    in2[...] = (normed * vecs[2:3, :] + vecs[3:4, :]).astype(bf16)
    rows_two = RowGather(s, m, tok, in2_hbm, (e_so, e_ro, e_ss, e_rs))
    rows_two.start(in2)
    in2_own = pltpu.make_async_copy(in2, in2_hbm.at[mine], load_sems.at[2])
    in2_own.start()
    if ticks:
        second.arrivals(jnp.int32(ticks.pop(0)))
    for d in range(1, m):
        rows_two.relay(d)
        if ticks and d < m - 1:
            second.arrivals(jnp.int32(ticks.pop(0)))
    rows_two.finish()
    for t in ticks:
        second.arrivals(jnp.int32(t))
    for copy in mlp_copies:
        copy.wait()
    store(w0, w0_hbm, 10)

    @pl.loop(1, total)
    def _(k):
        small(k).wait_send()
    for p in range(last_piece + 1):
        gather.drain(p)
    for p in range(head):
        second.drain(p)
    rows_x.drain(x_hbm)
    rows_cot.drain(cot_hbm)
    rows_two.drain(in2)
    sums.drain(lambda d: give.at[d])
    cot_own.wait()
    in2_own.wait()
    for st in stores:
        st.wait()


def front(x, cot, g1, b1, g2, b2, qb, wqkv, wo, wgu, wd, nf, ns, cid):
    r = piece_rows(wd.shape[0])
    tok, width = x.shape
    cols, wz = wo.shape
    length = tok * ns
    m = ns // 2
    w = g1.shape[1]
    pairs = cols // LANES
    D, V = pltpu.SemaphoreType.DMA, pltpu.VMEM
    A = pl.BlockSpec(memory_space=pl.ANY)
    M = pl.BlockSpec(memory_space=pltpu.VMEM)
    S = jax.ShapeDtypeStruct
    return pl.pallas_call(
        functools.partial(front_kernel, nf, ns),
        out_shape=(
            S((length, width), bf16), S((length, width), bf16), S((length, width), bf16),
            S((3, length, cols), bf16), S((length, cols), bf16), S((length, LANES), f32),
            S((tok, width), f32), S((3, width, cols), bf16), S((cols, width), bf16),
            S((8, width), f32), S((length, LANES), f32), S((length, LANES), f32), S((HEAD_PIECES, r, width), bf16),
        ),
        in_specs=[A, A, M, M, M, M, M, A, A, A, A],
        out_specs=[A] * 13,
        scratch_shapes=[
            V((length, width), bf16), V((length, width), bf16), V((8, LANES), f32), V((nf * ns, 8, LANES), f32),
            V((8, width), f32), V((3, width, cols), bf16), V((cols, width), bf16), V((3, length, cols), bf16),
            V((length, cols), bf16), V((length, LANES), f32), V((length, LANES), f32), V((length, LANES), f32),
            V((2 * tok, width), f32), V((m, tok, width), f32), V((m, tok, width), bf16),
            V((m, tok, width), bf16), V((m - 1, tok, width), bf16), V((tok, width), f32), V((tok, width), bf16),
            V((HEAD_PIECES, r, width), bf16),
            D((4,)), D((3 * pairs + 1 + HEAD_PIECES,)), D((nf * ns,)), D((nf * ns,)),
        ] + [D((3 * pairs + 1, nf - 1))] * 4 + [D((HEAD_PIECES, nf - 1))] * 4 + ([D((2 * m,))] * 2 + [D((m,))] * 2) * 3 + [D((m,))] * 2 + [D((2 * m,))] * 2 + [D((11,))],
        compiler_params=pltpu.CompilerParams(
            collective_id=cid, has_side_effects=True, vmem_limit_bytes=64 * 1024 * 1024 - 65536),
        name="front",
    )(x, cot, g1, b1, g2, b2, qb, wqkv, wo, wgu, wd)


def back_kernel(nf, ns, left,
                gsum_hbm, osum_hbm, res_hbm, cot_hbm, x_hbm, vec_hbm, qkv_hbm, att_hbm, lse_hbm, in1_hbm, wq_hbm, wo_hbm,
                cos_hbm, sin_hbm, *more):
    if left:
        (rest_hbm, _, _, out_hbm, ig_hbm, gqkv_hbm, gout_hbm, o_g1, o_b1, o_g2, o_b2, o_qb, ggu_hbm, gd_hbm) = more[:14]
        (rest, rest_left, rest_right, rest_stage, rest_sems, q_sr, q_rr, q_sl, q_rl) = more[-9:]
        more = more[14:-9]
    else:
        (out_hbm, ig_hbm, gqkv_hbm, gout_hbm, o_g1, o_b1, o_g2, o_b2, o_qb) = more[:9]
        more = more[9:]
    (keep, res, cot, vec, qkv, att, lse, in1, wq, wo, cos, sin,
                grows, ga, gq, dk, dv, parts, from_left, from_right, stage, stage_t,
                g_sib, g_off, o_sib, o_off, i_sib, i_off, gres, sums, tiles,
                load_sems, keep_sems, in1_sems, small_s, small_r,
                rs_sr, rs_rr, rs_sl, rs_rl,
                w_so, w_ro, w_ss, w_rs,
                g_ss, g_rs, g_so, g_ro, o_ss, o_rs, o_so, o_ro, i_ss, i_rs, i_so, i_ro,
     stage_sems, out_sems) = more
    f, s = lax.axis_index("fsdp"), lax.axis_index("seq")
    total = nf * ns
    me = f * ns + s
    m = ns // 2
    j, c = s // 2, s % 2
    tok, width = cot.shape
    length, cols = att.shape
    wz = width // nf
    pairs = cols // LANES
    block_rows = 2 * tok
    count = 4 * pairs
    span = 768 if length <= 1024 else 256
    mine = pl.ds(pl.multiple_of(s * tok, tok), tok)

    def rows_at(ref, chip, core):
        return ref.at[pl.ds(pl.multiple_of((chip * 2 + core) * tok, tok), tok)]

    def keep_load(hbm, d, at):
        return pltpu.make_async_copy(rows_at(hbm, xor(j, d, m), c), keep.at[d], keep_sems.at[2 * d + at])

    for d in range(m - 1, -1, -1):
        keep_load(gsum_hbm, d, 0).start()
    plain = [(res_hbm, res), (cot_hbm, cot), (vec_hbm, vec), (wo_hbm, wo), (att_hbm, att), (qkv_hbm, qkv),
             (lse_hbm, lse), (wq_hbm, wq), (cos_hbm, cos), (sin_hbm, sin)]
    loads = [pltpu.make_async_copy(a, b, load_sems.at[i]) for i, (a, b) in enumerate(plain)]
    for load in loads:
        load.start()

    def in1_load(k):
        return pltpu.make_async_copy(in1_hbm.at[:, pl.ds(k * wz, wz)], in1.at[k % 2], in1_sems.at[k % 2])
    in1_load(0).start()
    if left:
        rest_load = pltpu.make_async_copy(rest_hbm, rest, rest_sems.at[0])
        rest_load.start()

    everyone_barrier(me, nf, ns)
    two = RowReduce(s, m, g_sib, g_off, (g_ss, g_rs, g_so, g_ro))
    out = RowReduce(s, m, o_sib, o_off, (o_ss, o_rs, o_so, o_ro))

    waiting = []
    if left:
        r = rest.shape[1]
        skipped = 3 * (gd_hbm.shape[0] // r) - left

        def rest_out(p, act):
            kind, sl = lax.rem(p + skipped, 3), lax.rem(p, 2)
            at = pl.ds(pl.multiple_of((p + skipped) // 3 * r, 16), r)

            @pl.when(kind < 2)
            def _():
                act(pltpu.make_async_copy(rest_stage.at[sl], ggu_hbm.at[kind, at], rest_sems.at[sl]))

            @pl.when(kind == 2)
            def _():
                act(pltpu.make_async_copy(rest_stage.at[sl], gd_hbm.at[at], rest_sems.at[sl]))

        def rest_finish(p):
            @pl.when(p >= 2)
            def _():
                rest_out(p - 2, lambda cc: cc.wait())
            sl = lax.rem(p, 2)
            rest_stage[sl] = rest[p, :, pl.ds(pl.multiple_of(f * wz, wz), wz)].astype(f32)

            @pl.when(f > 0)
            def _():
                rest_stage[sl] += rest_left[p, jnp.maximum(f - 1, 0)].astype(f32)

            @pl.when(f < nf - 1)
            def _():
                rest_stage[sl] += rest_right[p, jnp.minimum(f, nf - 2)].astype(f32)
            rest_out(p, lambda cc: cc.start())

        rest_sum = LineReduce(f, nf, left, lambda p, k: rest.at[p, :, pl.ds(pl.multiple_of(k * wz, wz), wz)], rest_left, rest_right,
                              (q_sr, q_rr, q_sl, q_rl), rest_finish)
        waiting = list(range(left + nf - 1))

    def rest_tick(how_many=1):
        for _ in range(how_many):
            if waiting:
                rest_sum.tick(jnp.int32(waiting.pop(0)))

    def two_src(d):
        return rows_at(gsum_hbm, xor(j, d, m), 1 - c)

    def out_src(d):
        return rows_at(osum_hbm, xor(j, d, m), 1 - c)

    for d in range(m - 1, -1, -1):
        two.give(d, two_src(d))
    if left:
        rest_load.wait()
    rest_tick()
    for d in range(m - 1, -1, -1):
        keep_load(gsum_hbm, d, 0).wait()
    for d in range(m - 1, 0, -1):
        two.pass_on(d, keep[d])
    two.forward()
    for d in range(m - 1, -1, -1):
        out.give(d, out_src(d))
    rest_tick()
    for load in loads[:3]:
        load.wait()
    sums[...] = jnp.zeros_like(sums)
    normed, inverse = normed_rows(res[...])
    grad = two.collect(keep[0])
    for d in range(m - 1, -1, -1):
        keep_load(osum_hbm, d, 1).start()
    sums[2:3, :] = jnp.sum(grad * normed, axis=0, keepdims=True)
    sums[3:4, :] = jnp.sum(grad, axis=0, keepdims=True)

    def norm_grad(grad, normed, inverse, gain):
        scaled = grad * gain
        return inverse * (scaled - jnp.mean(scaled, axis=-1, keepdims=True)
                          - normed * jnp.mean(scaled * normed, axis=-1, keepdims=True))

    gres[...] = cot[...].astype(f32) + norm_grad(grad, normed, inverse, vec[2:3, :])
    grows[mine, :] = gres[...].astype(bf16)
    x_load = pltpu.make_async_copy(x_hbm, cot, load_sems.at[len(plain)])
    x_load.start()
    rows_w = RowGather(s, m, tok, grows, (w_so, w_ro, w_ss, w_rs))
    rows_w.start(grows.at[mine])
    rest_tick()
    for load in loads[3:]:
        load.wait()

    def block(p, k):
        return parts.at[p, :, pl.ds(pl.multiple_of(k * wz, wz), wz)]

    def staged(p, act):
        sl = lax.rem(p, 2)

        @pl.when(p < pairs)
        def _():
            act(pltpu.make_async_copy(
                stage.at[sl], gout_hbm.at[pl.ds(pl.multiple_of(p * LANES, LANES), LANES)], stage_sems.at[sl]))

        @pl.when(p >= pairs)
        def _():
            q = p - pairs
            lanes = pl.ds(pl.multiple_of(q // 3 * LANES, LANES), LANES)
            act(pltpu.make_async_copy(stage_t.at[sl], gqkv_hbm.at[lax.rem(q, 3), :, lanes], stage_sems.at[sl]))

    def finish(p):
        @pl.when(p >= 2)
        def _():
            staged(p - 2, lambda cc: cc.wait())
        sl = lax.rem(p, 2)
        stage[sl] = parts[p, :, pl.ds(pl.multiple_of(f * wz, wz), wz)].astype(f32)

        @pl.when(f > 0)
        def _():
            stage[sl] += from_left[p, jnp.maximum(f - 1, 0)].astype(f32)

        @pl.when(f < nf - 1)
        def _():
            stage[sl] += from_right[p, jnp.minimum(f, nf - 2)].astype(f32)

        @pl.when(p >= pairs)
        def _():
            stage_t[sl] = stage[sl].T
        staged(p, lambda cc: cc.start())

    reduce = LineReduce(f, nf, count, block, from_left, from_right, (rs_sr, rs_rr, rs_sl, rs_rl), finish)

    def attend_back(b, g):
        lanes = pl.ds(pl.multiple_of(g * LANES, LANES), LANES)
        lane = lane_of((block_rows, LANES))
        seen = lane_of((block_rows, block_rows)) <= lax.broadcasted_iota(jnp.int32, (block_rows, block_rows), 0)
        rows = pl.ds(b * block_rows, block_rows)
        q = qkv[0, rows, lanes].astype(f32) * HEAD_DIM ** -0.5
        go = ga[rows, lanes].astype(f32)
        both = go * att[rows, lanes].astype(f32)
        logs = lse[rows, :]
        grad_q = jnp.zeros((block_rows, LANES), f32)
        def one_head(h, grad_q):
            head = lane // HEAD_DIM == h
            qm = jnp.where(head, q, 0.0).astype(bf16)
            gm = jnp.where(head, go, 0.0).astype(bf16)
            delta = jnp.sum(jnp.where(head, both, 0.0), axis=1, keepdims=True)
            log = jnp.sum(jnp.where(lane == g * PER + h, logs, 0.0), axis=1, keepdims=True)
            acc = jnp.zeros((block_rows, LANES), f32)
            spans = [(k, min(span, b * block_rows - k)) for k in range(0, b * block_rows, span)]
            for first, size in spans + [(b * block_rows, block_rows)]:
                at = pl.ds(first, size)
                key, val = qkv[1, at, lanes], qkv[2, at, lanes]
                pr = jnp.exp(dot_nt(qm, key) - log)
                if first == b * block_rows:
                    pr = jnp.where(seen, pr, 0.0)
                gp = dot_nt(gm, val)
                gs = (pr * (gp - delta)).astype(bf16)
                dv[at, :] += dot_tn(pr.astype(bf16), gm)
                dk[at, :] += dot_tn(gs, qm)
                acc = acc + dot_nn(gs, key)
            return jnp.where(head, acc * HEAD_DIM ** -0.5, grad_q)

        grad_q = lax.fori_loop(0, PER, one_head, grad_q)
        gq[0, rows, lanes] = turn(grad_q, cos[rows, :], sin[rows, :], -1.0).astype(bf16)

    def weight_pieces(g):
        lanes = pl.ds(pl.multiple_of(g * LANES, LANES), LANES)

        @pl.loop(0, m)
        def _(b):
            rows = pl.ds(pl.multiple_of(b * block_rows, block_rows), block_rows)
            gq[1, rows, lanes] = turn(dk[rows, :], cos[rows, :], sin[rows, :], -1.0).astype(bf16)
            gq[2, rows, lanes] = dv[rows, :].astype(bf16)
        at_once = 3 if length <= 1024 else 1
        wide = [[gq[i, :, lanes] for i in range(3)]] if at_once == 3 else [[gq[i, :, lanes]] for i in range(3)]
        at = pl.ds(pl.multiple_of(s * cols + g * LANES, LANES), LANES)
        for k in range(3):
            sums[4 + k:5 + k, at] = jnp.sum(gq[k, :, lanes].astype(f32), axis=0, keepdims=True)
        for k in range(nf):
            in1_load(k).wait()
            in1_load((k + 1) % nf).start()
            for n, some in enumerate(wide):
                value = dot_tn(jnp.concatenate(some, axis=1), in1[k % 2]).astype(bf16)
                for i in range(at_once):
                    parts[pairs + 3 * g + n + i, :, k * wz:(k + 1) * wz] = value[i * LANES:(i + 1) * LANES, :]

    @pl.loop(0, pairs * m)
    def _(turn_here):
        g, step = turn_here // m, lax.rem(turn_here, m)
        chip = xor(j, step, m)
        rows = pl.ds(pl.multiple_of(chip * block_rows, block_rows), block_rows)

        @pl.when(step == 0)
        def _():
            dk[...] = jnp.zeros_like(dk)
            dv[...] = jnp.zeros_like(dv)
        for d in range(m):
            @pl.when((g == 0) & (step == d))
            def _(d=d):
                if d > 0:
                    rows_w.relay(d)
                rows_w.arrived(d)
                if d > 0:
                    rest_tick()

        @pl.when(g == 0)
        def _():
            ga[rows, :] = dot_nt(grows[rows, :], wo[...]).astype(bf16)

        @pl.when((g == 0) & (step == m - 1))
        def _():
            for d in range(m - 1, -1, -1):
                keep_load(osum_hbm, d, 1).wait()
            for d in range(m - 1, 0, -1):
                out.pass_on(d, keep[d])
            for k in range(nf):
                lanes = slice(k * wz, (k + 1) * wz)
                value = dot_tn(att[...], grows[:, lanes]).astype(bf16)
                for i in range(pairs):
                    parts[i, :, lanes] = value[i * LANES:(i + 1) * LANES, :]
            rest_tick(len(waiting))
            reduce.tick(jnp.int32(0))
        for b in range(m):
            @pl.when(chip == b)
            def _(b=b):
                attend_back(b, g)

        @pl.when((g > 0) & (step % (m // 2) == m // 2 - 1))
        def _():
            reduce.tick(pairs + 3 * (g - 1) + 1 + (step + 1) // (m // 2) - 1)

        @pl.when((g == pairs - 1) & (step == m - 1))
        def _():
            out.forward()

        @pl.when(step == m - 1)
        def _():
            @pl.when(g == 0)
            def _():
                for p in range(1, pairs):
                    reduce.tick(jnp.int32(p))
            weight_pieces(g)
            reduce.tick(pairs + 3 * g)
    in1_load(0).wait()

    keep[0] = (res[...] + out.collect(keep[0])).astype(bf16)
    stores = [pltpu.make_async_copy(keep.at[0], out_hbm, out_sems.at[0])]
    stores[0].start()
    out.drain(out_src)
    one = RowReduce(s, m, i_sib, i_off, (i_ss, i_rs, i_so, i_ro))
    rows_w.drain(grows.at[mine])

    def half_of(d, core):
        return grows.at[pl.ds(pl.multiple_of((2 * d + core) * tok, tok), tok)]

    late = list(range(pairs + 3 * (pairs - 1) + 1, count + nf - 1))
    for d in range(m - 1, -1, -1):
        rows = pl.ds(pl.multiple_of(xor(j, d, m) * block_rows, block_rows), block_rows)
        value = dot_nt(gq[0, rows, :], wq[0])
        for k in (1, 2):
            value = value + dot_nt(gq[k, rows, :], wq[k])
        grows[d * block_rows:(d + 1) * block_rows, :] = value.astype(bf16)
        one.give(d, half_of(d, 1 - c))
        if d < m - 1:
            one.pass_on(d + 1, half_of(d + 1, c)[...])
        if late and d % 2 == 1:
            reduce.tick(jnp.int32(late.pop(0)))
    grad = one.total(half_of(0, c)[...])
    x_load.wait()
    normed, inverse = normed_rows(cot[...].astype(f32))
    sums[0:1, :] = jnp.sum(grad * normed, axis=0, keepdims=True)
    sums[1:2, :] = jnp.sum(grad, axis=0, keepdims=True)
    res[...] = gres[...] + norm_grad(grad, normed, inverse, vec[0:1, :])
    stores.append(pltpu.make_async_copy(res, ig_hbm, out_sems.at[1]))
    stores[1].start()

    w = o_g1.shape[1]
    spread = LANES // w

    def tile_of(t):
        return sums.at[:, pl.ds(pl.multiple_of(t // spread * LANES, LANES), LANES)]

    def small(k):
        t = lax.rem(me + k, total)
        return remote(tile_of(t), tiles.at[k], small_s.at[k], small_r.at[k],
                      {"fsdp": t // ns, "seq": lax.rem(t, ns)})

    @pl.loop(1, total)
    def _(k):
        small(k).start()
    @pl.loop(late[0], late[-1] + 1)
    def _(t):
        reduce.tick(t)
    tiles[0] = tile_of(me)[...]

    @pl.loop(1, total)
    def _(k):
        small(k).wait_recv()
        tiles[0] += tiles[k]
    for k in range(spread):
        @pl.when(lax.rem(me, spread) == k)
        def _(k=k):
            lanes = slice(k * w, (k + 1) * w)
            for i, ref in enumerate((o_g1, o_b1, o_g2, o_b2)):
                ref[...] = tiles[0, i:i + 1, lanes]
            o_qb[...] = tiles[0, 4:7, lanes]

    @pl.loop(1, total)
    def _(k):
        small(k).wait_send()
    two.drain(two_src)
    one.drain(lambda d: half_of(d, 1 - c))
    for p in (count - 2, count - 1):
        staged(jnp.int32(p), lambda cc: cc.wait())
    for st in stores:
        st.wait()
    if left:
        for p in (left - 2, left - 1):
            rest_out(jnp.int32(p), lambda cc: cc.wait())


def back(gsum, osum, res, cot, x, vec, qkv, att, lse, in1, wq, wo, cos, sin, rest, ggu, gd, nf, ns, cid):
    left = 0 if rest is None else rest.shape[0]
    tok, width = x.shape
    length, cols = att.shape
    wz = width // nf
    m = ns // 2
    w = width // (nf * ns)
    pairs = cols // LANES
    count = 4 * pairs
    D, V = pltpu.SemaphoreType.DMA, pltpu.VMEM
    A = pl.BlockSpec(memory_space=pl.ANY)
    M = pl.BlockSpec(memory_space=pltpu.VMEM)
    S = jax.ShapeDtypeStruct
    extra_in, extra_out, extra_scratch = (), (), []
    if left:
        r = rest.shape[1]
        extra_in = (rest, ggu, gd)
        extra_out = (S(ggu.shape, f32), S(gd.shape, f32))
        extra_scratch = [V((left, r, width), bf16), V((left, nf - 1, r, wz), bf16),
                         V((left, nf - 1, r, wz), bf16), V((2, r, wz), f32), D((2,))] + [D((left, nf - 1))] * 4
    rows_v = V((m, tok, width), bf16)
    offs_v = V((m - 1, tok, width), bf16)
    return pl.pallas_call(
        functools.partial(back_kernel, nf, ns, left),
        out_shape=(
            S((tok, width), bf16), S((tok, width), f32), S((3, wz, cols), f32), S((cols, wz), f32),
            S((1, w), f32), S((1, w), f32), S((1, w), f32), S((1, w), f32), S((3, w), f32),
        ) + extra_out,
        in_specs=[A] * (14 + len(extra_in)),
        out_specs=[A] * 4 + [M] * 5 + [A] * len(extra_out),
        input_output_aliases={15: 9, 16: 10} if left else {},
        scratch_shapes=[
            rows_v, V((tok, width), f32), V((tok, width), bf16), V((8, width), f32),
            V((3, length, cols), bf16), V((length, cols), bf16), V((length, LANES), f32), V((2, length, wz), bf16),
            V((3, width, cols), bf16), V((cols, width), bf16), V((length, LANES), f32), V((length, LANES), f32),
            V((length, width), bf16), V((length, cols), bf16), V((3, length, cols), bf16),
            V((length, LANES), f32), V((length, LANES), f32),
            V((count, LANES, width), bf16), V((count, nf - 1, LANES, wz), bf16), V((count, nf - 1, LANES, wz), bf16),
            V((2, LANES, wz), f32), V((2, wz, LANES), f32),
            rows_v, offs_v, rows_v, offs_v, rows_v, offs_v,
            V((tok, width), f32),
            V((8, width), f32), V((nf * ns, 8, LANES), f32),
            D((11,)), D((2 * m,)), D((2,)), D((nf * ns,)), D((nf * ns,)),
        ] + [D((count, nf - 1))] * 4 + [D((2 * m,))] * 2 + [D((m,))] * 2 + [D((m,)), D((m,)), D((2 * m,)), D((2 * m,))] * 3 + [D((2,)), D((2,))]
        + extra_scratch,
        compiler_params=pltpu.CompilerParams(
            collective_id=cid, has_side_effects=True, vmem_limit_bytes=64 * 1024 * 1024 - 65536),
        name="back",
    )(gsum, osum, res, cot, x, vec, qkv, att, lse, in1, wq, wo, cos, sin, *extra_in)


def local(
    block_input,
    cotangent,
    ln1_gain,
    ln1_bias,
    qkv_weight,
    qkv_bias,
    out_weight,
    ln2_gain,
    ln2_bias,
    gate_up_weight,
    down_weight,
):
    fsdp, seq = lax.axis_size("fsdp"), lax.axis_size("seq")
    gate_up = jnp.transpose(gate_up_weight, (1, 2, 0))
    left = 4 if seq * block_input.shape[1] <= 1024 else 0
    (in_one, cot_all, in_two, qkv, mixed, logs, residual, qkv_full, out_full, vectors, cosine, sine, first) = front(
        block_input[0],
        cotangent[0],
        ln1_gain[None],
        ln1_bias[None],
        ln2_gain[None],
        ln2_bias[None],
        qkv_bias,
        jnp.transpose(qkv_weight, (1, 0, 2)),
        out_weight,
        gate_up,
        down_weight,
        fsdp,
        seq,
        1,
    )
    out_sum, grad_sum, grad_gate_up, grad_down, *rest = mlp(
        in_two, cot_all, first, gate_up, down_weight, fsdp, left, 0
    )
    block_output, input_grad, grad_qkv, grad_out, gain_one, bias_one, gain_two, bias_two, grad_bias, *grads = back(
        grad_sum,
        out_sum,
        residual,
        cotangent[0],
        block_input[0],
        vectors,
        qkv,
        mixed,
        logs,
        in_one,
        qkv_full,
        out_full,
        cosine,
        sine,
        rest[0] if left else None,
        grad_gate_up,
        grad_down,
        fsdp,
        seq,
        2,
    )
    if left:
        grad_gate_up, grad_down = grads
    return (
        block_output[None],
        input_grad[None],
        gain_one[0],
        bias_one[0],
        jnp.transpose(grad_qkv, (1, 0, 2)),
        grad_bias,
        grad_out,
        gain_two[0],
        bias_two[0],
        jnp.transpose(grad_gate_up, (2, 0, 1)),
        grad_down,
    )


def solution(mesh):
    placed = (
        P("fsdp", "seq", None),
        P("fsdp", "seq", None),
        P(("fsdp", "seq")),
        P(("fsdp", "seq")),
        P("fsdp", None, "seq"),
        P(None, ("fsdp", "seq")),
        P("seq", "fsdp"),
        P(("fsdp", "seq")),
        P(("fsdp", "seq")),
        P("fsdp", None, "seq"),
        P("seq", "fsdp"),
    )
    return jax.shard_map(
        local,
        mesh=mesh,
        in_specs=placed,
        out_specs=(
            P("fsdp", "seq", None),
            P("fsdp", "seq", None),
            P(("fsdp", "seq")),
            P(("fsdp", "seq")),
            P("fsdp", None, "seq"),
            P(None, ("fsdp", "seq")),
            P("seq", "fsdp"),
            P(("fsdp", "seq")),
            P(("fsdp", "seq")),
            P("fsdp", None, "seq"),
            P("seq", "fsdp"),
        ),
        check_vma=False,
    )
```
